32 devices in a mesh: gz: 16 (over z, y, x), gx: 2 (over core).
Axes of the slice: x: 2, y: 2, z: 4, core: 2. Of those that a mesh axis runs over, the one named last changes fastest.
Arguments:
- b_field: float32 [3, 48, 128, 256], P(None, 'gx', 'gz'), may hold values from -6 to 6
- resist: float32 [48, 128, 256], P('gx', 'gz'), may hold values from 0.05 to 0.8
- ymix: float32 [256, 256], replicated, may hold values from -0.5 to 1.5
- zmix: float32 [128, 128], replicated, may hold values from -0.5 to 1.5
Outputs:
- b_next: float32 [3, 48, 128, 256], P(None, 'gx', 'gz')
- potential: float32 [3, 48, 128, 256], P(None, 'gx', 'gz')
The draws below stay inside these ranges and needn't reach their ends.
All inputs are finite; a program needn't handle non-finite values.
Results may differ from the reference program's by a relative error of at most 0.000073.
Values sent between devices are 32-bit elements; how exact they have to be, the bound alone decides.
No kernel may reach another device: no remote copies, remote signals or barrier semaphores. Data moves between devices by JAX's collectives and lax.ppermute only.
A program may use at most 64 MiB of HBM per device.

```python
import math
import jax
import jax.numpy as jnp
from jax import lax

NY = 256
NX = 48
NZ = 128


def draw_ymix(key, part):
    noise = jax.random.normal(key, (NY, NY), jnp.float32)
    return jnp.eye(NY, dtype=jnp.float32) + 0.6 * noise * NY ** (-0.5)


def draw_zmix(key, part):
    subkey = jax.random.fold_in(key, 7)
    noise = jax.random.normal(subkey, (NZ, NZ), jnp.float32)
    return jnp.eye(NZ, dtype=jnp.float32) + 0.6 * noise * NZ ** (-0.5)


def block_levels(stream_key, extent, split, low, largest):
    level, own = 1.0, jax.random.fold_in(stream_key, 6)
    for dim, shards_of in split:
        heights = jnp.exp(jax.random.uniform(jax.random.fold_in(own, dim), (shards_of,), jnp.float32, low / len(split), largest / len(split)))
        level = level * jnp.repeat(heights, extent[dim] // shards_of).reshape([-1 if axis == dim else 1 for axis in range(len(extent))])
    return level


def centred(key, shape, width, reach, cuts=(), kind=jnp.bfloat16):
    result = width * jax.random.normal(key, shape, jnp.float32)
    if cuts:
        result = result * block_levels(key, shape, cuts, -0.22, 0.18)
    return jnp.clip(result, -reach, reach).astype(kind)


def setup_inputs(seed: int = 0) -> dict:
    key_list = jax.random.split(jax.random.key(seed), 5)
    return {
        "b_field": centred(key_list[0], (3, NX, NZ, NY), 1.0, 6.0, ((1, 2), (2, 16)), jnp.float32),
        "resist": jnp.clip(jnp.exp(math.log(0.8) - 2.7725887 * jax.random.uniform(key_list[1], (NX, NZ, NY), jnp.float32) ** block_levels(key_list[1], (NX, NZ, NY), ((0, 2), (1, 16)), -0.2, 0.2)), 0.05, 0.8),
        "ymix": draw_ymix(jax.random.fold_in(key_list[4], 71), 0),
        "zmix": draw_zmix(jax.random.fold_in(key_list[4], 71), 0),
    }


time_step = 0.1
friction = 1.0


def curl_of(padded):
    centre = padded[:, 1:-1, 1:-1, :]
    grad_x = (padded[:, 2:, 1:-1, :] - padded[:, :-2, 1:-1, :]) * 0.5
    grad_z = (padded[:, 1:-1, 2:, :] - padded[:, 1:-1, :-2, :]) * 0.5
    grad_y = (jnp.roll(centre, -1, 3) - jnp.roll(centre, 1, 3)) * 0.5
    return jnp.stack([grad_y[2] - grad_z[1], grad_z[0] - grad_x[2], grad_x[1] - grad_y[0]])


def cross_product(lhs_vec, rhs_vec):
    return jnp.stack([lhs_vec[1] * rhs_vec[2] - lhs_vec[2] * rhs_vec[1],
                      lhs_vec[2] * rhs_vec[0] - lhs_vec[0] * rhs_vec[2],
                      lhs_vec[0] * rhs_vec[1] - lhs_vec[1] * rhs_vec[0]])


def electric(current, field, resist):
    strength = jnp.sum(field * field, axis=0) + 1.0
    velocity = cross_product(current, field) / (friction * strength)
    return resist * current - cross_product(velocity, field)


def reference(b_field, resist, ymix, zmix):
    widths = ((0, 0), (1, 1), (1, 1), (0, 0))
    current = curl_of(jnp.pad(b_field, widths))
    efield = electric(current, b_field, resist)
    curl_e = curl_of(jnp.pad(efield, widths))
    stepped = b_field - time_step * curl_e
    along_y = jnp.einsum('cxzi,ij->cxzj', stepped, ymix, precision=lax.Precision.HIGHEST)
    b_next = jnp.einsum('cxmy,mk->cxky', along_y, zmix, precision=lax.Precision.HIGHEST)
    column = jnp.cumsum(b_next, axis=2) * (NZ ** -0.5)
    potential = jnp.stack([column[1], -column[0], column[2]])
    return b_next, potential
```

```python
import functools
import jax
import jax.numpy as jnp
from jax import lax
from jax.experimental import pallas as pl
from jax.experimental.pallas import tpu as pltpu
from jax.sharding import PartitionSpec as P

time_step = 0.1
friction = 1.0
LANES = 128
SUBLANES = 8
VMEM = pl.BlockSpec(memory_space=pltpu.VMEM)
SMEM = pl.BlockSpec(memory_space=pltpu.SMEM)


def with_halo(block, sides, width):
    for axis, dim in sides:
        count = lax.axis_size(axis)
        forward = [(i, i + 1) for i in range(count - 1)]
        backward = [(target, source) for source, target in forward]
        low = lax.ppermute(
            lax.slice_in_dim(block, block.shape[dim] - width, None, axis=dim), axis, forward
        )
        high = lax.ppermute(lax.slice_in_dim(block, 0, width, axis=dim), axis, backward)
        block = jnp.concatenate([low, block, high], axis=dim)
    return block


def curl_of(padded):
    centre = padded[:, 1:-1, 1:-1, :]
    grad_x = (padded[:, 2:, 1:-1, :] - padded[:, :-2, 1:-1, :]) * 0.5
    grad_z = (padded[:, 1:-1, 2:, :] - padded[:, 1:-1, :-2, :]) * 0.5
    grad_y = (jnp.roll(centre, -1, 3) - jnp.roll(centre, 1, 3)) * 0.5
    return jnp.stack([grad_y[2] - grad_z[1], grad_z[0] - grad_x[2], grad_x[1] - grad_y[0]])


def cross_parts(lhs, rhs):
    return (
        lhs[1] * rhs[2] - lhs[2] * rhs[1],
        lhs[2] * rhs[0] - lhs[0] * rhs[2],
        lhs[0] * rhs[1] - lhs[1] * rhs[0],
    )


def electric_parts(current, field, resist):
    strength = field[0] * field[0] + field[1] * field[1] + field[2] * field[2] + 1.0
    inverse = 1.0 / (friction * strength)
    velocity = [part * inverse for part in cross_parts(current, field)]
    pushed = cross_parts(velocity, field)
    return [resist * current[c] - pushed[c] for c in range(3)]


def plain_form(b_field, resist, ymix, zmix):
    cells_z = b_field.shape[2]
    total_z = cells_z * lax.axis_size("gz")
    padded = with_halo(b_field, (("gz", 2), ("gx", 1)), 1)
    efield = jnp.stack(electric_parts(curl_of(padded), b_field, resist))
    curl_e = curl_of(with_halo(efield, (("gz", 2), ("gx", 1)), 1))
    stepped = b_field - time_step * curl_e
    along_y = jnp.einsum("cxzi,ij->cxjz", stepped, ymix, precision=lax.Precision.HIGHEST)
    running = jnp.cumsum(zmix, axis=1)
    slab_ends = running[:, cells_z - 1 :: cells_z][:, :-1]
    lower_flux = jnp.concatenate([jnp.zeros((total_z, 1), jnp.float32), slab_ends], axis=1)
    line_matrix = jnp.concatenate([zmix, lower_flux], axis=1)
    product = jnp.einsum(
        "cxym,mk->cxyk",
        lax.all_to_all(along_y, "gz", split_axis=2, concat_axis=3, tiled=True),
        line_matrix,
        precision=lax.Precision.HIGHEST,
    )
    returned, returned_flux = (
        lax.all_to_all(part, "gz", split_axis=3, concat_axis=2, tiled=True)
        for part in (product[..., :total_z], product[..., total_z:])
    )
    b_next = jnp.transpose(returned, (0, 1, 3, 2))
    offset = jnp.transpose(returned_flux, (0, 1, 3, 2))
    column = (jnp.cumsum(b_next, axis=2) + offset) * total_z ** (-0.5)
    return b_next, jnp.stack([column[1], -column[0], column[2]])


def pack_rows_kernel(b_ref, r_ref, side_ref, gx_ref, up_ref, down_ref):
    cells_x, cells_z = b_ref.shape[1], b_ref.shape[2]
    near = jnp.where(gx_ref[0] == 0, 0, 1)
    up_ref[...] = jnp.zeros_like(up_ref)
    down_ref[...] = jnp.zeros_like(down_ref)
    for out, edge, inner in ((up_ref, cells_z - 1, cells_z - 2), (down_ref, 0, 1)):
        for x in range(cells_x):
            for c in range(3):
                out[pl.ds(c * cells_x + x, 1), :] = b_ref[c, x, pl.ds(edge, 1), :]
            out[pl.ds(3 * cells_x + x, 1), :] = r_ref[x, pl.ds(edge, 1), :]
            for c in range(2):
                out[pl.ds((4 + c) * cells_x + x, 1), :] = b_ref[c, x, pl.ds(inner, 1), :]
        for c in range(3):
            out[pl.ds(6 * cells_x + c, 1), :] = side_ref[2 * c + near, pl.ds(edge, 1), :]


def granule_transpose(tiles, width):
    count = len(tiles)
    index = lax.broadcasted_iota(jnp.int32, tiles[0].shape, 1) // width
    step = count // 2
    while step:
        keep = (index & step) == 0
        moved = list(tiles)
        for i in range(count):
            if i & step:
                continue
            low, high = tiles[i], tiles[i + step]
            moved[i] = jnp.where(keep, low, pltpu.roll(high, step * width, 1))
            moved[i + step] = jnp.where(keep, pltpu.roll(low, LANES - step * width, 1), high)
        tiles = moved
        step //= 2
    return tiles


def advance_kernel(b_ref, r_ref, side_ref, below_ref, above_ref, ymix_ref, gx_ref, out_ref,
                   field, eta, elec, rows, mixed):
    cells_x, cells_z, cells_y = b_ref.shape[1:]
    tall = 2 * cells_z
    first = gx_ref[0] == 0
    near = jnp.where(first, 0, 1)
    near_at = jnp.where(first, cells_x + 2, 1)
    far_at = jnp.where(first, cells_x + 3, 0)
    empty_at = jnp.where(first, 0, cells_x + 2)
    level = lax.broadcasted_iota(jnp.int32, (cells_z, cells_y), 0)
    zero = jnp.zeros((cells_z, cells_y), jnp.float32)

    def beyond(above, above2, below, below2):
        tile = jnp.where(level == 0, above, zero)
        tile = jnp.where(level == cells_z - 1, below, tile)
        if above2 is not None:
            tile = jnp.where(level == 1, above2, tile)
            tile = jnp.where(level == cells_z - 2, below2, tile)
        return tile

    def row(ref, at):
        return ref[pl.ds(at, 1), :]

    def fill(x, carry):
        for c in range(3):
            field[c, x + 2, :cells_z, :] = b_ref[c, x]
            at = c * cells_x + x
            if c < 2:
                at2 = (4 + c) * cells_x + x
                tile = beyond(row(above_ref, at), row(above_ref, at2), row(below_ref, at), row(below_ref, at2))
            else:
                tile = beyond(row(above_ref, at), None, row(below_ref, at), None)
            field[c, x + 2, cells_z:, :] = tile
        eta[x + 1, :cells_z, :] = r_ref[x]
        at = 3 * cells_x + x
        eta[x + 1, cells_z:, :] = beyond(row(above_ref, at), None, row(below_ref, at), None)
        return carry

    lax.fori_loop(0, cells_x, fill, 0)
    for c in range(3):
        field[c, near_at, :cells_z, :] = side_ref[2 * c + near]
        at = 6 * cells_x + c
        field[c, near_at, cells_z:, :] = beyond(row(above_ref, at), None, row(below_ref, at), None)
        field[c, far_at, :cells_z, :] = side_ref[2 * c + 1 - near]
        field[c, far_at, cells_z:, :] = zero
        field[c, empty_at] = jnp.zeros((tall, cells_y), jnp.float32)
        field[c, empty_at + 1] = jnp.zeros((tall, cells_y), jnp.float32)
    eta[near_at - 1, :cells_z, :] = side_ref[6 + near]
    eta[near_at - 1, cells_z:, :] = zero
    eta[jnp.where(first, 0, cells_x + 1)] = jnp.zeros((tall, cells_y), jnp.float32)

    def slope(after, before):
        return (after - before) * 0.5

    def along_z(value):
        return slope(pltpu.roll(value, tall - 1, 0), pltpu.roll(value, 1, 0))

    def along_row(value):
        return slope(pltpu.roll(value, cells_y - 1, 1), pltpu.roll(value, 1, 1))

    def electric_at(x, carry):
        here = [field[c, x + 1] for c in range(3)]
        dx = [None] + [slope(field[c, x + 2], field[c, x]) for c in (1, 2)]
        current = (
            along_row(here[2]) - along_z(here[1]),
            along_z(here[0]) - dx[2],
            dx[1] - along_row(here[0]),
        )
        made = electric_parts(current, here, eta[x])
        for c in range(3):
            elec[c, x] = made[c]
        return carry

    lax.fori_loop(0, cells_x + 2, electric_at, 0)

    def step_at(x, carry):
        here = [elec[c, x + 1] for c in range(3)]
        dx = [None] + [slope(elec[c, x + 2, :cells_z], elec[c, x, :cells_z]) for c in (1, 2)]
        inner = [value[:cells_z] for value in here]
        curl = (
            along_row(inner[2]) - along_z(here[1])[:cells_z],
            along_z(here[0])[:cells_z] - dx[2],
            dx[1] - along_row(inner[0]),
        )
        for c in range(3):
            rows[pl.ds((c * cells_x + x) * cells_z, cells_z), :] = b_ref[c, x] - time_step * curl[c]
        return carry

    lax.fori_loop(0, cells_x, step_at, 0)
    mixed[...] = jnp.dot(
        rows[...], ymix_ref[...], precision=lax.Precision.HIGHEST, preferred_element_type=jnp.float32
    )
    scatter_blocks(mixed, out_ref, cells_z)


def scatter_blocks(mixed, out_ref, cells_z):
    parts = out_ref.shape[0]
    width = mixed.shape[1] // parts
    count = LANES // width
    for group in range(mixed.shape[0] // (cells_z * count)):
        for half in range(mixed.shape[1] // LANES):
            tiles = [
                mixed[(group * count + i) * cells_z : (group * count + i + 1) * cells_z,
                      half * LANES : (half + 1) * LANES]
                for i in range(count)
            ]
            for i, tile in enumerate(granule_transpose(tiles, width)):
                out_ref[half * count + i, group * cells_z : (group + 1) * cells_z, :] = tile


def line_matrix_kernel(zmix_ref, out_ref):
    total = zmix_ref.shape[0]
    parts = out_ref.shape[0] - total
    turned = jnp.transpose(zmix_ref[...])
    slab = lax.broadcasted_iota(jnp.int32, (parts, total), 0) * (total // parts)
    lower = (lax.broadcasted_iota(jnp.int32, (parts, total), 1) < slab).astype(jnp.float32)
    out_ref[:total] = turned
    out_ref[total:] = jnp.dot(
        lower, turned, precision=lax.Precision.HIGHEST, preferred_element_type=jnp.float32
    )


def lines_kernel(cells_z, in_ref, line_ref, out_ref):
    parts, height, _ = in_ref.shape
    groups = height // cells_z
    total = parts * cells_z
    lines = jnp.concatenate(
        [in_ref[:, g * cells_z : (g + 1) * cells_z, :].reshape(total, LANES) for g in range(groups)], axis=1
    )
    product = jnp.dot(
        line_ref[...], lines, precision=lax.Precision.HIGHEST, preferred_element_type=jnp.float32
    )
    for g in range(groups):
        part = product[:, g * LANES : (g + 1) * LANES]
        out_ref[:, g * cells_z : (g + 1) * cells_z, :] = part[:total].reshape(parts, cells_z, LANES)
        for s in range(parts):
            out_ref[s, height + g : height + g + 1, :] = part[total + s : total + s + 1]


def finish_kernel(scale, in_ref, next_ref, pot_ref):
    cells_x, cells_z, cells_y = next_ref.shape[1:]
    parts = in_ref.shape[0]
    width = cells_y // parts
    count = LANES // width
    groups = 3 * cells_x // count
    level = lax.broadcasted_iota(jnp.int32, (cells_z, LANES), 0)
    for g in range(groups):
        c = g * count // cells_x
        for half in range(cells_y // LANES):
            lanes = slice(half * LANES, (half + 1) * LANES)
            tiles, columns = [], []
            for i in range(count):
                part = half * count + i
                tile = in_ref[part, g * cells_z : (g + 1) * cells_z, :]
                total, step = tile, 1
                while step < cells_z:
                    total = total + jnp.where(level >= step, pltpu.roll(total, step, 0), 0.0)
                    step *= 2
                offset = in_ref[part, groups * cells_z + g : groups * cells_z + g + 1, :]
                factor = -scale if c == 0 else scale
                tiles.append(tile)
                columns.append((total + offset) * factor)
            target = (1, 0, 2)[c]
            for i, tile in enumerate(granule_transpose(tiles, width)):
                next_ref[c, g * count + i - c * cells_x, :, lanes] = tile
            for i, tile in enumerate(granule_transpose(columns, width)):
                pot_ref[target, g * count + i - c * cells_x, :, lanes] = tile


def kernel_form(b_field, resist, ymix, zmix):
    _, cells_x, cells_z, cells_y = b_field.shape
    parts = lax.axis_size("gz")
    total_z = cells_z * parts
    f32 = jnp.float32
    gx = lax.axis_index("gx")
    place = gx.astype(jnp.int32).reshape(1)
    start = jnp.where(gx == 0, cells_x - 2, 0)
    edge = lax.dynamic_slice_in_dim(b_field, start, 2, axis=1).reshape(6, cells_z, cells_y)
    edge_r = lax.dynamic_slice_in_dim(resist, start, 2, axis=0)
    side = lax.ppermute(jnp.concatenate([edge, edge_r]), "gx", [(0, 1), (1, 0)])

    packed = -(-(6 * cells_x + 3) // SUBLANES) * SUBLANES
    slab = jax.ShapeDtypeStruct((packed, cells_y), f32)
    up, down = pl.pallas_call(
        pack_rows_kernel,
        out_shape=(slab, slab),
        in_specs=[VMEM, VMEM, VMEM, SMEM],
        out_specs=(VMEM, VMEM),
    )(b_field, resist, side, place)
    below = lax.ppermute(up, "gz", [(i, i + 1) for i in range(parts - 1)])
    above = lax.ppermute(down, "gz", [(i + 1, i) for i in range(parts - 1)])

    groups = 3 * cells_x * cells_y // parts // LANES
    height = groups * cells_z
    sent = pl.pallas_call(
        advance_kernel,
        out_shape=jax.ShapeDtypeStruct((parts, height, LANES), f32),
        in_specs=[VMEM] * 6 + [SMEM],
        out_specs=VMEM,
        scratch_shapes=[
            pltpu.VMEM((3, cells_x + 4, 2 * cells_z, cells_y), f32),
            pltpu.VMEM((cells_x + 2, 2 * cells_z, cells_y), f32),
            pltpu.VMEM((3, cells_x + 2, 2 * cells_z, cells_y), f32),
            pltpu.VMEM((3 * cells_x * cells_z, cells_y), f32),
            pltpu.VMEM((3 * cells_x * cells_z, cells_y), f32),
        ],
    )(b_field, resist, side, below, above, ymix, place)
    line = pl.pallas_call(
        line_matrix_kernel,
        out_shape=jax.ShapeDtypeStruct((total_z + parts, total_z), f32),
        in_specs=[VMEM],
        out_specs=VMEM,
    )(zmix)
    lines = lax.all_to_all(sent, "gz", split_axis=0, concat_axis=0, tiled=True)
    product = pl.pallas_call(
        functools.partial(lines_kernel, cells_z),
        out_shape=jax.ShapeDtypeStruct((parts, height + groups, LANES), f32),
        in_specs=[VMEM, VMEM],
        out_specs=VMEM,
    )(lines, line)
    returned = lax.all_to_all(product, "gz", split_axis=0, concat_axis=0, tiled=True)
    whole = jax.ShapeDtypeStruct(b_field.shape, f32)
    return pl.pallas_call(
        functools.partial(finish_kernel, total_z ** (-0.5)),
        out_shape=(whole, whole),
        in_specs=[VMEM],
        out_specs=(VMEM, VMEM),
    )(returned)


def on_device(b_field, resist, ymix, zmix):
    _, cells_x, cells_z, cells_y = b_field.shape
    parts = lax.axis_size("gz")
    width = cells_y // parts
    fits = (
        lax.axis_size("gx") == 2
        and parts > 1
        and cells_z == SUBLANES
        and cells_x >= 4
        and cells_y % LANES == 0
        and cells_y % parts == 0
        and LANES % width == 0
        and cells_x % (LANES // width) == 0
    )
    return (kernel_form if fits else plain_form)(b_field, resist, ymix, zmix)


def solution(mesh):
    in_specs = (P(None, "gx", "gz", None), P("gx", "gz", None), P(), P())
    out_specs = (P(None, "gx", "gz", None), P(None, "gx", "gz", None))
    return jax.shard_map(
        on_device, mesh=mesh, in_specs=in_specs, out_specs=out_specs, check_vma=False
    )
```

```python
import functools
import jax
import jax.numpy as jnp
from jax import lax
from jax.experimental import pallas as pl
from jax.experimental.pallas import tpu as pltpu
from jax.sharding import PartitionSpec as P

time_step = 0.1
friction = 1.0
LANES = 128
SUBLANES = 8
CHUNKS = 2
VMEM = pl.BlockSpec(memory_space=pltpu.VMEM)
SMEM = pl.BlockSpec(memory_space=pltpu.SMEM)


def with_halo(block, sides, width):
    for axis, dim in sides:
        count = lax.axis_size(axis)
        forward = [(i, i + 1) for i in range(count - 1)]
        backward = [(target, source) for source, target in forward]
        low = lax.ppermute(
            lax.slice_in_dim(block, block.shape[dim] - width, None, axis=dim), axis, forward
        )
        high = lax.ppermute(lax.slice_in_dim(block, 0, width, axis=dim), axis, backward)
        block = jnp.concatenate([low, block, high], axis=dim)
    return block


def curl_of(padded):
    centre = padded[:, 1:-1, 1:-1, :]
    grad_x = (padded[:, 2:, 1:-1, :] - padded[:, :-2, 1:-1, :]) * 0.5
    grad_z = (padded[:, 1:-1, 2:, :] - padded[:, 1:-1, :-2, :]) * 0.5
    grad_y = (jnp.roll(centre, -1, 3) - jnp.roll(centre, 1, 3)) * 0.5
    return jnp.stack([grad_y[2] - grad_z[1], grad_z[0] - grad_x[2], grad_x[1] - grad_y[0]])


def cross_parts(lhs, rhs):
    return (
        lhs[1] * rhs[2] - lhs[2] * rhs[1],
        lhs[2] * rhs[0] - lhs[0] * rhs[2],
        lhs[0] * rhs[1] - lhs[1] * rhs[0],
    )


def electric_parts(current, field, resist):
    strength = field[0] * field[0] + field[1] * field[1] + field[2] * field[2] + 1.0
    inverse = 1.0 / (friction * strength)
    velocity = [part * inverse for part in cross_parts(current, field)]
    pushed = cross_parts(velocity, field)
    return [resist * current[c] - pushed[c] for c in range(3)]


def plain_form(b_field, resist, ymix, zmix):
    cells_z = b_field.shape[2]
    total_z = cells_z * lax.axis_size("gz")
    padded = with_halo(b_field, (("gz", 2), ("gx", 1)), 1)
    efield = jnp.stack(electric_parts(curl_of(padded), b_field, resist))
    curl_e = curl_of(with_halo(efield, (("gz", 2), ("gx", 1)), 1))
    stepped = b_field - time_step * curl_e
    along_y = jnp.einsum("cxzi,ij->cxjz", stepped, ymix, precision=lax.Precision.HIGHEST)
    running = jnp.cumsum(zmix, axis=1)
    slab_ends = running[:, cells_z - 1 :: cells_z][:, :-1]
    lower_flux = jnp.concatenate([jnp.zeros((total_z, 1), jnp.float32), slab_ends], axis=1)
    line_matrix = jnp.concatenate([zmix, lower_flux], axis=1)
    product = jnp.einsum(
        "cxym,mk->cxyk",
        lax.all_to_all(along_y, "gz", split_axis=2, concat_axis=3, tiled=True),
        line_matrix,
        precision=lax.Precision.HIGHEST,
    )
    returned, returned_flux = (
        lax.all_to_all(part, "gz", split_axis=3, concat_axis=2, tiled=True)
        for part in (product[..., :total_z], product[..., total_z:])
    )
    b_next = jnp.transpose(returned, (0, 1, 3, 2))
    offset = jnp.transpose(returned_flux, (0, 1, 3, 2))
    column = (jnp.cumsum(b_next, axis=2) + offset) * total_z ** (-0.5)
    return b_next, jnp.stack([column[1], -column[0], column[2]])


def pack_rows_kernel(b_ref, r_ref, side_ref, gx_ref, up_ref, down_ref):
    cells_x, cells_z = b_ref.shape[1], b_ref.shape[2]
    near = jnp.where(gx_ref[0] == 0, 0, 1)
    up_ref[...] = jnp.zeros_like(up_ref)
    down_ref[...] = jnp.zeros_like(down_ref)
    for out, edge, inner in ((up_ref, cells_z - 1, cells_z - 2), (down_ref, 0, 1)):
        for x in range(cells_x):
            for c in range(3):
                out[pl.ds(c * cells_x + x, 1), :] = b_ref[c, x, pl.ds(edge, 1), :]
            out[pl.ds(3 * cells_x + x, 1), :] = r_ref[x, pl.ds(edge, 1), :]
            for c in range(2):
                out[pl.ds((4 + c) * cells_x + x, 1), :] = b_ref[c, x, pl.ds(inner, 1), :]
        for c in range(3):
            out[pl.ds(6 * cells_x + c, 1), :] = side_ref[2 * c + near, pl.ds(edge, 1), :]


def granule_transpose(tiles, width):
    count = len(tiles)
    index = lax.broadcasted_iota(jnp.int32, tiles[0].shape, 1) // width
    step = count // 2
    while step:
        keep = (index & step) == 0
        moved = list(tiles)
        for i in range(count):
            if i & step:
                continue
            low, high = tiles[i], tiles[i + step]
            moved[i] = jnp.where(keep, low, pltpu.roll(high, step * width, 1))
            moved[i + step] = jnp.where(keep, pltpu.roll(low, LANES - step * width, 1), high)
        tiles = moved
        step //= 2
    return tiles


def advance_kernel(b_ref, r_ref, side_ref, below_ref, above_ref, gx_ref, rows, field, eta, elec):
    cells_x, cells_z, cells_y = b_ref.shape[1:]
    tall = 2 * cells_z
    first = gx_ref[0] == 0
    near = jnp.where(first, 0, 1)
    near_at = jnp.where(first, cells_x + 2, 1)
    far_at = jnp.where(first, cells_x + 3, 0)
    empty_at = jnp.where(first, 0, cells_x + 2)
    level = lax.broadcasted_iota(jnp.int32, (cells_z, cells_y), 0)
    zero = jnp.zeros((cells_z, cells_y), jnp.float32)

    def beyond(above, above2, below, below2):
        tile = jnp.where(level == 0, above, zero)
        tile = jnp.where(level == cells_z - 1, below, tile)
        if above2 is not None:
            tile = jnp.where(level == 1, above2, tile)
            tile = jnp.where(level == cells_z - 2, below2, tile)
        return tile

    def row(ref, at):
        return ref[pl.ds(at, 1), :]

    def fill(x, carry):
        for c in range(3):
            field[c, x + 2, :cells_z, :] = b_ref[c, x]
            at = c * cells_x + x
            if c < 2:
                at2 = (4 + c) * cells_x + x
                tile = beyond(row(above_ref, at), row(above_ref, at2), row(below_ref, at), row(below_ref, at2))
            else:
                tile = beyond(row(above_ref, at), None, row(below_ref, at), None)
            field[c, x + 2, cells_z:, :] = tile
        eta[x + 1, :cells_z, :] = r_ref[x]
        at = 3 * cells_x + x
        eta[x + 1, cells_z:, :] = beyond(row(above_ref, at), None, row(below_ref, at), None)
        return carry

    lax.fori_loop(0, cells_x, fill, 0)
    for c in range(3):
        field[c, near_at, :cells_z, :] = side_ref[2 * c + near]
        at = 6 * cells_x + c
        field[c, near_at, cells_z:, :] = beyond(row(above_ref, at), None, row(below_ref, at), None)
        field[c, far_at, :cells_z, :] = side_ref[2 * c + 1 - near]
        field[c, far_at, cells_z:, :] = zero
        field[c, empty_at] = jnp.zeros((tall, cells_y), jnp.float32)
        field[c, empty_at + 1] = jnp.zeros((tall, cells_y), jnp.float32)
    eta[near_at - 1, :cells_z, :] = side_ref[6 + near]
    eta[near_at - 1, cells_z:, :] = zero
    eta[jnp.where(first, 0, cells_x + 1)] = jnp.zeros((tall, cells_y), jnp.float32)

    def slope(after, before):
        return (after - before) * 0.5

    def along_z(value):
        return slope(pltpu.roll(value, tall - 1, 0), pltpu.roll(value, 1, 0))

    def along_row(value):
        return slope(pltpu.roll(value, cells_y - 1, 1), pltpu.roll(value, 1, 1))

    def electric_at(x, carry):
        here = [field[c, x + 1] for c in range(3)]
        dx = [None] + [slope(field[c, x + 2], field[c, x]) for c in (1, 2)]
        current = (
            along_row(here[2]) - along_z(here[1]),
            along_z(here[0]) - dx[2],
            dx[1] - along_row(here[0]),
        )
        made = electric_parts(current, here, eta[x])
        for c in range(3):
            elec[c, x] = made[c]
        return carry

    lax.fori_loop(0, cells_x + 2, electric_at, 0)

    def step_at(x, carry):
        here = [elec[c, x + 1] for c in range(3)]
        dx = [None] + [slope(elec[c, x + 2, :cells_z], elec[c, x, :cells_z]) for c in (1, 2)]
        inner = [value[:cells_z] for value in here]
        curl = (
            along_row(inner[2]) - along_z(here[1])[:cells_z],
            along_z(here[0])[:cells_z] - dx[2],
            dx[1] - along_row(inner[0]),
        )
        for c in range(3):
            rows[pl.ds((c * cells_x + x) * cells_z, cells_z), :] = b_ref[c, x] - time_step * curl[c]
        return carry

    lax.fori_loop(0, cells_x, step_at, 0)


def mix_kernel(cells_z, first, rows_ref, ymix_ref, out_ref):
    parts, height, _ = out_ref.shape
    groups = height // cells_z
    cells_y = rows_ref.shape[1]
    width = cells_y // parts
    count = LANES // width
    each = count * cells_z
    mixed = jnp.dot(
        rows_ref[first * each : (first + groups) * each, :],
        ymix_ref[...],
        precision=lax.Precision.HIGHEST,
        preferred_element_type=jnp.float32,
    )
    for group in range(groups):
        for half in range(cells_y // LANES):
            lanes = slice(half * LANES, (half + 1) * LANES)
            tiles = [
                mixed[group * each + i * cells_z : group * each + (i + 1) * cells_z, lanes]
                for i in range(count)
            ]
            for i, tile in enumerate(granule_transpose(tiles, width)):
                out_ref[half * count + i, group * cells_z : (group + 1) * cells_z, :] = tile


def line_matrix_kernel(zmix_ref, out_ref):
    total = zmix_ref.shape[0]
    parts = out_ref.shape[0] - total
    turned = jnp.transpose(zmix_ref[...])
    slab = lax.broadcasted_iota(jnp.int32, (parts, total), 0) * (total // parts)
    lower = (lax.broadcasted_iota(jnp.int32, (parts, total), 1) < slab).astype(jnp.float32)
    out_ref[:total] = turned
    out_ref[total:] = jnp.dot(
        lower, turned, precision=lax.Precision.HIGHEST, preferred_element_type=jnp.float32
    )


def lines_kernel(cells_z, in_ref, line_ref, out_ref):
    parts, height, _ = in_ref.shape
    groups = height // cells_z
    total = parts * cells_z
    lines = jnp.concatenate(
        [in_ref[:, g * cells_z : (g + 1) * cells_z, :].reshape(total, LANES) for g in range(groups)], axis=1
    )
    product = jnp.dot(
        line_ref[...], lines, precision=lax.Precision.HIGHEST, preferred_element_type=jnp.float32
    )
    for g in range(groups):
        part = product[:, g * LANES : (g + 1) * LANES]
        out_ref[:, g * cells_z : (g + 1) * cells_z, :] = part[:total].reshape(parts, cells_z, LANES)
        for s in range(parts):
            out_ref[s, height + g : height + g + 1, :] = part[total + s : total + s + 1]


def finish_kernel(scale, cells_z, first, kept, *refs):
    in_ref = refs[0]
    next_ref, pot_ref, buffer, sems = refs[1 + kept :]
    _, cells_x, _, cells_y = next_ref.shape
    parts, rows, _ = in_ref.shape
    groups = rows // (cells_z + 1)
    width = cells_y // parts
    count = LANES // width
    level = lax.broadcasted_iota(jnp.int32, (cells_z, LANES), 0)
    copies = []
    for g in range(groups):
        c, x = divmod((first + g) * count, cells_x)
        for half in range(cells_y // LANES):
            lanes = slice(half * LANES, (half + 1) * LANES)
            tiles, columns = [], []
            for i in range(count):
                part = half * count + i
                tile = in_ref[part, g * cells_z : (g + 1) * cells_z, :]
                total, step = tile, 1
                while step < cells_z:
                    total = total + jnp.where(level >= step, pltpu.roll(total, step, 0), 0.0)
                    step *= 2
                offset = in_ref[part, groups * cells_z + g : groups * cells_z + g + 1, :]
                factor = -scale if c == 0 else scale
                tiles.append(tile)
                columns.append((total + offset) * factor)
            for k, made in enumerate((tiles, columns)):
                for i, tile in enumerate(granule_transpose(made, width)):
                    buffer[k, g, i, :, lanes] = tile
        for k, (target, ref) in enumerate(((c, next_ref), ((1, 0, 2)[c], pot_ref))):
            copy = pltpu.make_async_copy(
                buffer.at[k, g], ref.at[target, pl.ds(x, count)], sems.at[k, g]
            )
            copy.start()
            copies.append(copy)
    for copy in copies:
        copy.wait()


def limit(mib):
    return pltpu.CompilerParams(vmem_limit_bytes=mib * 2**20)


def kernel_form(b_field, resist, ymix, zmix):
    _, cells_x, cells_z, cells_y = b_field.shape
    parts = lax.axis_size("gz")
    total_z = cells_z * parts
    f32 = jnp.float32
    gx = lax.axis_index("gx")
    place = gx.astype(jnp.int32).reshape(1)
    start = jnp.where(gx == 0, cells_x - 2, 0)
    edge = lax.dynamic_slice_in_dim(b_field, start, 2, axis=1).reshape(6, cells_z, cells_y)
    edge_r = lax.dynamic_slice_in_dim(resist, start, 2, axis=0)
    side = lax.ppermute(jnp.concatenate([edge, edge_r]), "gx", [(0, 1), (1, 0)])

    packed = -(-(6 * cells_x + 3) // SUBLANES) * SUBLANES
    slab = jax.ShapeDtypeStruct((packed, cells_y), f32)
    up, down = pl.pallas_call(
        pack_rows_kernel,
        out_shape=(slab, slab),
        in_specs=[VMEM, VMEM, VMEM, SMEM],
        out_specs=(VMEM, VMEM),
        compiler_params=limit(6),
    )(b_field, resist, side, place)
    below = lax.ppermute(up, "gz", [(i, i + 1) for i in range(parts - 1)])
    above = lax.ppermute(down, "gz", [(i + 1, i) for i in range(parts - 1)])

    rows = pl.pallas_call(
        advance_kernel,
        out_shape=jax.ShapeDtypeStruct((3 * cells_x * cells_z, cells_y), f32),
        in_specs=[VMEM] * 5 + [SMEM],
        out_specs=VMEM,
        scratch_shapes=[
            pltpu.VMEM((3, cells_x + 4, 2 * cells_z, cells_y), f32),
            pltpu.VMEM((cells_x + 2, 2 * cells_z, cells_y), f32),
            pltpu.VMEM((3, cells_x + 2, 2 * cells_z, cells_y), f32),
        ],
        compiler_params=limit(10),
        cost_estimate=estimate(200.0 * 3 * cells_x * cells_z * cells_y),
    )(b_field, resist, side, below, above, place)
    line = pl.pallas_call(
        line_matrix_kernel,
        out_shape=jax.ShapeDtypeStruct((total_z + parts, total_z), f32),
        in_specs=[VMEM],
        out_specs=VMEM,
        compiler_params=limit(4),
    )(zmix)

    count = LANES // (cells_y // parts)
    groups = 3 * cells_x // count
    chunks = split_groups(groups)
    lines = []
    for first, size in chunks:
        sent = pl.pallas_call(
            functools.partial(mix_kernel, cells_z, first),
            out_shape=jax.ShapeDtypeStruct((parts, size * cells_z, LANES), f32),
            in_specs=[VMEM, VMEM],
            out_specs=VMEM,
            compiler_params=limit(6),
            cost_estimate=estimate(2.0 * size * count * cells_z * cells_y * cells_y),
        )(rows, ymix)
        lines.append(lax.all_to_all(sent, "gz", split_axis=0, concat_axis=0, tiled=True))
    returned = []
    for (first, size), part in zip(chunks, lines):
        product = pl.pallas_call(
            functools.partial(lines_kernel, cells_z),
            out_shape=jax.ShapeDtypeStruct((parts, size * (cells_z + 1), LANES), f32),
            in_specs=[VMEM, VMEM],
            out_specs=VMEM,
            compiler_params=limit(6),
            cost_estimate=estimate(2.0 * size * LANES * total_z * (total_z + parts)),
        )(part, line)
        returned.append(lax.all_to_all(product, "gz", split_axis=0, concat_axis=0, tiled=True))
    whole = jax.ShapeDtypeStruct(b_field.shape, f32)
    hbm = pl.BlockSpec(memory_space=pl.ANY)
    outs = ()
    for (first, size), part in zip(chunks, returned):
        outs = pl.pallas_call(
            functools.partial(finish_kernel, total_z ** (-0.5), cells_z, first, len(outs)),
            out_shape=(whole, whole),
            in_specs=[VMEM] + [hbm] * len(outs),
            out_specs=(hbm, hbm),
            scratch_shapes=[
                pltpu.VMEM((2, size, count, cells_z, cells_y), f32),
                pltpu.SemaphoreType.DMA((2, size)),
            ],
            input_output_aliases={1: 0, 2: 1} if outs else {},
            compiler_params=limit(6),
            cost_estimate=estimate(200.0 * size * count * cells_z * cells_y),
        )(part, *outs)
    return outs


def estimate(flops):
    return pl.CostEstimate(flops=int(flops), bytes_accessed=0, transcendentals=0)


def split_groups(groups):
    head = groups - groups // CHUNKS * (CHUNKS - 1)
    sizes = [head] + [groups // CHUNKS] * (CHUNKS - 1)
    return [(sum(sizes[:i]), size) for i, size in enumerate(sizes)]


def on_device(b_field, resist, ymix, zmix):
    _, cells_x, cells_z, cells_y = b_field.shape
    parts = lax.axis_size("gz")
    width = cells_y // parts
    fits = (
        lax.axis_size("gx") == 2
        and parts > 1
        and cells_z == SUBLANES
        and cells_x >= 4
        and cells_y % LANES == 0
        and cells_y % parts == 0
        and LANES % width == 0
        and cells_x % (LANES // width) == 0
    )
    return (kernel_form if fits else plain_form)(b_field, resist, ymix, zmix)


def solution(mesh):
    in_specs = (P(None, "gx", "gz", None), P("gx", "gz", None), P(), P())
    out_specs = (P(None, "gx", "gz", None), P(None, "gx", "gz", None))
    return jax.shard_map(
        on_device, mesh=mesh, in_specs=in_specs, out_specs=out_specs, check_vma=False
    )
```

```python
import functools
import jax
import jax.numpy as jnp
from jax import lax
from jax.experimental import pallas as pl
from jax.experimental.pallas import tpu as pltpu
from jax.sharding import PartitionSpec as P

time_step = 0.1
friction = 1.0
LANES = 128
SUBLANES = 8
CHUNKS = 1
VMEM = pl.BlockSpec(memory_space=pltpu.VMEM)
SMEM = pl.BlockSpec(memory_space=pltpu.SMEM)


def with_halo(block, sides, width):
    for axis, dim in sides:
        count = lax.axis_size(axis)
        forward = [(i, i + 1) for i in range(count - 1)]
        backward = [(target, source) for source, target in forward]
        low = lax.ppermute(
            lax.slice_in_dim(block, block.shape[dim] - width, None, axis=dim), axis, forward
        )
        high = lax.ppermute(lax.slice_in_dim(block, 0, width, axis=dim), axis, backward)
        block = jnp.concatenate([low, block, high], axis=dim)
    return block


def curl_of(padded):
    centre = padded[:, 1:-1, 1:-1, :]
    grad_x = (padded[:, 2:, 1:-1, :] - padded[:, :-2, 1:-1, :]) * 0.5
    grad_z = (padded[:, 1:-1, 2:, :] - padded[:, 1:-1, :-2, :]) * 0.5
    grad_y = (jnp.roll(centre, -1, 3) - jnp.roll(centre, 1, 3)) * 0.5
    return jnp.stack([grad_y[2] - grad_z[1], grad_z[0] - grad_x[2], grad_x[1] - grad_y[0]])


def cross_parts(lhs, rhs):
    return (
        lhs[1] * rhs[2] - lhs[2] * rhs[1],
        lhs[2] * rhs[0] - lhs[0] * rhs[2],
        lhs[0] * rhs[1] - lhs[1] * rhs[0],
    )


def electric_parts(current, field, resist):
    strength = field[0] * field[0] + field[1] * field[1] + field[2] * field[2] + 1.0
    inverse = 1.0 / (friction * strength)
    velocity = [part * inverse for part in cross_parts(current, field)]
    pushed = cross_parts(velocity, field)
    return [resist * current[c] - pushed[c] for c in range(3)]


def plain_form(b_field, resist, ymix, zmix):
    cells_z = b_field.shape[2]
    total_z = cells_z * lax.axis_size("gz")
    padded = with_halo(b_field, (("gz", 2), ("gx", 1)), 1)
    efield = jnp.stack(electric_parts(curl_of(padded), b_field, resist))
    curl_e = curl_of(with_halo(efield, (("gz", 2), ("gx", 1)), 1))
    stepped = b_field - time_step * curl_e
    along_y = jnp.einsum("cxzi,ij->cxjz", stepped, ymix, precision=lax.Precision.HIGHEST)
    running = jnp.cumsum(zmix, axis=1)
    slab_ends = running[:, cells_z - 1 :: cells_z][:, :-1]
    lower_flux = jnp.concatenate([jnp.zeros((total_z, 1), jnp.float32), slab_ends], axis=1)
    line_matrix = jnp.concatenate([zmix, lower_flux], axis=1)
    product = jnp.einsum(
        "cxym,mk->cxyk",
        lax.all_to_all(along_y, "gz", split_axis=2, concat_axis=3, tiled=True),
        line_matrix,
        precision=lax.Precision.HIGHEST,
    )
    returned, returned_flux = (
        lax.all_to_all(part, "gz", split_axis=3, concat_axis=2, tiled=True)
        for part in (product[..., :total_z], product[..., total_z:])
    )
    b_next = jnp.transpose(returned, (0, 1, 3, 2))
    offset = jnp.transpose(returned_flux, (0, 1, 3, 2))
    column = (jnp.cumsum(b_next, axis=2) + offset) * total_z ** (-0.5)
    return b_next, jnp.stack([column[1], -column[0], column[2]])


def pack_rows_kernel(b_ref, r_ref, side_ref, gx_ref, up_ref, down_ref):
    cells_x, cells_z = b_ref.shape[1], b_ref.shape[2]
    near = jnp.where(gx_ref[0] == 0, 0, 1)
    up_ref[...] = jnp.zeros_like(up_ref)
    down_ref[...] = jnp.zeros_like(down_ref)
    for out, edge, inner in ((up_ref, cells_z - 1, cells_z - 2), (down_ref, 0, 1)):
        for x in range(cells_x):
            for c in range(3):
                out[pl.ds(c * cells_x + x, 1), :] = b_ref[c, x, pl.ds(edge, 1), :]
            out[pl.ds(3 * cells_x + x, 1), :] = r_ref[x, pl.ds(edge, 1), :]
            for c in range(2):
                out[pl.ds((4 + c) * cells_x + x, 1), :] = b_ref[c, x, pl.ds(inner, 1), :]
        for c in range(3):
            out[pl.ds(6 * cells_x + c, 1), :] = side_ref[2 * c + near, pl.ds(edge, 1), :]


def granule_transpose(tiles, width):
    count = len(tiles)
    index = lax.broadcasted_iota(jnp.int32, tiles[0].shape, 1) // width
    step = count // 2
    while step:
        keep = (index & step) == 0
        moved = list(tiles)
        for i in range(count):
            if i & step:
                continue
            low, high = tiles[i], tiles[i + step]
            moved[i] = jnp.where(keep, low, pltpu.roll(high, step * width, 1))
            moved[i + step] = jnp.where(keep, pltpu.roll(low, LANES - step * width, 1), high)
        tiles = moved
        step //= 2
    return tiles


def advance_kernel(b_ref, r_ref, side_ref, below_ref, above_ref, gx_ref, rows, field, eta, elec):
    cells_x, cells_z, cells_y = b_ref.shape[1:]
    tall = 2 * cells_z
    first = gx_ref[0] == 0
    near = jnp.where(first, 0, 1)
    near_at = jnp.where(first, cells_x + 2, 1)
    far_at = jnp.where(first, cells_x + 3, 0)
    empty_at = jnp.where(first, 0, cells_x + 2)
    level = lax.broadcasted_iota(jnp.int32, (cells_z, cells_y), 0)
    zero = jnp.zeros((cells_z, cells_y), jnp.float32)

    def beyond(above, above2, below, below2):
        tile = jnp.where(level == 0, above, zero)
        tile = jnp.where(level == cells_z - 1, below, tile)
        if above2 is not None:
            tile = jnp.where(level == 1, above2, tile)
            tile = jnp.where(level == cells_z - 2, below2, tile)
        return tile

    def row(ref, at):
        return ref[pl.ds(at, 1), :]

    def fill(x, carry):
        for c in range(3):
            field[c, x + 2, :cells_z, :] = b_ref[c, x]
            at = c * cells_x + x
            if c < 2:
                at2 = (4 + c) * cells_x + x
                tile = beyond(row(above_ref, at), row(above_ref, at2), row(below_ref, at), row(below_ref, at2))
            else:
                tile = beyond(row(above_ref, at), None, row(below_ref, at), None)
            field[c, x + 2, cells_z:, :] = tile
        eta[x + 1, :cells_z, :] = r_ref[x]
        at = 3 * cells_x + x
        eta[x + 1, cells_z:, :] = beyond(row(above_ref, at), None, row(below_ref, at), None)
        return carry

    lax.fori_loop(0, cells_x, fill, 0)
    for c in range(3):
        field[c, near_at, :cells_z, :] = side_ref[2 * c + near]
        at = 6 * cells_x + c
        field[c, near_at, cells_z:, :] = beyond(row(above_ref, at), None, row(below_ref, at), None)
        field[c, far_at, :cells_z, :] = side_ref[2 * c + 1 - near]
        field[c, far_at, cells_z:, :] = zero
        field[c, empty_at] = jnp.zeros((tall, cells_y), jnp.float32)
        field[c, empty_at + 1] = jnp.zeros((tall, cells_y), jnp.float32)
    eta[near_at - 1, :cells_z, :] = side_ref[6 + near]
    eta[near_at - 1, cells_z:, :] = zero
    eta[jnp.where(first, 0, cells_x + 1)] = jnp.zeros((tall, cells_y), jnp.float32)

    def slope(after, before):
        return (after - before) * 0.5

    def along_z(value):
        return slope(pltpu.roll(value, tall - 1, 0), pltpu.roll(value, 1, 0))

    def along_row(value):
        return slope(pltpu.roll(value, cells_y - 1, 1), pltpu.roll(value, 1, 1))

    def electric_at(x, carry):
        here = [field[c, x + 1] for c in range(3)]
        dx = [None] + [slope(field[c, x + 2], field[c, x]) for c in (1, 2)]
        current = (
            along_row(here[2]) - along_z(here[1]),
            along_z(here[0]) - dx[2],
            dx[1] - along_row(here[0]),
        )
        made = electric_parts(current, here, eta[x])
        for c in range(3):
            elec[c, x] = made[c]
        return carry

    lax.fori_loop(0, cells_x + 2, electric_at, 0)

    def step_at(x, carry):
        here = [elec[c, x + 1] for c in range(3)]
        dx = [None] + [slope(elec[c, x + 2, :cells_z], elec[c, x, :cells_z]) for c in (1, 2)]
        inner = [value[:cells_z] for value in here]
        curl = (
            along_row(inner[2]) - along_z(here[1])[:cells_z],
            along_z(here[0])[:cells_z] - dx[2],
            dx[1] - along_row(inner[0]),
        )
        for c in range(3):
            rows[pl.ds((c * cells_x + x) * cells_z, cells_z), :] = b_ref[c, x] - time_step * curl[c]
        return carry

    lax.fori_loop(0, cells_x, step_at, 0)


def mix_kernel(cells_z, first, rows_ref, ymix_ref, out_ref):
    parts, height, _ = out_ref.shape
    groups = height // cells_z
    cells_y = rows_ref.shape[1]
    width = cells_y // parts
    count = LANES // width
    each = count * cells_z
    mixed = jnp.dot(
        rows_ref[first * each : (first + groups) * each, :],
        ymix_ref[...],
        precision=lax.Precision.HIGHEST,
        preferred_element_type=jnp.float32,
    )
    for group in range(groups):
        for half in range(cells_y // LANES):
            lanes = slice(half * LANES, (half + 1) * LANES)
            tiles = [
                mixed[group * each + i * cells_z : group * each + (i + 1) * cells_z, lanes]
                for i in range(count)
            ]
            for i, tile in enumerate(granule_transpose(tiles, width)):
                out_ref[half * count + i, group * cells_z : (group + 1) * cells_z, :] = tile


def line_matrix_kernel(zmix_ref, out_ref):
    total = zmix_ref.shape[0]
    parts = out_ref.shape[0] - total
    turned = jnp.transpose(zmix_ref[...])
    slab = lax.broadcasted_iota(jnp.int32, (parts, total), 0) * (total // parts)
    lower = (lax.broadcasted_iota(jnp.int32, (parts, total), 1) < slab).astype(jnp.float32)
    out_ref[:total] = turned
    out_ref[total:] = jnp.dot(
        lower, turned, precision=lax.Precision.HIGHEST, preferred_element_type=jnp.float32
    )


def lines_kernel(cells_z, in_ref, line_ref, out_ref):
    parts, height, _ = in_ref.shape
    groups = height // cells_z
    total = parts * cells_z
    lines = jnp.concatenate(
        [in_ref[:, g * cells_z : (g + 1) * cells_z, :].reshape(total, LANES) for g in range(groups)], axis=1
    )
    product = jnp.dot(
        line_ref[...], lines, precision=lax.Precision.HIGHEST, preferred_element_type=jnp.float32
    )
    for g in range(groups):
        part = product[:, g * LANES : (g + 1) * LANES]
        out_ref[:, g * cells_z : (g + 1) * cells_z, :] = part[:total].reshape(parts, cells_z, LANES)
        for s in range(parts):
            out_ref[s, height + g : height + g + 1, :] = part[total + s : total + s + 1]


def finish_kernel(scale, cells_z, first, kept, *refs):
    in_ref = refs[0]
    next_ref, pot_ref, buffer, sems = refs[1 + kept :]
    _, cells_x, _, cells_y = next_ref.shape
    parts, rows, _ = in_ref.shape
    groups = rows // (cells_z + 1)
    width = cells_y // parts
    count = LANES // width
    level = lax.broadcasted_iota(jnp.int32, (cells_z, LANES), 0)
    copies = []
    for g in range(groups):
        c, x = divmod((first + g) * count, cells_x)
        for half in range(cells_y // LANES):
            lanes = slice(half * LANES, (half + 1) * LANES)
            tiles, columns = [], []
            for i in range(count):
                part = half * count + i
                tile = in_ref[part, g * cells_z : (g + 1) * cells_z, :]
                total, step = tile, 1
                while step < cells_z:
                    total = total + jnp.where(level >= step, pltpu.roll(total, step, 0), 0.0)
                    step *= 2
                offset = in_ref[part, groups * cells_z + g : groups * cells_z + g + 1, :]
                factor = -scale if c == 0 else scale
                tiles.append(tile)
                columns.append((total + offset) * factor)
            for k, made in enumerate((tiles, columns)):
                for i, tile in enumerate(granule_transpose(made, width)):
                    buffer[k, g, i, :, lanes] = tile
        for k, (target, ref) in enumerate(((c, next_ref), ((1, 0, 2)[c], pot_ref))):
            copy = pltpu.make_async_copy(
                buffer.at[k, g], ref.at[target, pl.ds(x, count)], sems.at[k, g]
            )
            copy.start()
            copies.append(copy)
    for copy in copies:
        copy.wait()


def limit(mib):
    return pltpu.CompilerParams(vmem_limit_bytes=mib * 2**20)


def kernel_form(b_field, resist, ymix, zmix):
    _, cells_x, cells_z, cells_y = b_field.shape
    parts = lax.axis_size("gz")
    total_z = cells_z * parts
    f32 = jnp.float32
    gx = lax.axis_index("gx")
    place = gx.astype(jnp.int32).reshape(1)
    start = jnp.where(gx == 0, cells_x - 2, 0)
    edge = lax.dynamic_slice_in_dim(b_field, start, 2, axis=1).reshape(6, cells_z, cells_y)
    edge_r = lax.dynamic_slice_in_dim(resist, start, 2, axis=0)
    side = lax.ppermute(jnp.concatenate([edge, edge_r]), "gx", [(0, 1), (1, 0)])

    packed = -(-(6 * cells_x + 3) // SUBLANES) * SUBLANES
    slab = jax.ShapeDtypeStruct((packed, cells_y), f32)
    up, down = pl.pallas_call(
        pack_rows_kernel,
        out_shape=(slab, slab),
        in_specs=[VMEM, VMEM, VMEM, SMEM],
        out_specs=(VMEM, VMEM),
        compiler_params=limit(6),
    )(b_field, resist, side, place)
    below = lax.ppermute(up, "gz", [(i, i + 1) for i in range(parts - 1)])
    above = lax.ppermute(down, "gz", [(i + 1, i) for i in range(parts - 1)])

    rows = pl.pallas_call(
        advance_kernel,
        out_shape=jax.ShapeDtypeStruct((3 * cells_x * cells_z, cells_y), f32),
        in_specs=[VMEM] * 5 + [SMEM],
        out_specs=VMEM,
        scratch_shapes=[
            pltpu.VMEM((3, cells_x + 4, 2 * cells_z, cells_y), f32),
            pltpu.VMEM((cells_x + 2, 2 * cells_z, cells_y), f32),
            pltpu.VMEM((3, cells_x + 2, 2 * cells_z, cells_y), f32),
        ],
        compiler_params=limit(10),
        cost_estimate=estimate(200.0 * 3 * cells_x * cells_z * cells_y),
    )(b_field, resist, side, below, above, place)
    line = pl.pallas_call(
        line_matrix_kernel,
        out_shape=jax.ShapeDtypeStruct((total_z + parts, total_z), f32),
        in_specs=[VMEM],
        out_specs=VMEM,
        compiler_params=limit(4),
    )(zmix)

    count = LANES // (cells_y // parts)
    groups = 3 * cells_x // count
    chunks = split_groups(groups)
    lines = []
    for first, size in chunks:
        sent = pl.pallas_call(
            functools.partial(mix_kernel, cells_z, first),
            out_shape=jax.ShapeDtypeStruct((parts, size * cells_z, LANES), f32),
            in_specs=[VMEM, VMEM],
            out_specs=VMEM,
            compiler_params=limit(6),
            cost_estimate=estimate(2.0 * size * count * cells_z * cells_y * cells_y),
        )(rows, ymix)
        lines.append(lax.all_to_all(sent, "gz", split_axis=0, concat_axis=0, tiled=True))
    returned = []
    for (first, size), part in zip(chunks, lines):
        product = pl.pallas_call(
            functools.partial(lines_kernel, cells_z),
            out_shape=jax.ShapeDtypeStruct((parts, size * (cells_z + 1), LANES), f32),
            in_specs=[VMEM, VMEM],
            out_specs=VMEM,
            compiler_params=limit(6),
            cost_estimate=estimate(2.0 * size * LANES * total_z * (total_z + parts)),
        )(part, line)
        returned.append(lax.all_to_all(product, "gz", split_axis=0, concat_axis=0, tiled=True))
    whole = jax.ShapeDtypeStruct(b_field.shape, f32)
    hbm = pl.BlockSpec(memory_space=pl.ANY)
    outs = ()
    for (first, size), part in zip(chunks, returned):
        outs = pl.pallas_call(
            functools.partial(finish_kernel, total_z ** (-0.5), cells_z, first, len(outs)),
            out_shape=(whole, whole),
            in_specs=[VMEM] + [hbm] * len(outs),
            out_specs=(hbm, hbm),
            scratch_shapes=[
                pltpu.VMEM((2, size, count, cells_z, cells_y), f32),
                pltpu.SemaphoreType.DMA((2, size)),
            ],
            input_output_aliases={1: 0, 2: 1} if outs else {},
            compiler_params=limit(6),
            cost_estimate=estimate(200.0 * size * count * cells_z * cells_y),
        )(part, *outs)
    return outs


def estimate(flops):
    return pl.CostEstimate(flops=int(flops), bytes_accessed=0, transcendentals=0)


def split_groups(groups):
    head = groups - groups // CHUNKS * (CHUNKS - 1)
    sizes = [head] + [groups // CHUNKS] * (CHUNKS - 1)
    return [(sum(sizes[:i]), size) for i, size in enumerate(sizes)]


def on_device(b_field, resist, ymix, zmix):
    _, cells_x, cells_z, cells_y = b_field.shape
    parts = lax.axis_size("gz")
    width = cells_y // parts
    fits = (
        lax.axis_size("gx") == 2
        and parts > 1
        and cells_z == SUBLANES
        and cells_x >= 4
        and cells_y % LANES == 0
        and cells_y % parts == 0
        and LANES % width == 0
        and cells_x % (LANES // width) == 0
    )
    return (kernel_form if fits else plain_form)(b_field, resist, ymix, zmix)


def solution(mesh):
    in_specs = (P(None, "gx", "gz", None), P("gx", "gz", None), P(), P())
    out_specs = (P(None, "gx", "gz", None), P(None, "gx", "gz", None))
    return jax.shard_map(
        on_device, mesh=mesh, in_specs=in_specs, out_specs=out_specs, check_vma=False
    )
```

```python
import functools
import jax
import jax.numpy as jnp
from jax import lax
from jax.experimental import pallas as pl
from jax.experimental.pallas import tpu as pltpu
from jax.sharding import PartitionSpec as P

time_step = 0.1
friction = 1.0
LANES = 128
SUBLANES = 8
PIECES = 3
VMEM = pl.BlockSpec(memory_space=pltpu.VMEM)
SMEM = pl.BlockSpec(memory_space=pltpu.SMEM)


def with_halo(block, sides, width):
    for axis, dim in sides:
        count = lax.axis_size(axis)
        forward = [(i, i + 1) for i in range(count - 1)]
        backward = [(target, source) for source, target in forward]
        low = lax.ppermute(
            lax.slice_in_dim(block, block.shape[dim] - width, None, axis=dim), axis, forward
        )
        high = lax.ppermute(lax.slice_in_dim(block, 0, width, axis=dim), axis, backward)
        block = jnp.concatenate([low, block, high], axis=dim)
    return block


def curl_of(padded):
    centre = padded[:, 1:-1, 1:-1, :]
    grad_x = (padded[:, 2:, 1:-1, :] - padded[:, :-2, 1:-1, :]) * 0.5
    grad_z = (padded[:, 1:-1, 2:, :] - padded[:, 1:-1, :-2, :]) * 0.5
    grad_y = (jnp.roll(centre, -1, 3) - jnp.roll(centre, 1, 3)) * 0.5
    return jnp.stack([grad_y[2] - grad_z[1], grad_z[0] - grad_x[2], grad_x[1] - grad_y[0]])


def cross_parts(lhs, rhs):
    return (
        lhs[1] * rhs[2] - lhs[2] * rhs[1],
        lhs[2] * rhs[0] - lhs[0] * rhs[2],
        lhs[0] * rhs[1] - lhs[1] * rhs[0],
    )


def electric_parts(current, field, resist):
    strength = field[0] * field[0] + field[1] * field[1] + field[2] * field[2] + 1.0
    inverse = 1.0 / (friction * strength)
    velocity = [part * inverse for part in cross_parts(current, field)]
    pushed = cross_parts(velocity, field)
    return [resist * current[c] - pushed[c] for c in range(3)]


def plain_form(b_field, resist, ymix, zmix):
    cells_z = b_field.shape[2]
    total_z = cells_z * lax.axis_size("gz")
    padded = with_halo(b_field, (("gz", 2), ("gx", 1)), 1)
    efield = jnp.stack(electric_parts(curl_of(padded), b_field, resist))
    curl_e = curl_of(with_halo(efield, (("gz", 2), ("gx", 1)), 1))
    stepped = b_field - time_step * curl_e
    along_y = jnp.einsum("cxzi,ij->cxjz", stepped, ymix, precision=lax.Precision.HIGHEST)
    running = jnp.cumsum(zmix, axis=1)
    slab_ends = running[:, cells_z - 1 :: cells_z][:, :-1]
    lower_flux = jnp.concatenate([jnp.zeros((total_z, 1), jnp.float32), slab_ends], axis=1)
    line_matrix = jnp.concatenate([zmix, lower_flux], axis=1)
    product = jnp.einsum(
        "cxym,mk->cxyk",
        lax.all_to_all(along_y, "gz", split_axis=2, concat_axis=3, tiled=True),
        line_matrix,
        precision=lax.Precision.HIGHEST,
    )
    returned, returned_flux = (
        lax.all_to_all(part, "gz", split_axis=3, concat_axis=2, tiled=True)
        for part in (product[..., :total_z], product[..., total_z:])
    )
    b_next = jnp.transpose(returned, (0, 1, 3, 2))
    offset = jnp.transpose(returned_flux, (0, 1, 3, 2))
    column = (jnp.cumsum(b_next, axis=2) + offset) * total_z ** (-0.5)
    return b_next, jnp.stack([column[1], -column[0], column[2]])


def pack_rows_kernel(b_ref, r_ref, side_ref, gx_ref, up_ref, down_ref):
    cells_x, cells_z = b_ref.shape[1], b_ref.shape[2]
    near = jnp.where(gx_ref[0] == 0, 0, 1)
    up_ref[...] = jnp.zeros_like(up_ref)
    down_ref[...] = jnp.zeros_like(down_ref)
    for out, edge, inner in ((up_ref, cells_z - 1, cells_z - 2), (down_ref, 0, 1)):
        for x in range(cells_x):
            for c in range(3):
                out[pl.ds(c * cells_x + x, 1), :] = b_ref[c, x, pl.ds(edge, 1), :]
            out[pl.ds(3 * cells_x + x, 1), :] = r_ref[x, pl.ds(edge, 1), :]
            for c in range(2):
                out[pl.ds((4 + c) * cells_x + x, 1), :] = b_ref[c, x, pl.ds(inner, 1), :]
        for c in range(3):
            out[pl.ds(6 * cells_x + c, 1), :] = side_ref[2 * c + near, pl.ds(edge, 1), :]


def advance_kernel(b_ref, r_ref, side_ref, below_ref, above_ref, gx_ref, rows, field, eta, elec):
    cells_x, cells_z, cells_y = b_ref.shape[1:]
    tall = 2 * cells_z
    first = gx_ref[0] == 0
    near = jnp.where(first, 0, 1)
    near_at = jnp.where(first, cells_x + 2, 1)
    far_at = jnp.where(first, cells_x + 3, 0)
    empty_at = jnp.where(first, 0, cells_x + 2)
    level = lax.broadcasted_iota(jnp.int32, (cells_z, cells_y), 0)
    zero = jnp.zeros((cells_z, cells_y), jnp.float32)

    def beyond(above, above2, below, below2):
        tile = jnp.where(level == 0, above, zero)
        tile = jnp.where(level == cells_z - 1, below, tile)
        if above2 is not None:
            tile = jnp.where(level == 1, above2, tile)
            tile = jnp.where(level == cells_z - 2, below2, tile)
        return tile

    def row(ref, at):
        return ref[pl.ds(at, 1), :]

    def fill(x, carry):
        for c in range(3):
            field[c, x + 2, :cells_z, :] = b_ref[c, x]
            at = c * cells_x + x
            if c < 2:
                at2 = (4 + c) * cells_x + x
                tile = beyond(row(above_ref, at), row(above_ref, at2), row(below_ref, at), row(below_ref, at2))
            else:
                tile = beyond(row(above_ref, at), None, row(below_ref, at), None)
            field[c, x + 2, cells_z:, :] = tile
        eta[x + 1, :cells_z, :] = r_ref[x]
        at = 3 * cells_x + x
        eta[x + 1, cells_z:, :] = beyond(row(above_ref, at), None, row(below_ref, at), None)
        return carry

    lax.fori_loop(0, cells_x, fill, 0)
    for c in range(3):
        field[c, near_at, :cells_z, :] = side_ref[2 * c + near]
        at = 6 * cells_x + c
        field[c, near_at, cells_z:, :] = beyond(row(above_ref, at), None, row(below_ref, at), None)
        field[c, far_at, :cells_z, :] = side_ref[2 * c + 1 - near]
        field[c, far_at, cells_z:, :] = zero
        field[c, empty_at] = jnp.zeros((tall, cells_y), jnp.float32)
        field[c, empty_at + 1] = jnp.zeros((tall, cells_y), jnp.float32)
    eta[near_at - 1, :cells_z, :] = side_ref[6 + near]
    eta[near_at - 1, cells_z:, :] = zero
    eta[jnp.where(first, 0, cells_x + 1)] = jnp.zeros((tall, cells_y), jnp.float32)

    def slope(after, before):
        return (after - before) * 0.5

    def along_z(value):
        return slope(pltpu.roll(value, tall - 1, 0), pltpu.roll(value, 1, 0))

    def along_row(value):
        return slope(pltpu.roll(value, cells_y - 1, 1), pltpu.roll(value, 1, 1))

    def electric_at(x, carry):
        here = [field[c, x + 1] for c in range(3)]
        dx = [None] + [slope(field[c, x + 2], field[c, x]) for c in (1, 2)]
        current = (
            along_row(here[2]) - along_z(here[1]),
            along_z(here[0]) - dx[2],
            dx[1] - along_row(here[0]),
        )
        made = electric_parts(current, here, eta[x])
        for c in range(3):
            elec[c, x] = made[c]
        return carry

    lax.fori_loop(0, cells_x + 2, electric_at, 0)

    def step_at(x, carry):
        here = [elec[c, x + 1] for c in range(3)]
        dx = [None] + [slope(elec[c, x + 2, :cells_z], elec[c, x, :cells_z]) for c in (1, 2)]
        inner = [value[:cells_z] for value in here]
        curl = (
            along_row(inner[2]) - along_z(here[1])[:cells_z],
            along_z(here[0])[:cells_z] - dx[2],
            dx[1] - along_row(inner[0]),
        )
        for c in range(3):
            rows[pl.ds((c * cells_x + x) * cells_z, cells_z), :] = b_ref[c, x] - time_step * curl[c]
        return carry

    lax.fori_loop(0, cells_x, step_at, 0)


def mix_kernel(cells_z, rows_ref, ymix_ref, out_ref):
    parts, height, _ = out_ref.shape
    each = height // cells_z
    halves = rows_ref.shape[1] // LANES
    mixed = jnp.dot(
        rows_ref[...],
        ymix_ref[...],
        precision=lax.Precision.HIGHEST,
        preferred_element_type=jnp.float32,
    )
    for tile in range(parts * each):
        (part, at), (line, half) = divmod(tile, each), divmod(tile, halves)
        out_ref[part, at * cells_z : (at + 1) * cells_z, :] = mixed[
            line * cells_z : (line + 1) * cells_z, half * LANES : (half + 1) * LANES
        ]


def line_matrix_kernel(zmix_ref, out_ref):
    total = zmix_ref.shape[0]
    parts = out_ref.shape[0] - total
    turned = jnp.transpose(zmix_ref[...])
    slab = lax.broadcasted_iota(jnp.int32, (parts, total), 0) * (total // parts)
    lower = (lax.broadcasted_iota(jnp.int32, (parts, total), 1) < slab).astype(jnp.float32)
    out_ref[:total] = turned
    out_ref[total:] = jnp.dot(
        lower, turned, precision=lax.Precision.HIGHEST, preferred_element_type=jnp.float32
    )


def lines_kernel(cells_z, in_ref, line_ref, out_ref):
    parts, height, _ = in_ref.shape
    groups = height // cells_z
    total = parts * cells_z
    lines = jnp.concatenate(
        [in_ref[:, g * cells_z : (g + 1) * cells_z, :].reshape(total, LANES) for g in range(groups)], axis=1
    )
    product = jnp.dot(
        line_ref[...], lines, precision=lax.Precision.HIGHEST, preferred_element_type=jnp.float32
    )
    for g in range(groups):
        part = product[:, g * LANES : (g + 1) * LANES]
        out_ref[:, g * cells_z : (g + 1) * cells_z, :] = part[:total].reshape(parts, cells_z, LANES)
        for s in range(parts):
            out_ref[s, height + g : height + g + 1, :] = part[total + s : total + s + 1]


def finish_kernel(scale, cells_z, in_ref, next_ref, pot_ref, buffer, sems):
    _, cells_x, _, cells_y = next_ref.shape
    each = in_ref.shape[1] // (cells_z + 1)
    halves = cells_y // LANES
    batch = cells_x // PIECES
    level = lax.broadcasted_iota(jnp.int32, (cells_z, LANES), 0)
    copies = []
    for piece in range(3 * PIECES):
        c, x = divmod(piece * batch, cells_x)
        factor = -scale if c == 0 else scale
        for i in range(batch):
            for half in range(halves):
                part, at = divmod((piece * batch + i) * halves + half, each)
                tile = in_ref[part, at * cells_z : (at + 1) * cells_z, :]
                total, step = tile, 1
                while step < cells_z:
                    total = total + jnp.where(level >= step, pltpu.roll(total, step, 0), 0.0)
                    step *= 2
                offset = in_ref[part, each * cells_z + at : each * cells_z + at + 1, :]
                lanes = slice(half * LANES, (half + 1) * LANES)
                buffer[0, piece, i, :, lanes] = tile
                buffer[1, piece, i, :, lanes] = (total + offset) * factor
        for k, (target, ref) in enumerate(((c, next_ref), ((1, 0, 2)[c], pot_ref))):
            copy = pltpu.make_async_copy(
                buffer.at[k, piece], ref.at[target, pl.ds(x, batch)], sems.at[k, piece]
            )
            copy.start()
            copies.append(copy)
    for copy in copies:
        copy.wait()


def limit(mib):
    return pltpu.CompilerParams(vmem_limit_bytes=mib * 2**20)


def kernel_form(b_field, resist, ymix, zmix):
    _, cells_x, cells_z, cells_y = b_field.shape
    parts = lax.axis_size("gz")
    total_z = cells_z * parts
    f32 = jnp.float32
    gx = lax.axis_index("gx")
    place = gx.astype(jnp.int32).reshape(1)
    start = jnp.where(gx == 0, cells_x - 2, 0)
    edge = lax.dynamic_slice_in_dim(b_field, start, 2, axis=1).reshape(6, cells_z, cells_y)
    edge_r = lax.dynamic_slice_in_dim(resist, start, 2, axis=0)
    side = lax.ppermute(jnp.concatenate([edge, edge_r]), "gx", [(0, 1), (1, 0)])

    packed = -(-(6 * cells_x + 3) // SUBLANES) * SUBLANES
    slab = jax.ShapeDtypeStruct((packed, cells_y), f32)
    up, down = pl.pallas_call(
        pack_rows_kernel,
        out_shape=(slab, slab),
        in_specs=[VMEM, VMEM, VMEM, SMEM],
        out_specs=(VMEM, VMEM),
        compiler_params=limit(6),
    )(b_field, resist, side, place)
    below = lax.ppermute(up, "gz", [(i, i + 1) for i in range(parts - 1)])
    above = lax.ppermute(down, "gz", [(i + 1, i) for i in range(parts - 1)])

    rows = pl.pallas_call(
        advance_kernel,
        out_shape=jax.ShapeDtypeStruct((3 * cells_x * cells_z, cells_y), f32),
        in_specs=[VMEM] * 5 + [SMEM],
        out_specs=VMEM,
        scratch_shapes=[
            pltpu.VMEM((3, cells_x + 4, 2 * cells_z, cells_y), f32),
            pltpu.VMEM((cells_x + 2, 2 * cells_z, cells_y), f32),
            pltpu.VMEM((3, cells_x + 2, 2 * cells_z, cells_y), f32),
        ],
        compiler_params=limit(10),
        cost_estimate=estimate(200.0 * 3 * cells_x * cells_z * cells_y),
    )(b_field, resist, side, below, above, place)
    line = pl.pallas_call(
        line_matrix_kernel,
        out_shape=jax.ShapeDtypeStruct((total_z + parts, total_z), f32),
        in_specs=[VMEM],
        out_specs=VMEM,
        compiler_params=limit(4),
    )(zmix)

    each = 3 * cells_x * (cells_y // LANES) // parts
    sent = pl.pallas_call(
        functools.partial(mix_kernel, cells_z),
        out_shape=jax.ShapeDtypeStruct((parts, each * cells_z, LANES), f32),
        in_specs=[VMEM, VMEM],
        out_specs=VMEM,
        compiler_params=limit(6),
    )(rows, ymix)
    lines = lax.all_to_all(sent, "gz", split_axis=0, concat_axis=0, tiled=True)
    product = pl.pallas_call(
        functools.partial(lines_kernel, cells_z),
        out_shape=jax.ShapeDtypeStruct((parts, each * (cells_z + 1), LANES), f32),
        in_specs=[VMEM, VMEM],
        out_specs=VMEM,
        compiler_params=limit(6),
    )(lines, line)
    returned = lax.all_to_all(product, "gz", split_axis=0, concat_axis=0, tiled=True)
    whole = jax.ShapeDtypeStruct(b_field.shape, f32)
    hbm = pl.BlockSpec(memory_space=pl.ANY)
    return pl.pallas_call(
        functools.partial(finish_kernel, total_z ** (-0.5), cells_z),
        out_shape=(whole, whole),
        in_specs=[VMEM],
        out_specs=(hbm, hbm),
        scratch_shapes=[
            pltpu.VMEM((2, 3 * PIECES, cells_x // PIECES, cells_z, cells_y), f32),
            pltpu.SemaphoreType.DMA((2, 3 * PIECES)),
        ],
        compiler_params=limit(6),
    )(returned)


def estimate(flops):
    return pl.CostEstimate(flops=int(flops), bytes_accessed=0, transcendentals=0)


def on_device(b_field, resist, ymix, zmix):
    _, cells_x, cells_z, cells_y = b_field.shape
    parts = lax.axis_size("gz")
    fits = (
        lax.axis_size("gx") == 2
        and parts > 1
        and cells_z == SUBLANES
        and cells_x % PIECES == 0
        and cells_y % LANES == 0
        and 3 * cells_x * (cells_y // LANES) % parts == 0
    )
    return (kernel_form if fits else plain_form)(b_field, resist, ymix, zmix)


def solution(mesh):
    in_specs = (P(None, "gx", "gz", None), P("gx", "gz", None), P(), P())
    out_specs = (P(None, "gx", "gz", None), P(None, "gx", "gz", None))
    return jax.shard_map(
        on_device, mesh=mesh, in_specs=in_specs, out_specs=out_specs, check_vma=False
    )
```

```python
import functools
import jax
import jax.numpy as jnp
from jax import lax
from jax.experimental import pallas as pl
from jax.experimental.pallas import tpu as pltpu
from jax.sharding import PartitionSpec as P

time_step = 0.1
friction = 1.0
LANES = 128
SUBLANES = 8
PIECES = 3
BATCH = 6
VMEM = pl.BlockSpec(memory_space=pltpu.VMEM)
SMEM = pl.BlockSpec(memory_space=pltpu.SMEM)


def with_halo(block, sides, width):
    for axis, dim in sides:
        count = lax.axis_size(axis)
        forward = [(i, i + 1) for i in range(count - 1)]
        backward = [(target, source) for source, target in forward]
        low = lax.ppermute(
            lax.slice_in_dim(block, block.shape[dim] - width, None, axis=dim), axis, forward
        )
        high = lax.ppermute(lax.slice_in_dim(block, 0, width, axis=dim), axis, backward)
        block = jnp.concatenate([low, block, high], axis=dim)
    return block


def curl_of(padded):
    centre = padded[:, 1:-1, 1:-1, :]
    grad_x = (padded[:, 2:, 1:-1, :] - padded[:, :-2, 1:-1, :]) * 0.5
    grad_z = (padded[:, 1:-1, 2:, :] - padded[:, 1:-1, :-2, :]) * 0.5
    grad_y = (jnp.roll(centre, -1, 3) - jnp.roll(centre, 1, 3)) * 0.5
    return jnp.stack([grad_y[2] - grad_z[1], grad_z[0] - grad_x[2], grad_x[1] - grad_y[0]])


def cross_parts(lhs, rhs):
    return (
        lhs[1] * rhs[2] - lhs[2] * rhs[1],
        lhs[2] * rhs[0] - lhs[0] * rhs[2],
        lhs[0] * rhs[1] - lhs[1] * rhs[0],
    )


def electric_parts(current, field, resist):
    strength = field[0] * field[0] + field[1] * field[1] + field[2] * field[2] + 1.0
    inverse = 1.0 / (friction * strength)
    velocity = [part * inverse for part in cross_parts(current, field)]
    pushed = cross_parts(velocity, field)
    return [resist * current[c] - pushed[c] for c in range(3)]


def plain_form(b_field, resist, ymix, zmix):
    cells_z = b_field.shape[2]
    total_z = cells_z * lax.axis_size("gz")
    padded = with_halo(b_field, (("gz", 2), ("gx", 1)), 1)
    efield = jnp.stack(electric_parts(curl_of(padded), b_field, resist))
    curl_e = curl_of(with_halo(efield, (("gz", 2), ("gx", 1)), 1))
    stepped = b_field - time_step * curl_e
    along_y = jnp.einsum("cxzi,ij->cxjz", stepped, ymix, precision=lax.Precision.HIGHEST)
    running = jnp.cumsum(zmix, axis=1)
    slab_ends = running[:, cells_z - 1 :: cells_z][:, :-1]
    lower_flux = jnp.concatenate([jnp.zeros((total_z, 1), jnp.float32), slab_ends], axis=1)
    line_matrix = jnp.concatenate([zmix, lower_flux], axis=1)
    product = jnp.einsum(
        "cxym,mk->cxyk",
        lax.all_to_all(along_y, "gz", split_axis=2, concat_axis=3, tiled=True),
        line_matrix,
        precision=lax.Precision.HIGHEST,
    )
    returned, returned_flux = (
        lax.all_to_all(part, "gz", split_axis=3, concat_axis=2, tiled=True)
        for part in (product[..., :total_z], product[..., total_z:])
    )
    b_next = jnp.transpose(returned, (0, 1, 3, 2))
    offset = jnp.transpose(returned_flux, (0, 1, 3, 2))
    column = (jnp.cumsum(b_next, axis=2) + offset) * total_z ** (-0.5)
    return b_next, jnp.stack([column[1], -column[0], column[2]])


def slope(after, before):
    return (after - before) * 0.5


def along_row(value):
    cells_y = value.shape[1]
    return slope(pltpu.roll(value, cells_y - 1, 1), pltpu.roll(value, 1, 1))


def along_z(value, above, below):
    cells_z = value.shape[0]
    level = lax.broadcasted_iota(jnp.int32, value.shape, 0)
    after = jnp.where(level == cells_z - 1, above, pltpu.roll(value, cells_z - 1, 0))
    before = jnp.where(level == 0, below, pltpu.roll(value, 1, 0))
    return slope(after, before)


def over_x(cells_x, body):
    def trip(i, carry):
        for j in range(BATCH):
            body(i * BATCH + j)
        return carry

    lax.fori_loop(0, cells_x // BATCH, trip, 0)


def pack_kernel(b_ref, gx_ref, up_ref, down_ref, side_ref):
    cells_x, cells_z = b_ref.shape[1], b_ref.shape[2]
    edge = jnp.where(gx_ref[0] == 0, cells_x - 1, 0)
    for c in range(2):
        side_ref[c] = b_ref[c + 1, edge]
        for x in range(cells_x):
            at = pl.ds(c * cells_x + x, 1)
            up_ref[at, :] = b_ref[c, x, cells_z - 1 :, :]
            down_ref[at, :] = b_ref[c, x, :1, :]


def x_neighbours(ref, side_ref, first, c, x):
    cells_x = ref.shape[1]
    after = ref[c, jnp.minimum(x + 1, cells_x - 1)]
    before = ref[c, jnp.maximum(x - 1, 0)]
    zero = jnp.zeros_like(after)
    if side_ref is None:
        past_end, past_start = zero, zero
    else:
        side = side_ref[c - 1]
        past_end, past_start = jnp.where(first, side, zero), jnp.where(first, zero, side)
    return (
        jnp.where(x == cells_x - 1, past_end, after),
        jnp.where(x == 0, past_start, before),
    )


def electric_kernel(b_ref, r_ref, side_ref, below_ref, above_ref, gx_ref, elec_ref, edge_ref):
    cells_x = b_ref.shape[1]
    first = gx_ref[0] == 0

    def at(x):
        here = [b_ref[c, x] for c in range(3)]
        rows = [pl.ds(c * cells_x + x, 1) for c in range(2)]
        dz = [along_z(here[c], above_ref[rows[c], :], below_ref[rows[c], :]) for c in range(2)]
        dx = [None] + [slope(*x_neighbours(b_ref, side_ref, first, c, x)) for c in (1, 2)]
        current = (along_row(here[2]) - dz[1], dz[0] - dx[2], dx[1] - along_row(here[0]))
        for c, value in enumerate(electric_parts(current, here, r_ref[x])):
            elec_ref[c, x] = value

    over_x(cells_x, at)
    edge = jnp.where(first, cells_x - 1, 0)
    for c in range(2):
        edge_ref[c] = elec_ref[c + 1, edge]


def step_kernel(b_ref, elec_ref, rows_ref):
    cells_x, cells_z = b_ref.shape[1], b_ref.shape[2]
    half = 0.5 * time_step

    def at(x):
        here = [elec_ref[c, x] for c in range(3)]
        dz = [along_z(here[c], 0.0, 0.0) for c in range(2)]
        dx = [None] + [slope(*x_neighbours(elec_ref, None, None, c, x)) for c in (1, 2)]
        curl = (along_row(here[2]) - dz[1], dz[0] - dx[2], dx[1] - along_row(here[0]))
        for c in range(3):
            start = pl.multiple_of((c * cells_x + x) * cells_z, cells_z)
            rows_ref[pl.ds(start, cells_z), :] = b_ref[c, x] - time_step * curl[c]
        extra = 3 * cells_x * cells_z + 4 * x
        rows_ref[pl.ds(extra, 1), :] = half * here[1][:1]
        rows_ref[pl.ds(extra + 1, 1), :] = -half * here[1][cells_z - 1 :]
        rows_ref[pl.ds(extra + 2, 1), :] = -half * here[0][:1]
        rows_ref[pl.ds(extra + 3, 1), :] = half * here[0][cells_z - 1 :]

    over_x(cells_x, at)


def full_dot(lhs, rhs):
    return jnp.dot(lhs, rhs, precision=lax.Precision.HIGHEST, preferred_element_type=jnp.float32)


def mix_kernel(cells_x, cells_z, rows_ref, edge_ref, ymix_ref, gx_ref, out_ref, mixed):
    cells_y = rows_ref.shape[1]
    halves = cells_y // LANES
    mixed[...] = full_dot(rows_ref[...], ymix_ref[...])
    first = gx_ref[0] == 0
    factor = jnp.where(first, 0.5 * time_step, -0.5 * time_step)
    added = full_dot(edge_ref[...].reshape(2 * cells_z, cells_y), ymix_ref[...]) * factor
    edge = jnp.where(first, cells_x - 1, 0)
    for c, term in ((1, added[cells_z:]), (2, -added[:cells_z])):
        at = pl.ds(pl.multiple_of((c * cells_x + edge) * cells_z, cells_z), cells_z)
        mixed[at, :] = mixed[at, :] + term
    pairs = cells_x * halves // out_ref.shape[0]
    extra = 3 * cells_x * cells_z
    for x in range(cells_x):
        for half in range(halves):
            part, q = divmod(x * halves + half, pairs)
            lanes = slice(half * LANES, (half + 1) * LANES)
            for c in range(3):
                at = (q * 3 + c) * cells_z
                line = (c * cells_x + x) * cells_z
                out_ref[part, at : at + cells_z, :] = mixed[line : line + cells_z, lanes]
            at = pairs * 3 * cells_z + q * 4
            out_ref[part, at : at + 4, :] = mixed[extra + 4 * x : extra + 4 * x + 4, lanes]


def line_matrix_kernel(zmix_ref, out_ref):
    total = zmix_ref.shape[0]
    parts = out_ref.shape[0] - total
    turned = jnp.transpose(zmix_ref[...])
    slab = lax.broadcasted_iota(jnp.int32, (parts, total), 0) * (total // parts)
    lower = (lax.broadcasted_iota(jnp.int32, (parts, total), 1) < slab).astype(jnp.float32)
    out_ref[:total] = turned
    out_ref[total:] = jnp.dot(
        lower, turned, precision=lax.Precision.HIGHEST, preferred_element_type=jnp.float32
    )


def lines_kernel(cells_z, pairs, in_ref, line_ref, out_ref):
    parts = in_ref.shape[0]
    total = parts * cells_z
    height = pairs * 3 * cells_z
    level = lax.broadcasted_iota(jnp.int32, (cells_z, LANES), 0)
    columns = []
    for q in range(pairs):
        for c in range(3):
            at = (q * 3 + c) * cells_z
            tiles = [in_ref[s, at : at + cells_z, :] for s in range(parts)]
            if c < 2:
                low = height + q * 4 + c * 2
                for s in range(parts):
                    if s < parts - 1:
                        tiles[s] = tiles[s] + jnp.where(
                            level == cells_z - 1, in_ref[s + 1, low : low + 1, :], 0.0
                        )
                    if s > 0:
                        tiles[s] = tiles[s] + jnp.where(
                            level == 0, in_ref[s - 1, low + 1 : low + 2, :], 0.0
                        )
            columns.append(jnp.concatenate(tiles, axis=0))
    product = full_dot(line_ref[...], jnp.concatenate(columns, axis=1))
    for g in range(3 * pairs):
        part = product[:, g * LANES : (g + 1) * LANES]
        out_ref[:, g * cells_z : (g + 1) * cells_z, :] = part[:total].reshape(parts, cells_z, LANES)
        for s in range(parts):
            out_ref[s, height + g : height + g + 1, :] = part[total + s : total + s + 1]


def finish_kernel(scale, cells_z, in_ref, next_ref, pot_ref, buffer, sems):
    _, cells_x, _, cells_y = next_ref.shape
    each = in_ref.shape[1] // (cells_z + 1)
    halves = cells_y // LANES
    batch = cells_x // PIECES
    level = lax.broadcasted_iota(jnp.int32, (cells_z, LANES), 0)
    copies = []
    for piece in range(3 * PIECES):
        c, x = divmod(piece * batch, cells_x)
        factor = -scale if c == 0 else scale
        for i in range(batch):
            for half in range(halves):
                part, q = divmod((x + i) * halves + half, each // 3)
                at = q * 3 + c
                tile = in_ref[part, at * cells_z : (at + 1) * cells_z, :]
                total, step = tile, 1
                while step < cells_z:
                    total = total + jnp.where(level >= step, pltpu.roll(total, step, 0), 0.0)
                    step *= 2
                offset = in_ref[part, each * cells_z + at : each * cells_z + at + 1, :]
                lanes = slice(half * LANES, (half + 1) * LANES)
                buffer[0, piece, i, :, lanes] = tile
                buffer[1, piece, i, :, lanes] = (total + offset) * factor
        for k, (target, ref) in enumerate(((c, next_ref), ((1, 0, 2)[c], pot_ref))):
            copy = pltpu.make_async_copy(
                buffer.at[k, piece], ref.at[target, pl.ds(x, batch)], sems.at[k, piece]
            )
            copy.start()
            copies.append(copy)
    for copy in copies:
        copy.wait()


def limit(mib):
    return pltpu.CompilerParams(vmem_limit_bytes=mib * 2**20)


def kernel_form(b_field, resist, ymix, zmix):
    _, cells_x, cells_z, cells_y = b_field.shape
    parts = lax.axis_size("gz")
    total_z = cells_z * parts
    f32 = jnp.float32
    shape = lambda *sizes: jax.ShapeDtypeStruct(sizes, f32)
    place = lax.axis_index("gx").astype(jnp.int32).reshape(1)
    swap = lambda value: lax.ppermute(value, "gx", [(0, 1), (1, 0)])

    up, down, side = pl.pallas_call(
        pack_kernel,
        out_shape=(shape(2 * cells_x, cells_y), shape(2 * cells_x, cells_y), shape(2, cells_z, cells_y)),
        in_specs=[VMEM, SMEM],
        out_specs=(VMEM, VMEM, VMEM),
        compiler_params=limit(6),
    )(b_field, place)
    below = lax.ppermute(up, "gz", [(i, i + 1) for i in range(parts - 1)])
    above = lax.ppermute(down, "gz", [(i + 1, i) for i in range(parts - 1)])
    elec, edge = pl.pallas_call(
        electric_kernel,
        out_shape=(shape(*b_field.shape), shape(2, cells_z, cells_y)),
        in_specs=[VMEM] * 5 + [SMEM],
        out_specs=(VMEM, VMEM),
        compiler_params=limit(6),
        cost_estimate=estimate(200.0 * b_field.size),
    )(b_field, resist, swap(side), below, above, place)
    rows = pl.pallas_call(
        step_kernel,
        out_shape=shape(3 * cells_x * cells_z + 4 * cells_x, cells_y),
        in_specs=[VMEM] * 2,
        out_specs=VMEM,
        compiler_params=limit(6),
        cost_estimate=estimate(200.0 * b_field.size),
    )(b_field, elec)
    line = pl.pallas_call(
        line_matrix_kernel,
        out_shape=shape(total_z + parts, total_z),
        in_specs=[VMEM],
        out_specs=VMEM,
        compiler_params=limit(4),
    )(zmix)

    pairs = cells_x * (cells_y // LANES) // parts
    sent = pl.pallas_call(
        functools.partial(mix_kernel, cells_x, cells_z),
        out_shape=shape(parts, pairs * (3 * cells_z + 4), LANES),
        in_specs=[VMEM] * 3 + [SMEM],
        out_specs=VMEM,
        scratch_shapes=[pltpu.VMEM(rows.shape, f32)],
        compiler_params=limit(6),
    )(rows, swap(edge), ymix, place)
    lines = lax.all_to_all(sent, "gz", split_axis=0, concat_axis=0, tiled=True)
    product = pl.pallas_call(
        functools.partial(lines_kernel, cells_z, pairs),
        out_shape=shape(parts, pairs * 3 * (cells_z + 1), LANES),
        in_specs=[VMEM, VMEM],
        out_specs=VMEM,
        compiler_params=limit(6),
    )(lines, line)
    returned = lax.all_to_all(product, "gz", split_axis=0, concat_axis=0, tiled=True)
    whole = jax.ShapeDtypeStruct(b_field.shape, f32)
    hbm = pl.BlockSpec(memory_space=pl.ANY)
    return pl.pallas_call(
        functools.partial(finish_kernel, total_z ** (-0.5), cells_z),
        out_shape=(whole, whole),
        in_specs=[VMEM],
        out_specs=(hbm, hbm),
        scratch_shapes=[
            pltpu.VMEM((2, 3 * PIECES, cells_x // PIECES, cells_z, cells_y), f32),
            pltpu.SemaphoreType.DMA((2, 3 * PIECES)),
        ],
        compiler_params=limit(6),
    )(returned)


def estimate(flops):
    return pl.CostEstimate(flops=int(flops), bytes_accessed=0, transcendentals=0)


def on_device(b_field, resist, ymix, zmix):
    _, cells_x, cells_z, cells_y = b_field.shape
    parts = lax.axis_size("gz")
    fits = (
        lax.axis_size("gx") == 2
        and parts > 1
        and cells_z == SUBLANES
        and cells_x % PIECES == 0
        and cells_y % LANES == 0
        and cells_x % BATCH == 0
        and cells_x * (cells_y // LANES) % parts == 0
    )
    return (kernel_form if fits else plain_form)(b_field, resist, ymix, zmix)


def solution(mesh):
    in_specs = (P(None, "gx", "gz", None), P("gx", "gz", None), P(), P())
    out_specs = (P(None, "gx", "gz", None), P(None, "gx", "gz", None))
    return jax.shard_map(
        on_device, mesh=mesh, in_specs=in_specs, out_specs=out_specs, check_vma=False
    )
```

```python
import functools
import jax
import jax.numpy as jnp
from jax import lax
from jax.experimental import pallas as pl
from jax.experimental.pallas import tpu as pltpu
from jax.sharding import PartitionSpec as P

time_step = 0.1
friction = 1.0
LANES = 128
SUBLANES = 8
PIECES = 3
BATCH = 6
VMEM = pl.BlockSpec(memory_space=pltpu.VMEM)
SMEM = pl.BlockSpec(memory_space=pltpu.SMEM)


def with_halo(block, sides, width):
    for axis, dim in sides:
        count = lax.axis_size(axis)
        forward = [(i, i + 1) for i in range(count - 1)]
        backward = [(target, source) for source, target in forward]
        low = lax.ppermute(
            lax.slice_in_dim(block, block.shape[dim] - width, None, axis=dim), axis, forward
        )
        high = lax.ppermute(lax.slice_in_dim(block, 0, width, axis=dim), axis, backward)
        block = jnp.concatenate([low, block, high], axis=dim)
    return block


def curl_of(padded):
    centre = padded[:, 1:-1, 1:-1, :]
    grad_x = (padded[:, 2:, 1:-1, :] - padded[:, :-2, 1:-1, :]) * 0.5
    grad_z = (padded[:, 1:-1, 2:, :] - padded[:, 1:-1, :-2, :]) * 0.5
    grad_y = (jnp.roll(centre, -1, 3) - jnp.roll(centre, 1, 3)) * 0.5
    return jnp.stack([grad_y[2] - grad_z[1], grad_z[0] - grad_x[2], grad_x[1] - grad_y[0]])


def cross_parts(lhs, rhs):
    return (
        lhs[1] * rhs[2] - lhs[2] * rhs[1],
        lhs[2] * rhs[0] - lhs[0] * rhs[2],
        lhs[0] * rhs[1] - lhs[1] * rhs[0],
    )


def electric_parts(current, field, resist):
    strength = field[0] * field[0] + field[1] * field[1] + field[2] * field[2] + 1.0
    inverse = 1.0 / (friction * strength)
    velocity = [part * inverse for part in cross_parts(current, field)]
    pushed = cross_parts(velocity, field)
    return [resist * current[c] - pushed[c] for c in range(3)]


def plain_form(b_field, resist, ymix, zmix):
    cells_z = b_field.shape[2]
    total_z = cells_z * lax.axis_size("gz")
    padded = with_halo(b_field, (("gz", 2), ("gx", 1)), 1)
    efield = jnp.stack(electric_parts(curl_of(padded), b_field, resist))
    curl_e = curl_of(with_halo(efield, (("gz", 2), ("gx", 1)), 1))
    stepped = b_field - time_step * curl_e
    along_y = jnp.einsum("cxzi,ij->cxjz", stepped, ymix, precision=lax.Precision.HIGHEST)
    running = jnp.cumsum(zmix, axis=1)
    slab_ends = running[:, cells_z - 1 :: cells_z][:, :-1]
    lower_flux = jnp.concatenate([jnp.zeros((total_z, 1), jnp.float32), slab_ends], axis=1)
    line_matrix = jnp.concatenate([zmix, lower_flux], axis=1)
    product = jnp.einsum(
        "cxym,mk->cxyk",
        lax.all_to_all(along_y, "gz", split_axis=2, concat_axis=3, tiled=True),
        line_matrix,
        precision=lax.Precision.HIGHEST,
    )
    returned, returned_flux = (
        lax.all_to_all(part, "gz", split_axis=3, concat_axis=2, tiled=True)
        for part in (product[..., :total_z], product[..., total_z:])
    )
    b_next = jnp.transpose(returned, (0, 1, 3, 2))
    offset = jnp.transpose(returned_flux, (0, 1, 3, 2))
    column = (jnp.cumsum(b_next, axis=2) + offset) * total_z ** (-0.5)
    return b_next, jnp.stack([column[1], -column[0], column[2]])


def slope(after, before):
    return (after - before) * 0.5


def along_row(value):
    cells_y = value.shape[1]
    return slope(pltpu.roll(value, cells_y - 1, 1), pltpu.roll(value, 1, 1))


def along_z(value, above, below):
    cells_z = value.shape[0]
    level = lax.broadcasted_iota(jnp.int32, value.shape, 0)
    after = jnp.where(level == cells_z - 1, above, pltpu.roll(value, cells_z - 1, 0))
    before = jnp.where(level == 0, below, pltpu.roll(value, 1, 0))
    return slope(after, before)


def over_x(cells_x, body):
    def trip(i, carry):
        for j in range(BATCH):
            body(i * BATCH + j)
        return carry

    lax.fori_loop(0, cells_x // BATCH, trip, 0)


def pack_kernel(b_ref, gx_ref, up_ref, down_ref, side_ref):
    cells_x, cells_z = b_ref.shape[1], b_ref.shape[2]
    edge = jnp.where(gx_ref[0] == 0, cells_x - 1, 0)
    for c in range(2):
        side_ref[c] = b_ref[c + 1, edge]
        for x in range(cells_x):
            at = pl.ds(c * cells_x + x, 1)
            up_ref[at, :] = b_ref[c, x, cells_z - 1 :, :]
            down_ref[at, :] = b_ref[c, x, :1, :]


def x_neighbours(ref, side_ref, first, c, x):
    cells_x = ref.shape[1]
    after = ref[c, jnp.minimum(x + 1, cells_x - 1)]
    before = ref[c, jnp.maximum(x - 1, 0)]
    zero = jnp.zeros_like(after)
    if side_ref is None:
        past_end, past_start = zero, zero
    else:
        side = side_ref[c - 1]
        past_end, past_start = jnp.where(first, side, zero), jnp.where(first, zero, side)
    return (
        jnp.where(x == cells_x - 1, past_end, after),
        jnp.where(x == 0, past_start, before),
    )


def electric_kernel(b_ref, r_ref, side_ref, below_ref, above_ref, gx_ref, elec_ref, edge_ref):
    cells_x = b_ref.shape[1]
    first = gx_ref[0] == 0

    def at(x):
        here = [b_ref[c, x] for c in range(3)]
        rows = [pl.ds(c * cells_x + x, 1) for c in range(2)]
        dz = [along_z(here[c], above_ref[rows[c], :], below_ref[rows[c], :]) for c in range(2)]
        dx = [None] + [slope(*x_neighbours(b_ref, side_ref, first, c, x)) for c in (1, 2)]
        current = (along_row(here[2]) - dz[1], dz[0] - dx[2], dx[1] - along_row(here[0]))
        for c, value in enumerate(electric_parts(current, here, r_ref[x])):
            elec_ref[c, x] = value

    over_x(cells_x, at)
    edge = jnp.where(first, cells_x - 1, 0)
    for c in range(2):
        edge_ref[c] = elec_ref[c + 1, edge]


def step_kernel(b_ref, elec_ref, rows_ref):
    cells_x, cells_z = b_ref.shape[1], b_ref.shape[2]
    half = 0.5 * time_step

    def at(x):
        here = [elec_ref[c, x] for c in range(3)]
        dz = [along_z(here[c], 0.0, 0.0) for c in range(2)]
        dx = [None] + [slope(*x_neighbours(elec_ref, None, None, c, x)) for c in (1, 2)]
        curl = (along_row(here[2]) - dz[1], dz[0] - dx[2], dx[1] - along_row(here[0]))
        for c in range(3):
            start = pl.multiple_of((c * cells_x + x) * cells_z, cells_z)
            rows_ref[pl.ds(start, cells_z), :] = b_ref[c, x] - time_step * curl[c]
        extra = 3 * cells_x * cells_z + 4 * x
        rows_ref[pl.ds(extra, 1), :] = half * here[1][:1]
        rows_ref[pl.ds(extra + 1, 1), :] = -half * here[1][cells_z - 1 :]
        rows_ref[pl.ds(extra + 2, 1), :] = -half * here[0][:1]
        rows_ref[pl.ds(extra + 3, 1), :] = half * here[0][cells_z - 1 :]

    over_x(cells_x, at)


def split(value):
    high = value.astype(jnp.bfloat16)
    return high, (value - high.astype(jnp.float32)).astype(jnp.bfloat16)


def full_dot(lhs, rhs):
    dot = functools.partial(jnp.dot, preferred_element_type=jnp.float32)
    (lhs_high, lhs_low), (rhs_high, rhs_low) = split(lhs), split(rhs)
    return dot(lhs_high, rhs_high) + (dot(lhs_high, rhs_low) + dot(lhs_low, rhs_high))


def mix_kernel(cells_x, cells_z, rows_ref, edge_ref, ymix_ref, gx_ref, out_ref, mixed):
    cells_y = rows_ref.shape[1]
    halves = cells_y // LANES
    mixed[...] = full_dot(rows_ref[...], ymix_ref[...])
    first = gx_ref[0] == 0
    factor = jnp.where(first, 0.5 * time_step, -0.5 * time_step)
    added = full_dot(edge_ref[...].reshape(2 * cells_z, cells_y), ymix_ref[...]) * factor
    edge = jnp.where(first, cells_x - 1, 0)
    for c, term in ((1, added[cells_z:]), (2, -added[:cells_z])):
        at = pl.ds(pl.multiple_of((c * cells_x + edge) * cells_z, cells_z), cells_z)
        mixed[at, :] = mixed[at, :] + term
    pairs = cells_x * halves // out_ref.shape[0]
    extra = 3 * cells_x * cells_z
    for x in range(cells_x):
        for half in range(halves):
            part, q = divmod(x * halves + half, pairs)
            lanes = slice(half * LANES, (half + 1) * LANES)
            for c in range(3):
                at = (q * 3 + c) * cells_z
                line = (c * cells_x + x) * cells_z
                out_ref[part, at : at + cells_z, :] = mixed[line : line + cells_z, lanes]
            at = pairs * 3 * cells_z + q * 4
            out_ref[part, at : at + 4, :] = mixed[extra + 4 * x : extra + 4 * x + 4, lanes]


def line_matrix_kernel(zmix_ref, out_ref):
    total = zmix_ref.shape[0]
    parts = out_ref.shape[0] - total
    turned = jnp.transpose(zmix_ref[...])
    slab = lax.broadcasted_iota(jnp.int32, (parts, total), 0) * (total // parts)
    lower = (lax.broadcasted_iota(jnp.int32, (parts, total), 1) < slab).astype(jnp.float32)
    out_ref[:total] = turned
    out_ref[total:] = jnp.dot(
        lower, turned, precision=lax.Precision.HIGHEST, preferred_element_type=jnp.float32
    )


def lines_kernel(cells_z, pairs, in_ref, line_ref, out_ref):
    parts = in_ref.shape[0]
    total = parts * cells_z
    height = pairs * 3 * cells_z
    level = lax.broadcasted_iota(jnp.int32, (cells_z, LANES), 0)
    columns = []
    for q in range(pairs):
        for c in range(3):
            at = (q * 3 + c) * cells_z
            tiles = [in_ref[s, at : at + cells_z, :] for s in range(parts)]
            if c < 2:
                low = height + q * 4 + c * 2
                for s in range(parts):
                    if s < parts - 1:
                        tiles[s] = tiles[s] + jnp.where(
                            level == cells_z - 1, in_ref[s + 1, low : low + 1, :], 0.0
                        )
                    if s > 0:
                        tiles[s] = tiles[s] + jnp.where(
                            level == 0, in_ref[s - 1, low + 1 : low + 2, :], 0.0
                        )
            columns.append(jnp.concatenate(tiles, axis=0))
    product = full_dot(line_ref[...], jnp.concatenate(columns, axis=1))
    for g in range(3 * pairs):
        part = product[:, g * LANES : (g + 1) * LANES]
        out_ref[:, g * cells_z : (g + 1) * cells_z, :] = part[:total].reshape(parts, cells_z, LANES)
        for s in range(parts):
            out_ref[s, height + g : height + g + 1, :] = part[total + s : total + s + 1]


def finish_kernel(scale, cells_z, in_ref, next_ref, pot_ref, buffer, sems):
    _, cells_x, _, cells_y = next_ref.shape
    each = in_ref.shape[1] // (cells_z + 1)
    halves = cells_y // LANES
    batch = cells_x // PIECES
    level = lax.broadcasted_iota(jnp.int32, (cells_z, LANES), 0)
    copies = []
    for piece in range(3 * PIECES):
        c, x = divmod(piece * batch, cells_x)
        factor = -scale if c == 0 else scale
        for i in range(batch):
            for half in range(halves):
                part, q = divmod((x + i) * halves + half, each // 3)
                at = q * 3 + c
                tile = in_ref[part, at * cells_z : (at + 1) * cells_z, :]
                total, step = tile, 1
                while step < cells_z:
                    total = total + jnp.where(level >= step, pltpu.roll(total, step, 0), 0.0)
                    step *= 2
                offset = in_ref[part, each * cells_z + at : each * cells_z + at + 1, :]
                lanes = slice(half * LANES, (half + 1) * LANES)
                buffer[0, piece, i, :, lanes] = tile
                buffer[1, piece, i, :, lanes] = (total + offset) * factor
        for k, (target, ref) in enumerate(((c, next_ref), ((1, 0, 2)[c], pot_ref))):
            copy = pltpu.make_async_copy(
                buffer.at[k, piece], ref.at[target, pl.ds(x, batch)], sems.at[k, piece]
            )
            copy.start()
            copies.append(copy)
    for copy in copies:
        copy.wait()


def limit(mib):
    return pltpu.CompilerParams(vmem_limit_bytes=mib * 2**20)


def kernel_form(b_field, resist, ymix, zmix):
    _, cells_x, cells_z, cells_y = b_field.shape
    parts = lax.axis_size("gz")
    total_z = cells_z * parts
    f32 = jnp.float32
    shape = lambda *sizes: jax.ShapeDtypeStruct(sizes, f32)
    place = lax.axis_index("gx").astype(jnp.int32).reshape(1)
    swap = lambda value: lax.ppermute(value, "gx", [(0, 1), (1, 0)])

    up, down, side = pl.pallas_call(
        pack_kernel,
        out_shape=(shape(2 * cells_x, cells_y), shape(2 * cells_x, cells_y), shape(2, cells_z, cells_y)),
        in_specs=[VMEM, SMEM],
        out_specs=(VMEM, VMEM, VMEM),
        compiler_params=limit(6),
    )(b_field, place)
    below = lax.ppermute(up, "gz", [(i, i + 1) for i in range(parts - 1)])
    above = lax.ppermute(down, "gz", [(i + 1, i) for i in range(parts - 1)])
    line = pl.pallas_call(
        line_matrix_kernel,
        out_shape=shape(total_z + parts, total_z),
        in_specs=[VMEM],
        out_specs=VMEM,
        compiler_params=limit(4),
    )(zmix)
    line, below = lax.optimization_barrier((line, below))
    elec, edge = pl.pallas_call(
        electric_kernel,
        out_shape=(shape(*b_field.shape), shape(2, cells_z, cells_y)),
        in_specs=[VMEM] * 5 + [SMEM],
        out_specs=(VMEM, VMEM),
        compiler_params=limit(6),
        cost_estimate=estimate(200.0 * b_field.size),
    )(b_field, resist, swap(side), below, above, place)
    rows = pl.pallas_call(
        step_kernel,
        out_shape=shape(3 * cells_x * cells_z + 4 * cells_x, cells_y),
        in_specs=[VMEM] * 2,
        out_specs=VMEM,
        compiler_params=limit(6),
        cost_estimate=estimate(200.0 * b_field.size),
    )(b_field, elec)
    pairs = cells_x * (cells_y // LANES) // parts
    sent = pl.pallas_call(
        functools.partial(mix_kernel, cells_x, cells_z),
        out_shape=shape(parts, pairs * (3 * cells_z + 4), LANES),
        in_specs=[VMEM] * 3 + [SMEM],
        out_specs=VMEM,
        scratch_shapes=[pltpu.VMEM(rows.shape, f32)],
        compiler_params=limit(6),
    )(rows, swap(edge), ymix, place)
    lines = lax.all_to_all(sent, "gz", split_axis=0, concat_axis=0, tiled=True)
    product = pl.pallas_call(
        functools.partial(lines_kernel, cells_z, pairs),
        out_shape=shape(parts, pairs * 3 * (cells_z + 1), LANES),
        in_specs=[VMEM, VMEM],
        out_specs=VMEM,
        compiler_params=limit(6),
    )(lines, line)
    returned = lax.all_to_all(product, "gz", split_axis=0, concat_axis=0, tiled=True)
    whole = jax.ShapeDtypeStruct(b_field.shape, f32)
    hbm = pl.BlockSpec(memory_space=pl.ANY)
    return pl.pallas_call(
        functools.partial(finish_kernel, total_z ** (-0.5), cells_z),
        out_shape=(whole, whole),
        in_specs=[VMEM],
        out_specs=(hbm, hbm),
        scratch_shapes=[
            pltpu.VMEM((2, 3 * PIECES, cells_x // PIECES, cells_z, cells_y), f32),
            pltpu.SemaphoreType.DMA((2, 3 * PIECES)),
        ],
        compiler_params=limit(6),
    )(returned)


def estimate(flops):
    return pl.CostEstimate(flops=int(flops), bytes_accessed=0, transcendentals=0)


def on_device(b_field, resist, ymix, zmix):
    _, cells_x, cells_z, cells_y = b_field.shape
    parts = lax.axis_size("gz")
    fits = (
        lax.axis_size("gx") == 2
        and parts > 1
        and cells_z == SUBLANES
        and cells_x % PIECES == 0
        and cells_y % LANES == 0
        and cells_x % BATCH == 0
        and cells_x * (cells_y // LANES) % parts == 0
    )
    return (kernel_form if fits else plain_form)(b_field, resist, ymix, zmix)


def solution(mesh):
    in_specs = (P(None, "gx", "gz", None), P("gx", "gz", None), P(), P())
    out_specs = (P(None, "gx", "gz", None), P(None, "gx", "gz", None))
    return jax.shard_map(
        on_device, mesh=mesh, in_specs=in_specs, out_specs=out_specs, check_vma=False
    )
```

```python
import functools
import jax
import jax.numpy as jnp
from jax import lax
from jax.experimental import pallas as pl
from jax.experimental.pallas import tpu as pltpu
from jax.sharding import PartitionSpec as P

time_step = 0.1
friction = 1.0
LANES = 128
SUBLANES = 8
SHORT = 4
PIECES = 3
BATCH = 6
VMEM = pl.BlockSpec(memory_space=pltpu.VMEM)
SMEM = pl.BlockSpec(memory_space=pltpu.SMEM)


def with_halo(block, sides, width):
    for axis, dim in sides:
        count = lax.axis_size(axis)
        forward = [(i, i + 1) for i in range(count - 1)]
        backward = [(target, source) for source, target in forward]
        low = lax.ppermute(
            lax.slice_in_dim(block, block.shape[dim] - width, None, axis=dim), axis, forward
        )
        high = lax.ppermute(lax.slice_in_dim(block, 0, width, axis=dim), axis, backward)
        block = jnp.concatenate([low, block, high], axis=dim)
    return block


def curl_of(padded):
    centre = padded[:, 1:-1, 1:-1, :]
    grad_x = (padded[:, 2:, 1:-1, :] - padded[:, :-2, 1:-1, :]) * 0.5
    grad_z = (padded[:, 1:-1, 2:, :] - padded[:, 1:-1, :-2, :]) * 0.5
    grad_y = (jnp.roll(centre, -1, 3) - jnp.roll(centre, 1, 3)) * 0.5
    return jnp.stack([grad_y[2] - grad_z[1], grad_z[0] - grad_x[2], grad_x[1] - grad_y[0]])


def cross_parts(lhs, rhs):
    return (
        lhs[1] * rhs[2] - lhs[2] * rhs[1],
        lhs[2] * rhs[0] - lhs[0] * rhs[2],
        lhs[0] * rhs[1] - lhs[1] * rhs[0],
    )


def electric_parts(current, field, resist):
    strength = field[0] * field[0] + field[1] * field[1] + field[2] * field[2] + 1.0
    inverse = 1.0 / (friction * strength)
    velocity = [part * inverse for part in cross_parts(current, field)]
    pushed = cross_parts(velocity, field)
    return [resist * current[c] - pushed[c] for c in range(3)]


def plain_form(b_field, resist, ymix, zmix):
    cells_z = b_field.shape[2]
    total_z = cells_z * lax.axis_size("gz")
    padded = with_halo(b_field, (("gz", 2), ("gx", 1)), 1)
    efield = jnp.stack(electric_parts(curl_of(padded), b_field, resist))
    curl_e = curl_of(with_halo(efield, (("gz", 2), ("gx", 1)), 1))
    stepped = b_field - time_step * curl_e
    along_y = jnp.einsum("cxzi,ij->cxjz", stepped, ymix, precision=lax.Precision.HIGHEST)
    running = jnp.cumsum(zmix, axis=1)
    slab_ends = running[:, cells_z - 1 :: cells_z][:, :-1]
    lower_flux = jnp.concatenate([jnp.zeros((total_z, 1), jnp.float32), slab_ends], axis=1)
    line_matrix = jnp.concatenate([zmix, lower_flux], axis=1)
    product = jnp.einsum(
        "cxym,mk->cxyk",
        lax.all_to_all(along_y, "gz", split_axis=2, concat_axis=3, tiled=True),
        line_matrix,
        precision=lax.Precision.HIGHEST,
    )
    returned, returned_flux = (
        lax.all_to_all(part, "gz", split_axis=3, concat_axis=2, tiled=True)
        for part in (product[..., :total_z], product[..., total_z:])
    )
    b_next = jnp.transpose(returned, (0, 1, 3, 2))
    offset = jnp.transpose(returned_flux, (0, 1, 3, 2))
    column = (jnp.cumsum(b_next, axis=2) + offset) * total_z ** (-0.5)
    return b_next, jnp.stack([column[1], -column[0], column[2]])


def store_tile(ref, part, at, tile):
    count = tile.shape[0] // SHORT
    ref[part, at // SHORT : at // SHORT + count] = tile.reshape(count, SHORT, LANES)


def load_tile(ref, part, at, height):
    return ref[part, at // SHORT : (at + height) // SHORT].reshape(height, LANES)


def one_row(ref, part, at):
    return ref[part, at // SHORT, at % SHORT : at % SHORT + 1, :]


def slope(after, before):
    return (after - before) * 0.5


def along_row(value):
    cells_y = value.shape[1]
    return slope(pltpu.roll(value, cells_y - 1, 1), pltpu.roll(value, 1, 1))


def along_z(value, above, below):
    cells_z = value.shape[0]
    level = lax.broadcasted_iota(jnp.int32, value.shape, 0)
    after = jnp.where(level == cells_z - 1, above, pltpu.roll(value, cells_z - 1, 0))
    before = jnp.where(level == 0, below, pltpu.roll(value, 1, 0))
    return slope(after, before)


def over_x(cells_x, body):
    def trip(i, carry):
        for j in range(BATCH):
            body(i * BATCH + j)
        return carry

    lax.fori_loop(0, cells_x // BATCH, trip, 0)


def pack_kernel(b_ref, gx_ref, up_ref, down_ref, side_ref):
    cells_x, cells_z = b_ref.shape[1], b_ref.shape[2]
    edge = jnp.where(gx_ref[0] == 0, cells_x - 1, 0)
    for c in range(2):
        side_ref[c] = b_ref[c + 1, edge]
        for x in range(cells_x):
            at = pl.ds(c * cells_x + x, 1)
            up_ref[at, :] = b_ref[c, x, cells_z - 1 :, :]
            down_ref[at, :] = b_ref[c, x, :1, :]


def x_neighbours(ref, side_ref, first, c, x):
    cells_x = ref.shape[1]
    after = ref[c, jnp.minimum(x + 1, cells_x - 1)]
    before = ref[c, jnp.maximum(x - 1, 0)]
    zero = jnp.zeros_like(after)
    if side_ref is None:
        past_end, past_start = zero, zero
    else:
        side = side_ref[c - 1]
        past_end, past_start = jnp.where(first, side, zero), jnp.where(first, zero, side)
    return (
        jnp.where(x == cells_x - 1, past_end, after),
        jnp.where(x == 0, past_start, before),
    )


def electric_kernel(b_ref, r_ref, side_ref, below_ref, above_ref, gx_ref, elec_ref, edge_ref):
    cells_x = b_ref.shape[1]
    first = gx_ref[0] == 0

    def at(x):
        here = [b_ref[c, x] for c in range(3)]
        rows = [pl.ds(c * cells_x + x, 1) for c in range(2)]
        dz = [along_z(here[c], above_ref[rows[c], :], below_ref[rows[c], :]) for c in range(2)]
        dx = [None] + [slope(*x_neighbours(b_ref, side_ref, first, c, x)) for c in (1, 2)]
        current = (along_row(here[2]) - dz[1], dz[0] - dx[2], dx[1] - along_row(here[0]))
        for c, value in enumerate(electric_parts(current, here, r_ref[x])):
            elec_ref[c, x] = value

    over_x(cells_x, at)
    edge = jnp.where(first, cells_x - 1, 0)
    for c in range(2):
        edge_ref[c] = elec_ref[c + 1, edge]


def step_kernel(b_ref, elec_ref, rows_ref):
    cells_x, cells_z = b_ref.shape[1], b_ref.shape[2]
    half = 0.5 * time_step

    def at(x):
        here = [elec_ref[c, x] for c in range(3)]
        dz = [along_z(here[c], 0.0, 0.0) for c in range(2)]
        dx = [None] + [slope(*x_neighbours(elec_ref, None, None, c, x)) for c in (1, 2)]
        curl = (along_row(here[2]) - dz[1], dz[0] - dx[2], dx[1] - along_row(here[0]))
        for c in range(3):
            start = pl.multiple_of((c * cells_x + x) * cells_z, cells_z)
            rows_ref[pl.ds(start, cells_z), :] = b_ref[c, x] - time_step * curl[c]
        extra = 3 * cells_x * cells_z + 4 * x
        rows_ref[pl.ds(extra, 1), :] = half * here[1][:1]
        rows_ref[pl.ds(extra + 1, 1), :] = -half * here[1][cells_z - 1 :]
        rows_ref[pl.ds(extra + 2, 1), :] = -half * here[0][:1]
        rows_ref[pl.ds(extra + 3, 1), :] = half * here[0][cells_z - 1 :]

    over_x(cells_x, at)


def split(value):
    high = value.astype(jnp.bfloat16)
    return high, (value - high.astype(jnp.float32)).astype(jnp.bfloat16)


def full_dot(lhs, rhs):
    dot = functools.partial(jnp.dot, preferred_element_type=jnp.float32)
    (lhs_high, lhs_low), (rhs_high, rhs_low) = split(lhs), split(rhs)
    return dot(lhs_high, rhs_high) + (dot(lhs_high, rhs_low) + dot(lhs_low, rhs_high))


def mix_kernel(cells_x, cells_z, rows_ref, edge_ref, ymix_ref, gx_ref, out_ref, mixed):
    cells_y = rows_ref.shape[1]
    halves = cells_y // LANES
    mixed[...] = full_dot(rows_ref[...], ymix_ref[...])
    first = gx_ref[0] == 0
    factor = jnp.where(first, 0.5 * time_step, -0.5 * time_step)
    added = full_dot(edge_ref[...].reshape(2 * cells_z, cells_y), ymix_ref[...]) * factor
    edge = jnp.where(first, cells_x - 1, 0)
    for c, term in ((1, added[cells_z:]), (2, -added[:cells_z])):
        at = pl.ds(pl.multiple_of((c * cells_x + edge) * cells_z, cells_z), cells_z)
        mixed[at, :] = mixed[at, :] + term
    pairs = cells_x * halves // out_ref.shape[0]
    extra = 3 * cells_x * cells_z
    for x in range(cells_x):
        for half in range(halves):
            part, q = divmod(x * halves + half, pairs)
            lanes = slice(half * LANES, (half + 1) * LANES)
            for c in range(3):
                at = (q * 3 + c) * cells_z
                line = (c * cells_x + x) * cells_z
                store_tile(out_ref, part, at, mixed[line : line + cells_z, lanes])
            at = pairs * 3 * cells_z + q * 4
            store_tile(out_ref, part, at, mixed[extra + 4 * x : extra + 4 * x + 4, lanes])


def line_matrix_kernel(zmix_ref, out_ref):
    total = zmix_ref.shape[0]
    parts = out_ref.shape[0] - total
    turned = jnp.transpose(zmix_ref[...])
    slab = lax.broadcasted_iota(jnp.int32, (parts, total), 0) * (total // parts)
    lower = (lax.broadcasted_iota(jnp.int32, (parts, total), 1) < slab).astype(jnp.float32)
    out_ref[:total] = turned
    out_ref[total:] = jnp.dot(
        lower, turned, precision=lax.Precision.HIGHEST, preferred_element_type=jnp.float32
    )


def lines_kernel(cells_z, pairs, in_ref, line_ref, out_ref):
    parts = in_ref.shape[0]
    total = parts * cells_z
    height = pairs * 3 * cells_z
    level = lax.broadcasted_iota(jnp.int32, (cells_z, LANES), 0)
    columns = []
    for q in range(pairs):
        for c in range(3):
            at = (q * 3 + c) * cells_z
            tiles = [load_tile(in_ref, s, at, cells_z) for s in range(parts)]
            if c < 2:
                low = height + q * 4 + c * 2
                for s in range(parts):
                    if s < parts - 1:
                        tiles[s] = tiles[s] + jnp.where(
                            level == cells_z - 1, one_row(in_ref, s + 1, low), 0.0
                        )
                    if s > 0:
                        tiles[s] = tiles[s] + jnp.where(
                            level == 0, one_row(in_ref, s - 1, low + 1), 0.0
                        )
            columns.append(jnp.concatenate(tiles, axis=0))
    product = full_dot(line_ref[...], jnp.concatenate(columns, axis=1))
    for g in range(3 * pairs):
        part = product[:, g * LANES : (g + 1) * LANES]
        row = height + g
        for s in range(parts):
            store_tile(out_ref, s, g * cells_z, part[s * cells_z : (s + 1) * cells_z])
            out_ref[s, row // SHORT, row % SHORT : row % SHORT + 1, :] = part[total + s : total + s + 1]


def finish_kernel(scale, cells_z, each, in_ref, next_ref, pot_ref, buffer, sems):
    _, cells_x, _, cells_y = next_ref.shape
    halves = cells_y // LANES
    batch = cells_x // PIECES
    level = lax.broadcasted_iota(jnp.int32, (cells_z, LANES), 0)
    copies = []
    for piece in range(3 * PIECES):
        c, x = divmod(piece * batch, cells_x)
        factor = -scale if c == 0 else scale
        for i in range(batch):
            for half in range(halves):
                part, q = divmod((x + i) * halves + half, each // 3)
                at = q * 3 + c
                tile = load_tile(in_ref, part, at * cells_z, cells_z)
                total, step = tile, 1
                while step < cells_z:
                    total = total + jnp.where(level >= step, pltpu.roll(total, step, 0), 0.0)
                    step *= 2
                offset = one_row(in_ref, part, each * cells_z + at)
                lanes = slice(half * LANES, (half + 1) * LANES)
                buffer[0, piece, i, :, lanes] = tile
                buffer[1, piece, i, :, lanes] = (total + offset) * factor
        for k, (target, ref) in enumerate(((c, next_ref), ((1, 0, 2)[c], pot_ref))):
            copy = pltpu.make_async_copy(
                buffer.at[k, piece], ref.at[target, pl.ds(x, batch)], sems.at[k, piece]
            )
            copy.start()
            copies.append(copy)
    for copy in copies:
        copy.wait()


def limit(mib):
    return pltpu.CompilerParams(vmem_limit_bytes=mib * 2**20)


def kernel_form(b_field, resist, ymix, zmix):
    _, cells_x, cells_z, cells_y = b_field.shape
    parts = lax.axis_size("gz")
    total_z = cells_z * parts
    f32 = jnp.float32
    shape = lambda *sizes: jax.ShapeDtypeStruct(sizes, f32)
    place = lax.axis_index("gx").astype(jnp.int32).reshape(1)
    swap = lambda value: lax.ppermute(value, "gx", [(0, 1), (1, 0)])

    up, down, side = pl.pallas_call(
        pack_kernel,
        out_shape=(shape(2 * cells_x, cells_y), shape(2 * cells_x, cells_y), shape(2, cells_z, cells_y)),
        in_specs=[VMEM, SMEM],
        out_specs=(VMEM, VMEM, VMEM),
        compiler_params=limit(6),
    )(b_field, place)
    below = lax.ppermute(up, "gz", [(i, i + 1) for i in range(parts - 1)])
    above = lax.ppermute(down, "gz", [(i + 1, i) for i in range(parts - 1)])
    line = pl.pallas_call(
        line_matrix_kernel,
        out_shape=shape(total_z + parts, total_z),
        in_specs=[VMEM],
        out_specs=VMEM,
        compiler_params=limit(4),
    )(zmix)
    line, below = lax.optimization_barrier((line, below))
    elec, edge = pl.pallas_call(
        electric_kernel,
        out_shape=(shape(*b_field.shape), shape(2, cells_z, cells_y)),
        in_specs=[VMEM] * 5 + [SMEM],
        out_specs=(VMEM, VMEM),
        compiler_params=limit(6),
        cost_estimate=estimate(200.0 * b_field.size),
    )(b_field, resist, swap(side), below, above, place)
    rows = pl.pallas_call(
        step_kernel,
        out_shape=shape(3 * cells_x * cells_z + 4 * cells_x, cells_y),
        in_specs=[VMEM] * 2,
        out_specs=VMEM,
        compiler_params=limit(6),
        cost_estimate=estimate(200.0 * b_field.size),
    )(b_field, elec)
    pairs = cells_x * (cells_y // LANES) // parts
    sent = pl.pallas_call(
        functools.partial(mix_kernel, cells_x, cells_z),
        out_shape=shape(parts, pairs * (3 * cells_z + 4) // SHORT, SHORT, LANES),
        in_specs=[VMEM] * 3 + [SMEM],
        out_specs=VMEM,
        scratch_shapes=[pltpu.VMEM(rows.shape, f32)],
        compiler_params=limit(6),
    )(rows, swap(edge), ymix, place)
    lines = lax.all_to_all(sent, "gz", split_axis=0, concat_axis=0, tiled=True)
    product = pl.pallas_call(
        functools.partial(lines_kernel, cells_z, pairs),
        out_shape=shape(parts, -(-pairs * 3 * (cells_z + 1) // SHORT), SHORT, LANES),
        in_specs=[VMEM, VMEM],
        out_specs=VMEM,
        compiler_params=limit(6),
    )(lines, line)
    returned = lax.all_to_all(product, "gz", split_axis=0, concat_axis=0, tiled=True)
    whole = jax.ShapeDtypeStruct(b_field.shape, f32)
    hbm = pl.BlockSpec(memory_space=pl.ANY)
    return pl.pallas_call(
        functools.partial(finish_kernel, total_z ** (-0.5), cells_z, 3 * pairs),
        out_shape=(whole, whole),
        in_specs=[VMEM],
        out_specs=(hbm, hbm),
        scratch_shapes=[
            pltpu.VMEM((2, 3 * PIECES, cells_x // PIECES, cells_z, cells_y), f32),
            pltpu.SemaphoreType.DMA((2, 3 * PIECES)),
        ],
        compiler_params=limit(6),
    )(returned)


def estimate(flops):
    return pl.CostEstimate(flops=int(flops), bytes_accessed=0, transcendentals=0)


def on_device(b_field, resist, ymix, zmix):
    _, cells_x, cells_z, cells_y = b_field.shape
    parts = lax.axis_size("gz")
    fits = (
        lax.axis_size("gx") == 2
        and parts > 1
        and cells_z == SUBLANES
        and cells_x % PIECES == 0
        and cells_y % LANES == 0
        and cells_x % BATCH == 0
        and cells_x * (cells_y // LANES) % parts == 0
    )
    return (kernel_form if fits else plain_form)(b_field, resist, ymix, zmix)


def solution(mesh):
    in_specs = (P(None, "gx", "gz", None), P("gx", "gz", None), P(), P())
    out_specs = (P(None, "gx", "gz", None), P(None, "gx", "gz", None))
    return jax.shard_map(
        on_device, mesh=mesh, in_specs=in_specs, out_specs=out_specs, check_vma=False
    )
```

```python
import functools
import jax
import jax.numpy as jnp
from jax import lax
from jax.experimental import pallas as pl
from jax.experimental.pallas import tpu as pltpu
from jax.sharding import PartitionSpec as P

time_step = 0.1
friction = 1.0
LANES = 128
SUBLANES = 8
SHORT = 4
PIECES = 3
BATCH = 6
VMEM = pl.BlockSpec(memory_space=pltpu.VMEM)
SMEM = pl.BlockSpec(memory_space=pltpu.SMEM)


def with_halo(block, sides, width):
    for axis, dim in sides:
        count = lax.axis_size(axis)
        forward = [(i, i + 1) for i in range(count - 1)]
        backward = [(target, source) for source, target in forward]
        low = lax.ppermute(
            lax.slice_in_dim(block, block.shape[dim] - width, None, axis=dim), axis, forward
        )
        high = lax.ppermute(lax.slice_in_dim(block, 0, width, axis=dim), axis, backward)
        block = jnp.concatenate([low, block, high], axis=dim)
    return block


def curl_of(padded):
    centre = padded[:, 1:-1, 1:-1, :]
    grad_x = (padded[:, 2:, 1:-1, :] - padded[:, :-2, 1:-1, :]) * 0.5
    grad_z = (padded[:, 1:-1, 2:, :] - padded[:, 1:-1, :-2, :]) * 0.5
    grad_y = (jnp.roll(centre, -1, 3) - jnp.roll(centre, 1, 3)) * 0.5
    return jnp.stack([grad_y[2] - grad_z[1], grad_z[0] - grad_x[2], grad_x[1] - grad_y[0]])


def cross_parts(lhs, rhs):
    return (
        lhs[1] * rhs[2] - lhs[2] * rhs[1],
        lhs[2] * rhs[0] - lhs[0] * rhs[2],
        lhs[0] * rhs[1] - lhs[1] * rhs[0],
    )


def electric_parts(current, field, resist):
    strength = field[0] * field[0] + field[1] * field[1] + field[2] * field[2] + 1.0
    inverse = 1.0 / (friction * strength)
    velocity = [part * inverse for part in cross_parts(current, field)]
    pushed = cross_parts(velocity, field)
    return [resist * current[c] - pushed[c] for c in range(3)]


def plain_form(b_field, resist, ymix, zmix):
    cells_z = b_field.shape[2]
    total_z = cells_z * lax.axis_size("gz")
    padded = with_halo(b_field, (("gz", 2), ("gx", 1)), 1)
    efield = jnp.stack(electric_parts(curl_of(padded), b_field, resist))
    curl_e = curl_of(with_halo(efield, (("gz", 2), ("gx", 1)), 1))
    stepped = b_field - time_step * curl_e
    along_y = jnp.einsum("cxzi,ij->cxjz", stepped, ymix, precision=lax.Precision.HIGHEST)
    running = jnp.cumsum(zmix, axis=1)
    slab_ends = running[:, cells_z - 1 :: cells_z][:, :-1]
    lower_flux = jnp.concatenate([jnp.zeros((total_z, 1), jnp.float32), slab_ends], axis=1)
    line_matrix = jnp.concatenate([zmix, lower_flux], axis=1)
    product = jnp.einsum(
        "cxym,mk->cxyk",
        lax.all_to_all(along_y, "gz", split_axis=2, concat_axis=3, tiled=True),
        line_matrix,
        precision=lax.Precision.HIGHEST,
    )
    returned, returned_flux = (
        lax.all_to_all(part, "gz", split_axis=3, concat_axis=2, tiled=True)
        for part in (product[..., :total_z], product[..., total_z:])
    )
    b_next = jnp.transpose(returned, (0, 1, 3, 2))
    offset = jnp.transpose(returned_flux, (0, 1, 3, 2))
    column = (jnp.cumsum(b_next, axis=2) + offset) * total_z ** (-0.5)
    return b_next, jnp.stack([column[1], -column[0], column[2]])


def store_tile(ref, part, at, tile):
    count = tile.shape[0] // SHORT
    ref[part, at // SHORT : at // SHORT + count] = tile.reshape(count, SHORT, LANES)


def load_tile(ref, part, at, height):
    return ref[part, at // SHORT : (at + height) // SHORT].reshape(height, LANES)


def one_row(ref, part, at):
    return ref[part, at // SHORT, at % SHORT : at % SHORT + 1, :]


def slope(after, before):
    return (after - before) * 0.5


def along_row(value):
    cells_y = value.shape[1]
    return slope(pltpu.roll(value, cells_y - 1, 1), pltpu.roll(value, 1, 1))


def along_z(value, above, below):
    cells_z = value.shape[0]
    level = lax.broadcasted_iota(jnp.int32, value.shape, 0)
    after = jnp.where(level == cells_z - 1, above, pltpu.roll(value, cells_z - 1, 0))
    before = jnp.where(level == 0, below, pltpu.roll(value, 1, 0))
    return slope(after, before)


def over_x(cells_x, body):
    def trip(i, carry):
        for j in range(BATCH):
            body(i * BATCH + j)
        return carry

    lax.fori_loop(0, cells_x // BATCH, trip, 0)


def pack_kernel(b_ref, place_ref, far_ref, near_ref, side_ref):
    cells_x, cells_z = b_ref.shape[1], b_ref.shape[2]
    edge = jnp.where((place_ref[0] & 1) == 0, cells_x - 1, 0)
    odd = place_ref[0] >= 2
    far_row = jnp.where(odd, cells_z - 1, 0)
    near_row = jnp.where(odd, 0, cells_z - 1)
    for c in range(2):
        side_ref[c] = b_ref[c + 1, edge]
        for x in range(cells_x):
            at = pl.ds(c * cells_x + x, 1)
            far_ref[at, :] = b_ref[c, x, pl.ds(far_row, 1), :]
            near_ref[at, :] = b_ref[c, x, pl.ds(near_row, 1), :]


def x_neighbours(ref, side_ref, first, c, x):
    cells_x = ref.shape[1]
    after = ref[c, jnp.minimum(x + 1, cells_x - 1)]
    before = ref[c, jnp.maximum(x - 1, 0)]
    zero = jnp.zeros_like(after)
    if side_ref is None:
        past_end, past_start = zero, zero
    else:
        side = side_ref[c - 1]
        past_end, past_start = jnp.where(first, side, zero), jnp.where(first, zero, side)
    return (
        jnp.where(x == cells_x - 1, past_end, after),
        jnp.where(x == 0, past_start, before),
    )


def electric_at(b_ref, r_ref, side_ref, far_ref, near_ref, place_ref, x):
    cells_x = b_ref.shape[1]
    odd = place_ref[0] >= 2
    here = [b_ref[c, x] for c in range(3)]
    dz = []
    for c in range(2):
        at = pl.ds(c * cells_x + x, 1)
        far, near = far_ref[at, :], near_ref[at, :]
        dz.append(along_z(here[c], jnp.where(odd, far, near), jnp.where(odd, near, far)))
    first = (place_ref[0] & 1) == 0
    dx = [None] + [slope(*x_neighbours(b_ref, side_ref, first, c, x)) for c in (1, 2)]
    current = (along_row(here[2]) - dz[1], dz[0] - dx[2], dx[1] - along_row(here[0]))
    return electric_parts(current, here, r_ref[x])


def edge_kernel(b_ref, r_ref, side_ref, far_ref, near_ref, place_ref, edge_ref):
    edge = jnp.where((place_ref[0] & 1) == 0, b_ref.shape[1] - 1, 0)
    made = electric_at(b_ref, r_ref, side_ref, far_ref, near_ref, place_ref, edge)
    edge_ref[0], edge_ref[1] = made[1], made[2]


def step_kernel(b_ref, r_ref, side_ref, far_ref, near_ref, place_ref, rows_ref, elec_ref):
    cells_x, cells_z = b_ref.shape[1], b_ref.shape[2]
    half = 0.5 * time_step

    def make(x):
        made = electric_at(b_ref, r_ref, side_ref, far_ref, near_ref, place_ref, x)
        for c in range(3):
            elec_ref[c, x] = made[c]

    def step(x):
        here = [elec_ref[c, x] for c in range(3)]
        dz = [along_z(here[c], 0.0, 0.0) for c in range(2)]
        dx = [None] + [slope(*x_neighbours(elec_ref, None, None, c, x)) for c in (1, 2)]
        curl = (along_row(here[2]) - dz[1], dz[0] - dx[2], dx[1] - along_row(here[0]))
        for c in range(3):
            start = pl.multiple_of((c * cells_x + x) * cells_z, cells_z)
            rows_ref[pl.ds(start, cells_z), :] = b_ref[c, x] - time_step * curl[c]
        extra = 3 * cells_x * cells_z + 4 * x
        rows_ref[pl.ds(extra, 1), :] = half * here[1][:1]
        rows_ref[pl.ds(extra + 1, 1), :] = -half * here[1][cells_z - 1 :]
        rows_ref[pl.ds(extra + 2, 1), :] = -half * here[0][:1]
        rows_ref[pl.ds(extra + 3, 1), :] = half * here[0][cells_z - 1 :]

    over_x(cells_x, make)
    over_x(cells_x, step)


def split(value):
    high = value.astype(jnp.bfloat16)
    return high, (value - high.astype(jnp.float32)).astype(jnp.bfloat16)


def full_dot(lhs, rhs):
    dot = functools.partial(jnp.dot, preferred_element_type=jnp.float32)
    (lhs_high, lhs_low), (rhs_high, rhs_low) = split(lhs), split(rhs)
    return dot(lhs_high, rhs_high) + (dot(lhs_high, rhs_low) + dot(lhs_low, rhs_high))


def mix_kernel(cells_x, cells_z, rows_ref, edge_ref, ymix_ref, place_ref, out_ref, mixed):
    cells_y = rows_ref.shape[1]
    halves = cells_y // LANES
    mixed[...] = full_dot(rows_ref[...], ymix_ref[...])
    first = (place_ref[0] & 1) == 0
    factor = jnp.where(first, 0.5 * time_step, -0.5 * time_step)
    added = full_dot(edge_ref[...].reshape(2 * cells_z, cells_y), ymix_ref[...]) * factor
    edge = jnp.where(first, cells_x - 1, 0)
    for c, term in ((1, added[cells_z:]), (2, -added[:cells_z])):
        at = pl.ds(pl.multiple_of((c * cells_x + edge) * cells_z, cells_z), cells_z)
        mixed[at, :] = mixed[at, :] + term
    pairs = cells_x * halves // out_ref.shape[0]
    extra = 3 * cells_x * cells_z
    for x in range(cells_x):
        for half in range(halves):
            part, q = divmod(x * halves + half, pairs)
            lanes = slice(half * LANES, (half + 1) * LANES)
            for c in range(3):
                at = (q * 3 + c) * cells_z
                line = (c * cells_x + x) * cells_z
                store_tile(out_ref, part, at, mixed[line : line + cells_z, lanes])
            at = pairs * 3 * cells_z + q * 4
            store_tile(out_ref, part, at, mixed[extra + 4 * x : extra + 4 * x + 4, lanes])


def line_matrix_kernel(zmix_ref, out_ref):
    total = zmix_ref.shape[0]
    parts = out_ref.shape[0] - total
    turned = jnp.transpose(zmix_ref[...])
    slab = lax.broadcasted_iota(jnp.int32, (parts, total), 0) * (total // parts)
    lower = (lax.broadcasted_iota(jnp.int32, (parts, total), 1) < slab).astype(jnp.float32)
    out_ref[:total] = turned
    out_ref[total:] = jnp.dot(
        lower, turned, precision=lax.Precision.HIGHEST, preferred_element_type=jnp.float32
    )


def lines_kernel(cells_z, pairs, in_ref, line_ref, out_ref):
    parts = in_ref.shape[0]
    total = parts * cells_z
    height = pairs * 3 * cells_z
    level = lax.broadcasted_iota(jnp.int32, (cells_z, LANES), 0)
    columns = []
    for q in range(pairs):
        for c in range(3):
            at = (q * 3 + c) * cells_z
            tiles = [load_tile(in_ref, s, at, cells_z) for s in range(parts)]
            if c < 2:
                low = height + q * 4 + c * 2
                for s in range(parts):
                    if s < parts - 1:
                        tiles[s] = tiles[s] + jnp.where(
                            level == cells_z - 1, one_row(in_ref, s + 1, low), 0.0
                        )
                    if s > 0:
                        tiles[s] = tiles[s] + jnp.where(
                            level == 0, one_row(in_ref, s - 1, low + 1), 0.0
                        )
            columns.append(jnp.concatenate(tiles, axis=0))
    product = full_dot(line_ref[...], jnp.concatenate(columns, axis=1))
    for g in range(3 * pairs):
        part = product[:, g * LANES : (g + 1) * LANES]
        row = height + g
        for s in range(parts):
            store_tile(out_ref, s, g * cells_z, part[s * cells_z : (s + 1) * cells_z])
            out_ref[s, row // SHORT, row % SHORT : row % SHORT + 1, :] = part[total + s : total + s + 1]


def finish_kernel(scale, cells_z, each, in_ref, next_ref, pot_ref, buffer, sems):
    _, cells_x, _, cells_y = next_ref.shape
    halves = cells_y // LANES
    batch = cells_x // PIECES
    level = lax.broadcasted_iota(jnp.int32, (cells_z, LANES), 0)
    copies = []
    for piece in range(3 * PIECES):
        c, x = divmod(piece * batch, cells_x)
        factor = -scale if c == 0 else scale
        for i in range(batch):
            for half in range(halves):
                part, q = divmod((x + i) * halves + half, each // 3)
                at = q * 3 + c
                tile = load_tile(in_ref, part, at * cells_z, cells_z)
                total, step = tile, 1
                while step < cells_z:
                    total = total + jnp.where(level >= step, pltpu.roll(total, step, 0), 0.0)
                    step *= 2
                offset = one_row(in_ref, part, each * cells_z + at)
                lanes = slice(half * LANES, (half + 1) * LANES)
                buffer[0, piece, i, :, lanes] = tile
                buffer[1, piece, i, :, lanes] = (total + offset) * factor
        for k, (target, ref) in enumerate(((c, next_ref), ((1, 0, 2)[c], pot_ref))):
            copy = pltpu.make_async_copy(
                buffer.at[k, piece], ref.at[target, pl.ds(x, batch)], sems.at[k, piece]
            )
            copy.start()
            copies.append(copy)
    for copy in copies:
        copy.wait()


def limit(mib):
    return pltpu.CompilerParams(vmem_limit_bytes=mib * 2**20)


def kernel_form(b_field, resist, ymix, zmix):
    _, cells_x, cells_z, cells_y = b_field.shape
    parts = lax.axis_size("gz")
    total_z = cells_z * parts
    f32 = jnp.float32
    shape = lambda *sizes: jax.ShapeDtypeStruct(sizes, f32)
    place = (lax.axis_index("gx") + 2 * (lax.axis_index("gz") & 1)).astype(jnp.int32).reshape(1)
    swap = lambda value: lax.ppermute(value, "gx", [(0, 1), (1, 0)])

    far, near, side = pl.pallas_call(
        pack_kernel,
        out_shape=(shape(2 * cells_x, cells_y), shape(2 * cells_x, cells_y), shape(2, cells_z, cells_y)),
        in_specs=[VMEM, SMEM],
        out_specs=(VMEM, VMEM, VMEM),
        compiler_params=limit(6),
    )(b_field, place)
    exchange = lambda value, low: lax.ppermute(
        value,
        "gz",
        [pair for i in range(low, parts - 1, 2) for pair in ((i, i + 1), (i + 1, i))],
    )
    far, near = exchange(far, 1), exchange(near, 0)
    line = pl.pallas_call(
        line_matrix_kernel,
        out_shape=shape(total_z + parts, total_z),
        in_specs=[VMEM],
        out_specs=VMEM,
        compiler_params=limit(4),
    )(zmix)
    line, far = lax.optimization_barrier((line, far))
    known = (b_field, resist, swap(side), far, near, place)
    edge = pl.pallas_call(
        edge_kernel,
        out_shape=shape(2, cells_z, cells_y),
        in_specs=[VMEM] * 5 + [SMEM],
        out_specs=VMEM,
        compiler_params=limit(6),
    )(*known)
    rows = pl.pallas_call(
        step_kernel,
        out_shape=shape(3 * cells_x * cells_z + 4 * cells_x, cells_y),
        in_specs=[VMEM] * 5 + [SMEM],
        out_specs=VMEM,
        scratch_shapes=[pltpu.VMEM(b_field.shape, f32)],
        compiler_params=limit(6),
        cost_estimate=estimate(400.0 * b_field.size),
    )(*known)
    pairs = cells_x * (cells_y // LANES) // parts
    sent = pl.pallas_call(
        functools.partial(mix_kernel, cells_x, cells_z),
        out_shape=shape(parts, pairs * (3 * cells_z + 4) // SHORT, SHORT, LANES),
        in_specs=[VMEM] * 3 + [SMEM],
        out_specs=VMEM,
        scratch_shapes=[pltpu.VMEM(rows.shape, f32)],
        compiler_params=limit(6),
    )(rows, swap(edge), ymix, place)
    lines = lax.all_to_all(sent, "gz", split_axis=0, concat_axis=0, tiled=True)
    product = pl.pallas_call(
        functools.partial(lines_kernel, cells_z, pairs),
        out_shape=shape(parts, -(-pairs * 3 * (cells_z + 1) // SHORT), SHORT, LANES),
        in_specs=[VMEM, VMEM],
        out_specs=VMEM,
        compiler_params=limit(6),
    )(lines, line)
    returned = lax.all_to_all(product, "gz", split_axis=0, concat_axis=0, tiled=True)
    whole = jax.ShapeDtypeStruct(b_field.shape, f32)
    hbm = pl.BlockSpec(memory_space=pl.ANY)
    return pl.pallas_call(
        functools.partial(finish_kernel, total_z ** (-0.5), cells_z, 3 * pairs),
        out_shape=(whole, whole),
        in_specs=[VMEM],
        out_specs=(hbm, hbm),
        scratch_shapes=[
            pltpu.VMEM((2, 3 * PIECES, cells_x // PIECES, cells_z, cells_y), f32),
            pltpu.SemaphoreType.DMA((2, 3 * PIECES)),
        ],
        compiler_params=limit(6),
    )(returned)


def estimate(flops):
    return pl.CostEstimate(flops=int(flops), bytes_accessed=0, transcendentals=0)


def on_device(b_field, resist, ymix, zmix):
    _, cells_x, cells_z, cells_y = b_field.shape
    parts = lax.axis_size("gz")
    fits = (
        lax.axis_size("gx") == 2
        and parts > 1
        and cells_z == SUBLANES
        and cells_x % PIECES == 0
        and cells_y % LANES == 0
        and cells_x % BATCH == 0
        and cells_x * (cells_y // LANES) % parts == 0
    )
    return (kernel_form if fits else plain_form)(b_field, resist, ymix, zmix)


def solution(mesh):
    in_specs = (P(None, "gx", "gz", None), P("gx", "gz", None), P(), P())
    out_specs = (P(None, "gx", "gz", None), P(None, "gx", "gz", None))
    return jax.shard_map(
        on_device, mesh=mesh, in_specs=in_specs, out_specs=out_specs, check_vma=False
    )
```

```python
import functools
import jax
import jax.numpy as jnp
from jax import lax
from jax.experimental import pallas as pl
from jax.experimental.pallas import tpu as pltpu
from jax.sharding import PartitionSpec as P

time_step = 0.1
friction = 1.0
LANES = 128
SUBLANES = 8
SHORT = 4
PIECES = 3
BATCH = 11
VMEM = pl.BlockSpec(memory_space=pltpu.VMEM)
SMEM = pl.BlockSpec(memory_space=pltpu.SMEM)


def with_halo(block, sides, width):
    for axis, dim in sides:
        count = lax.axis_size(axis)
        forward = [(i, i + 1) for i in range(count - 1)]
        backward = [(target, source) for source, target in forward]
        low = lax.ppermute(
            lax.slice_in_dim(block, block.shape[dim] - width, None, axis=dim), axis, forward
        )
        high = lax.ppermute(lax.slice_in_dim(block, 0, width, axis=dim), axis, backward)
        block = jnp.concatenate([low, block, high], axis=dim)
    return block


def curl_of(padded):
    centre = padded[:, 1:-1, 1:-1, :]
    grad_x = (padded[:, 2:, 1:-1, :] - padded[:, :-2, 1:-1, :]) * 0.5
    grad_z = (padded[:, 1:-1, 2:, :] - padded[:, 1:-1, :-2, :]) * 0.5
    grad_y = (jnp.roll(centre, -1, 3) - jnp.roll(centre, 1, 3)) * 0.5
    return jnp.stack([grad_y[2] - grad_z[1], grad_z[0] - grad_x[2], grad_x[1] - grad_y[0]])


def cross_parts(lhs, rhs):
    return (
        lhs[1] * rhs[2] - lhs[2] * rhs[1],
        lhs[2] * rhs[0] - lhs[0] * rhs[2],
        lhs[0] * rhs[1] - lhs[1] * rhs[0],
    )


def electric_parts(current, field, resist):
    strength = field[0] * field[0] + field[1] * field[1] + field[2] * field[2] + 1.0
    inverse = 1.0 / (friction * strength)
    velocity = [part * inverse for part in cross_parts(current, field)]
    pushed = cross_parts(velocity, field)
    return [resist * current[c] - pushed[c] for c in range(3)]


def plain_form(b_field, resist, ymix, zmix):
    cells_z = b_field.shape[2]
    total_z = cells_z * lax.axis_size("gz")
    padded = with_halo(b_field, (("gz", 2), ("gx", 1)), 1)
    efield = jnp.stack(electric_parts(curl_of(padded), b_field, resist))
    curl_e = curl_of(with_halo(efield, (("gz", 2), ("gx", 1)), 1))
    stepped = b_field - time_step * curl_e
    along_y = jnp.einsum("cxzi,ij->cxjz", stepped, ymix, precision=lax.Precision.HIGHEST)
    running = jnp.cumsum(zmix, axis=1)
    slab_ends = running[:, cells_z - 1 :: cells_z][:, :-1]
    lower_flux = jnp.concatenate([jnp.zeros((total_z, 1), jnp.float32), slab_ends], axis=1)
    line_matrix = jnp.concatenate([zmix, lower_flux], axis=1)
    product = jnp.einsum(
        "cxym,mk->cxyk",
        lax.all_to_all(along_y, "gz", split_axis=2, concat_axis=3, tiled=True),
        line_matrix,
        precision=lax.Precision.HIGHEST,
    )
    returned, returned_flux = (
        lax.all_to_all(part, "gz", split_axis=3, concat_axis=2, tiled=True)
        for part in (product[..., :total_z], product[..., total_z:])
    )
    b_next = jnp.transpose(returned, (0, 1, 3, 2))
    offset = jnp.transpose(returned_flux, (0, 1, 3, 2))
    column = (jnp.cumsum(b_next, axis=2) + offset) * total_z ** (-0.5)
    return b_next, jnp.stack([column[1], -column[0], column[2]])


def store_tile(ref, part, at, tile):
    count = tile.shape[0] // SHORT
    ref[part, at // SHORT : at // SHORT + count] = tile.reshape(count, SHORT, LANES)


def load_tile(ref, part, at, height):
    return ref[part, at // SHORT : (at + height) // SHORT].reshape(height, LANES)


def one_row(ref, part, at):
    return ref[part, at // SHORT, at % SHORT : at % SHORT + 1, :]


def slope(after, before):
    return (after - before) * 0.5


def along_row(value):
    cells_y = value.shape[1]
    return slope(pltpu.roll(value, cells_y - 1, 1), pltpu.roll(value, 1, 1))


def along_z(value, above, below):
    cells_z = value.shape[0]
    level = lax.broadcasted_iota(jnp.int32, value.shape, 0)
    after = jnp.where(level == cells_z - 1, above, pltpu.roll(value, cells_z - 1, 0))
    before = jnp.where(level == 0, below, pltpu.roll(value, 1, 0))
    return slope(after, before)


def over_x(cells_x, body):
    batch = next(size for size in range(BATCH, 0, -1) if (cells_x - 2) % size == 0)

    def trip(i, carry):
        for j in range(batch):
            body(1 + i * batch + j)
        return carry

    lax.fori_loop(0, (cells_x - 2) // batch, trip, 0)
    body(0)
    body(cells_x - 1)


def pack_kernel(b_ref, place_ref, far_ref, near_ref, side_ref, held, sems):
    cells_x, cells_z = b_ref.shape[1], b_ref.shape[2]
    edge = jnp.where((place_ref[0] & 1) == 0, cells_x - 1, 0)
    odd = place_ref[0] >= 2
    far_row = jnp.where(odd, cells_z - 1, 0)
    near_row = jnp.where(odd, 0, cells_z - 1)
    batch = cells_x // PIECES
    copies = [
        pltpu.make_async_copy(
            b_ref.at[c, pl.ds(i * batch, batch)], held.at[c, pl.ds(i * batch, batch)], sems.at[c, i]
        )
        for c in range(2)
        for i in range(PIECES)
    ]
    copies.append(pltpu.make_async_copy(b_ref.at[pl.ds(1, 2), edge], side_ref, sems.at[2, 0]))
    for copy in copies:
        copy.start()
    for copy in copies:
        copy.wait()
    for c in range(2):
        for x in range(cells_x):
            at = pl.ds(c * cells_x + x, 1)
            far_ref[at, :] = held[c, x, pl.ds(far_row, 1), :]
            near_ref[at, :] = held[c, x, pl.ds(near_row, 1), :]


def x_slope(ref, side_ref, first, c, x):
    last = ref.shape[1] - 1

    def beyond(mine):
        if side_ref is None:
            return 0.0
        return jnp.where(mine, side_ref[c - 1], 0.0)

    if isinstance(x, int) and x == 0:
        return slope(ref[c, 1], beyond(jnp.logical_not(first) if side_ref is not None else None))
    if isinstance(x, int) and x == last:
        return slope(beyond(first), ref[c, last - 1])
    return slope(ref[c, x + 1], ref[c, x - 1])


def electric_at(b_ref, r_ref, side_ref, far_ref, near_ref, place_ref, x):
    cells_x = b_ref.shape[1]
    odd = place_ref[0] >= 2
    here = [b_ref[c, x] for c in range(3)]
    dz = []
    for c in range(2):
        at = pl.ds(c * cells_x + x, 1)
        far, near = far_ref[at, :], near_ref[at, :]
        dz.append(along_z(here[c], jnp.where(odd, far, near), jnp.where(odd, near, far)))
    first = (place_ref[0] & 1) == 0
    dx = [None] + [x_slope(b_ref, side_ref, first, c, x) for c in (1, 2)]
    current = (along_row(here[2]) - dz[1], dz[0] - dx[2], dx[1] - along_row(here[0]))
    return electric_parts(current, here, r_ref[x])


def edge_kernel(b_ref, r_ref, side_ref, far_ref, near_ref, place_ref, edge_ref):
    known = (b_ref, r_ref, side_ref, far_ref, near_ref, place_ref)
    low, high = electric_at(*known, 0), electric_at(*known, b_ref.shape[1] - 1)
    first = (place_ref[0] & 1) == 0
    for c in range(2):
        edge_ref[c] = jnp.where(first, high[c + 1], low[c + 1])


def step_kernel(b_ref, r_ref, side_ref, far_ref, near_ref, place_ref, rows_ref, elec_ref):
    cells_x, cells_z = b_ref.shape[1], b_ref.shape[2]
    half = 0.5 * time_step

    def make(x):
        made = electric_at(b_ref, r_ref, side_ref, far_ref, near_ref, place_ref, x)
        for c in range(3):
            elec_ref[c, x] = made[c]

    def step(x):
        here = [elec_ref[c, x] for c in range(3)]
        dz = [along_z(here[c], 0.0, 0.0) for c in range(2)]
        dx = [None] + [x_slope(elec_ref, None, None, c, x) for c in (1, 2)]
        curl = (along_row(here[2]) - dz[1], dz[0] - dx[2], dx[1] - along_row(here[0]))
        for c in range(3):
            start = pl.multiple_of((c * cells_x + x) * cells_z, cells_z)
            rows_ref[pl.ds(start, cells_z), :] = b_ref[c, x] - time_step * curl[c]
        extra = 3 * cells_x * cells_z + 4 * x
        rows_ref[pl.ds(extra, 1), :] = half * here[1][:1]
        rows_ref[pl.ds(extra + 1, 1), :] = -half * here[1][cells_z - 1 :]
        rows_ref[pl.ds(extra + 2, 1), :] = -half * here[0][:1]
        rows_ref[pl.ds(extra + 3, 1), :] = half * here[0][cells_z - 1 :]

    over_x(cells_x, make)
    over_x(cells_x, step)


def split(value):
    high = value.astype(jnp.bfloat16)
    return high, (value - high.astype(jnp.float32)).astype(jnp.bfloat16)


def full_dot(lhs, rhs):
    dot = functools.partial(jnp.dot, preferred_element_type=jnp.float32)
    (lhs_high, lhs_low), (rhs_high, rhs_low) = split(lhs), split(rhs)
    return dot(lhs_high, rhs_high) + (dot(lhs_high, rhs_low) + dot(lhs_low, rhs_high))


def mix_kernel(cells_x, cells_z, rows_ref, edge_ref, ymix_ref, place_ref, out_ref, mixed):
    cells_y = rows_ref.shape[1]
    halves = cells_y // LANES
    mixed[...] = full_dot(rows_ref[...], ymix_ref[...])
    first = (place_ref[0] & 1) == 0
    factor = jnp.where(first, 0.5 * time_step, -0.5 * time_step)
    added = full_dot(edge_ref[...].reshape(2 * cells_z, cells_y), ymix_ref[...]) * factor
    edge = jnp.where(first, cells_x - 1, 0)
    for c, term in ((1, added[cells_z:]), (2, -added[:cells_z])):
        at = pl.ds(pl.multiple_of((c * cells_x + edge) * cells_z, cells_z), cells_z)
        mixed[at, :] = mixed[at, :] + term
    pairs = cells_x * halves // out_ref.shape[0]
    extra = 3 * cells_x * cells_z
    for x in range(cells_x):
        for half in range(halves):
            part, q = divmod(x * halves + half, pairs)
            lanes = slice(half * LANES, (half + 1) * LANES)
            for c in range(3):
                at = (q * 3 + c) * cells_z
                line = (c * cells_x + x) * cells_z
                store_tile(out_ref, part, at, mixed[line : line + cells_z, lanes])
            at = pairs * 3 * cells_z + q * 4
            store_tile(out_ref, part, at, mixed[extra + 4 * x : extra + 4 * x + 4, lanes])


def line_matrix_kernel(zmix_ref, out_ref):
    total = zmix_ref.shape[0]
    parts = out_ref.shape[0] - total
    turned = jnp.transpose(zmix_ref[...])
    slab = lax.broadcasted_iota(jnp.int32, (parts, total), 0) * (total // parts)
    lower = (lax.broadcasted_iota(jnp.int32, (parts, total), 1) < slab).astype(jnp.float32)
    out_ref[:total] = turned
    out_ref[total:] = jnp.dot(
        lower, turned, precision=lax.Precision.HIGHEST, preferred_element_type=jnp.float32
    )


def lines_kernel(cells_z, pairs, in_ref, line_ref, out_ref):
    parts = in_ref.shape[0]
    total = parts * cells_z
    height = pairs * 3 * cells_z
    level = lax.broadcasted_iota(jnp.int32, (cells_z, LANES), 0)
    columns = []
    for q in range(pairs):
        for c in range(3):
            at = (q * 3 + c) * cells_z
            tiles = [load_tile(in_ref, s, at, cells_z) for s in range(parts)]
            if c < 2:
                low = height + q * 4 + c * 2
                for s in range(parts):
                    if s < parts - 1:
                        tiles[s] = tiles[s] + jnp.where(
                            level == cells_z - 1, one_row(in_ref, s + 1, low), 0.0
                        )
                    if s > 0:
                        tiles[s] = tiles[s] + jnp.where(
                            level == 0, one_row(in_ref, s - 1, low + 1), 0.0
                        )
            columns.append(jnp.concatenate(tiles, axis=0))
    product = full_dot(line_ref[...], jnp.concatenate(columns, axis=1))
    for g in range(3 * pairs):
        part = product[:, g * LANES : (g + 1) * LANES]
        row = height + g
        for s in range(parts):
            store_tile(out_ref, s, g * cells_z, part[s * cells_z : (s + 1) * cells_z])
            out_ref[s, row // SHORT, row % SHORT : row % SHORT + 1, :] = part[total + s : total + s + 1]


def finish_kernel(scale, cells_z, each, in_ref, next_ref, pot_ref, buffer, sems):
    _, cells_x, _, cells_y = next_ref.shape
    halves = cells_y // LANES
    batch = cells_x // PIECES
    level = lax.broadcasted_iota(jnp.int32, (cells_z, LANES), 0)
    copies = []
    for piece in range(3 * PIECES):
        c, x = divmod(piece * batch, cells_x)
        factor = -scale if c == 0 else scale
        for i in range(batch):
            for half in range(halves):
                part, q = divmod((x + i) * halves + half, each // 3)
                at = q * 3 + c
                tile = load_tile(in_ref, part, at * cells_z, cells_z)
                total, step = tile, 1
                while step < cells_z:
                    total = total + jnp.where(level >= step, pltpu.roll(total, step, 0), 0.0)
                    step *= 2
                offset = one_row(in_ref, part, each * cells_z + at)
                lanes = slice(half * LANES, (half + 1) * LANES)
                buffer[0, piece, i, :, lanes] = tile
                buffer[1, piece, i, :, lanes] = (total + offset) * factor
        for k, (target, ref) in enumerate(((c, next_ref), ((1, 0, 2)[c], pot_ref))):
            copy = pltpu.make_async_copy(
                buffer.at[k, piece], ref.at[target, pl.ds(x, batch)], sems.at[k, piece]
            )
            copy.start()
            copies.append(copy)
    for copy in copies:
        copy.wait()


def limit(mib):
    return pltpu.CompilerParams(vmem_limit_bytes=mib * 2**20)


def kernel_form(b_field, resist, ymix, zmix):
    _, cells_x, cells_z, cells_y = b_field.shape
    parts = lax.axis_size("gz")
    total_z = cells_z * parts
    f32 = jnp.float32
    shape = lambda *sizes: jax.ShapeDtypeStruct(sizes, f32)
    place = (lax.axis_index("gx") + 2 * (lax.axis_index("gz") & 1)).astype(jnp.int32).reshape(1)
    swap = lambda value: lax.ppermute(value, "gx", [(0, 1), (1, 0)])

    far, near, side = pl.pallas_call(
        pack_kernel,
        out_shape=(shape(2 * cells_x, cells_y), shape(2 * cells_x, cells_y), shape(2, cells_z, cells_y)),
        in_specs=[pl.BlockSpec(memory_space=pltpu.HBM), SMEM],
        out_specs=(VMEM, VMEM, VMEM),
        scratch_shapes=[
            pltpu.VMEM((2,) + b_field.shape[1:], f32),
            pltpu.SemaphoreType.DMA((3, PIECES)),
        ],
        compiler_params=limit(6),
    )(pltpu.with_memory_space_constraint(b_field, pltpu.HBM), place)
    exchange = lambda value, low: lax.ppermute(
        value,
        "gz",
        [pair for i in range(low, parts - 1, 2) for pair in ((i, i + 1), (i + 1, i))],
    )
    far, near = exchange(far, 1), exchange(near, 0)
    line = pl.pallas_call(
        line_matrix_kernel,
        out_shape=shape(total_z + parts, total_z),
        in_specs=[VMEM],
        out_specs=VMEM,
        compiler_params=limit(4),
    )(zmix)
    line, far = lax.optimization_barrier((line, far))
    known = (b_field, resist, swap(side), far, near, place)
    edge = pl.pallas_call(
        edge_kernel,
        out_shape=shape(2, cells_z, cells_y),
        in_specs=[VMEM] * 5 + [SMEM],
        out_specs=VMEM,
        compiler_params=limit(6),
    )(*known)
    rows = pl.pallas_call(
        step_kernel,
        out_shape=shape(3 * cells_x * cells_z + 4 * cells_x, cells_y),
        in_specs=[VMEM] * 5 + [SMEM],
        out_specs=VMEM,
        scratch_shapes=[pltpu.VMEM(b_field.shape, f32)],
        compiler_params=limit(6),
        cost_estimate=estimate(400.0 * b_field.size),
    )(*known)
    pairs = cells_x * (cells_y // LANES) // parts
    sent = pl.pallas_call(
        functools.partial(mix_kernel, cells_x, cells_z),
        out_shape=shape(parts, pairs * (3 * cells_z + 4) // SHORT, SHORT, LANES),
        in_specs=[VMEM] * 3 + [SMEM],
        out_specs=VMEM,
        scratch_shapes=[pltpu.VMEM(rows.shape, f32)],
        compiler_params=limit(6),
    )(rows, swap(edge), ymix, place)
    lines = lax.all_to_all(sent, "gz", split_axis=0, concat_axis=0, tiled=True)
    product = pl.pallas_call(
        functools.partial(lines_kernel, cells_z, pairs),
        out_shape=shape(parts, -(-pairs * 3 * (cells_z + 1) // SHORT), SHORT, LANES),
        in_specs=[VMEM, VMEM],
        out_specs=VMEM,
        compiler_params=limit(6),
    )(lines, line)
    returned = lax.all_to_all(product, "gz", split_axis=0, concat_axis=0, tiled=True)
    whole = jax.ShapeDtypeStruct(b_field.shape, f32)
    hbm = pl.BlockSpec(memory_space=pl.ANY)
    return pl.pallas_call(
        functools.partial(finish_kernel, total_z ** (-0.5), cells_z, 3 * pairs),
        out_shape=(whole, whole),
        in_specs=[VMEM],
        out_specs=(hbm, hbm),
        scratch_shapes=[
            pltpu.VMEM((2, 3 * PIECES, cells_x // PIECES, cells_z, cells_y), f32),
            pltpu.SemaphoreType.DMA((2, 3 * PIECES)),
        ],
        compiler_params=limit(6),
    )(returned)


def estimate(flops):
    return pl.CostEstimate(flops=int(flops), bytes_accessed=0, transcendentals=0)


def on_device(b_field, resist, ymix, zmix):
    _, cells_x, cells_z, cells_y = b_field.shape
    parts = lax.axis_size("gz")
    fits = (
        lax.axis_size("gx") == 2
        and parts > 1
        and cells_z == SUBLANES
        and cells_x % PIECES == 0
        and cells_y % LANES == 0
        and cells_x >= 4
        and cells_x * (cells_y // LANES) % parts == 0
    )
    return (kernel_form if fits else plain_form)(b_field, resist, ymix, zmix)


def solution(mesh):
    in_specs = (P(None, "gx", "gz", None), P("gx", "gz", None), P(), P())
    out_specs = (P(None, "gx", "gz", None), P(None, "gx", "gz", None))
    return jax.shard_map(
        on_device, mesh=mesh, in_specs=in_specs, out_specs=out_specs, check_vma=False
    )
```

```python
import functools
import jax
import jax.numpy as jnp
from jax import lax
from jax.experimental import pallas as pl
from jax.experimental.pallas import tpu as pltpu
from jax.sharding import PartitionSpec as P

time_step = 0.1
friction = 1.0
LANES = 128
SUBLANES = 8
SHORT = 4
PIECES = 6
BATCH = 11
VMEM = pl.BlockSpec(memory_space=pltpu.VMEM)
SMEM = pl.BlockSpec(memory_space=pltpu.SMEM)


def with_halo(block, sides, width):
    for axis, dim in sides:
        count = lax.axis_size(axis)
        forward = [(i, i + 1) for i in range(count - 1)]
        backward = [(target, source) for source, target in forward]
        low = lax.ppermute(
            lax.slice_in_dim(block, block.shape[dim] - width, None, axis=dim), axis, forward
        )
        high = lax.ppermute(lax.slice_in_dim(block, 0, width, axis=dim), axis, backward)
        block = jnp.concatenate([low, block, high], axis=dim)
    return block


def curl_of(padded):
    centre = padded[:, 1:-1, 1:-1, :]
    grad_x = (padded[:, 2:, 1:-1, :] - padded[:, :-2, 1:-1, :]) * 0.5
    grad_z = (padded[:, 1:-1, 2:, :] - padded[:, 1:-1, :-2, :]) * 0.5
    grad_y = (jnp.roll(centre, -1, 3) - jnp.roll(centre, 1, 3)) * 0.5
    return jnp.stack([grad_y[2] - grad_z[1], grad_z[0] - grad_x[2], grad_x[1] - grad_y[0]])


def cross_parts(lhs, rhs):
    return (
        lhs[1] * rhs[2] - lhs[2] * rhs[1],
        lhs[2] * rhs[0] - lhs[0] * rhs[2],
        lhs[0] * rhs[1] - lhs[1] * rhs[0],
    )


def electric_parts(current, field, resist):
    strength = field[0] * field[0] + field[1] * field[1] + field[2] * field[2] + 1.0
    inverse = 1.0 / (friction * strength)
    velocity = [part * inverse for part in cross_parts(current, field)]
    pushed = cross_parts(velocity, field)
    return [resist * current[c] - pushed[c] for c in range(3)]


def plain_form(b_field, resist, ymix, zmix):
    cells_z = b_field.shape[2]
    total_z = cells_z * lax.axis_size("gz")
    padded = with_halo(b_field, (("gz", 2), ("gx", 1)), 1)
    efield = jnp.stack(electric_parts(curl_of(padded), b_field, resist))
    curl_e = curl_of(with_halo(efield, (("gz", 2), ("gx", 1)), 1))
    stepped = b_field - time_step * curl_e
    along_y = jnp.einsum("cxzi,ij->cxjz", stepped, ymix, precision=lax.Precision.HIGHEST)
    running = jnp.cumsum(zmix, axis=1)
    slab_ends = running[:, cells_z - 1 :: cells_z][:, :-1]
    lower_flux = jnp.concatenate([jnp.zeros((total_z, 1), jnp.float32), slab_ends], axis=1)
    line_matrix = jnp.concatenate([zmix, lower_flux], axis=1)
    product = jnp.einsum(
        "cxym,mk->cxyk",
        lax.all_to_all(along_y, "gz", split_axis=2, concat_axis=3, tiled=True),
        line_matrix,
        precision=lax.Precision.HIGHEST,
    )
    returned, returned_flux = (
        lax.all_to_all(part, "gz", split_axis=3, concat_axis=2, tiled=True)
        for part in (product[..., :total_z], product[..., total_z:])
    )
    b_next = jnp.transpose(returned, (0, 1, 3, 2))
    offset = jnp.transpose(returned_flux, (0, 1, 3, 2))
    column = (jnp.cumsum(b_next, axis=2) + offset) * total_z ** (-0.5)
    return b_next, jnp.stack([column[1], -column[0], column[2]])


def store_tile(ref, part, at, tile):
    count = tile.shape[0] // SHORT
    ref[part, at // SHORT : at // SHORT + count] = tile.reshape(count, SHORT, LANES)


def load_tile(ref, part, at, height):
    return ref[part, at // SHORT : (at + height) // SHORT].reshape(height, LANES)


def one_row(ref, part, at):
    return ref[part, at // SHORT, at % SHORT : at % SHORT + 1, :]


def slope(after, before):
    return (after - before) * 0.5


def along_row(value):
    cells_y = value.shape[1]
    return slope(pltpu.roll(value, cells_y - 1, 1), pltpu.roll(value, 1, 1))


def along_z(value, above, below):
    cells_z = value.shape[0]
    level = lax.broadcasted_iota(jnp.int32, value.shape, 0)
    after = jnp.where(level == cells_z - 1, above, pltpu.roll(value, cells_z - 1, 0))
    before = jnp.where(level == 0, below, pltpu.roll(value, 1, 0))
    return slope(after, before)


def over_x(cells_x, body):
    batch = next(size for size in range(BATCH, 0, -1) if (cells_x - 2) % size == 0)

    def trip(i, carry):
        for j in range(batch):
            body(1 + i * batch + j)
        return carry

    lax.fori_loop(0, (cells_x - 2) // batch, trip, 0)
    body(0)
    body(cells_x - 1)


def pack_kernel(b_ref, place_ref, far_ref, near_ref, side_ref):
    cells_x, cells_z = b_ref.shape[1], b_ref.shape[2]
    edge = jnp.where((place_ref[0] & 1) == 0, cells_x - 1, 0)
    odd = place_ref[0] >= 2
    far_row = jnp.where(odd, cells_z - 1, 0)
    near_row = jnp.where(odd, 0, cells_z - 1)
    for c in range(2):
        side_ref[c] = b_ref[c + 1, edge]
        for x in range(cells_x):
            at = pl.ds(c * cells_x + x, 1)
            far_ref[at, :] = b_ref[c, x, pl.ds(far_row, 1), :]
            near_ref[at, :] = b_ref[c, x, pl.ds(near_row, 1), :]


def x_slope(ref, side_ref, first, c, x):
    last = ref.shape[1] - 1

    def beyond(mine):
        if side_ref is None:
            return 0.0
        return jnp.where(mine, side_ref[c - 1], 0.0)

    if isinstance(x, int) and x == 0:
        return slope(ref[c, 1], beyond(jnp.logical_not(first) if side_ref is not None else None))
    if isinstance(x, int) and x == last:
        return slope(beyond(first), ref[c, last - 1])
    return slope(ref[c, x + 1], ref[c, x - 1])


def electric_at(b_ref, r_ref, side_ref, far_ref, near_ref, place_ref, x):
    cells_x = b_ref.shape[1]
    odd = place_ref[0] >= 2
    here = [b_ref[c, x] for c in range(3)]
    dz = []
    for c in range(2):
        at = pl.ds(c * cells_x + x, 1)
        far, near = far_ref[at, :], near_ref[at, :]
        dz.append(along_z(here[c], jnp.where(odd, far, near), jnp.where(odd, near, far)))
    first = (place_ref[0] & 1) == 0
    dx = [None] + [x_slope(b_ref, side_ref, first, c, x) for c in (1, 2)]
    current = (along_row(here[2]) - dz[1], dz[0] - dx[2], dx[1] - along_row(here[0]))
    return electric_parts(current, here, r_ref[x])


def edge_kernel(b_ref, r_ref, side_ref, far_ref, near_ref, place_ref, edge_ref):
    known = (b_ref, r_ref, side_ref, far_ref, near_ref, place_ref)
    low, high = electric_at(*known, 0), electric_at(*known, b_ref.shape[1] - 1)
    first = (place_ref[0] & 1) == 0
    for c in range(2):
        edge_ref[c] = jnp.where(first, high[c + 1], low[c + 1])


def step_kernel(b_ref, r_ref, side_ref, far_ref, near_ref, place_ref, rows_ref, elec_ref):
    cells_x, cells_z = b_ref.shape[1], b_ref.shape[2]
    half = 0.5 * time_step

    def make(x):
        made = electric_at(b_ref, r_ref, side_ref, far_ref, near_ref, place_ref, x)
        for c in range(3):
            elec_ref[c, x] = made[c]

    def step(x):
        here = [elec_ref[c, x] for c in range(3)]
        dz = [along_z(here[c], 0.0, 0.0) for c in range(2)]
        dx = [None] + [x_slope(elec_ref, None, None, c, x) for c in (1, 2)]
        curl = (along_row(here[2]) - dz[1], dz[0] - dx[2], dx[1] - along_row(here[0]))
        for c in range(3):
            start = pl.multiple_of((c * cells_x + x) * cells_z, cells_z)
            rows_ref[pl.ds(start, cells_z), :] = b_ref[c, x] - time_step * curl[c]
        extra = 3 * cells_x * cells_z + 4 * x
        rows_ref[pl.ds(extra, 1), :] = half * here[1][:1]
        rows_ref[pl.ds(extra + 1, 1), :] = -half * here[1][cells_z - 1 :]
        rows_ref[pl.ds(extra + 2, 1), :] = -half * here[0][:1]
        rows_ref[pl.ds(extra + 3, 1), :] = half * here[0][cells_z - 1 :]

    over_x(cells_x, make)
    over_x(cells_x, step)


def split(value):
    high = value.astype(jnp.bfloat16)
    return high, (value - high.astype(jnp.float32)).astype(jnp.bfloat16)


def full_dot(lhs, rhs):
    dot = functools.partial(jnp.dot, preferred_element_type=jnp.float32)
    (lhs_high, lhs_low), (rhs_high, rhs_low) = split(lhs), split(rhs)
    return dot(lhs_high, rhs_high) + (dot(lhs_high, rhs_low) + dot(lhs_low, rhs_high))


def mix_kernel(cells_x, cells_z, rows_ref, edge_ref, ymix_ref, place_ref, out_ref, mixed):
    cells_y = rows_ref.shape[1]
    halves = cells_y // LANES
    mixed[...] = full_dot(rows_ref[...], ymix_ref[...])
    first = (place_ref[0] & 1) == 0
    factor = jnp.where(first, 0.5 * time_step, -0.5 * time_step)
    added = full_dot(edge_ref[...].reshape(2 * cells_z, cells_y), ymix_ref[...]) * factor
    edge = jnp.where(first, cells_x - 1, 0)
    for c, term in ((1, added[cells_z:]), (2, -added[:cells_z])):
        at = pl.ds(pl.multiple_of((c * cells_x + edge) * cells_z, cells_z), cells_z)
        mixed[at, :] = mixed[at, :] + term
    pairs = cells_x * halves // out_ref.shape[0]
    extra = 3 * cells_x * cells_z
    for x in range(cells_x):
        for half in range(halves):
            part, q = divmod(x * halves + half, pairs)
            lanes = slice(half * LANES, (half + 1) * LANES)
            for c in range(3):
                at = (q * 3 + c) * cells_z
                line = (c * cells_x + x) * cells_z
                store_tile(out_ref, part, at, mixed[line : line + cells_z, lanes])
            at = pairs * 3 * cells_z + q * 4
            store_tile(out_ref, part, at, mixed[extra + 4 * x : extra + 4 * x + 4, lanes])


def line_matrix_kernel(zmix_ref, out_ref):
    total = zmix_ref.shape[0]
    parts = out_ref.shape[0] - total
    turned = jnp.transpose(zmix_ref[...])
    slab = lax.broadcasted_iota(jnp.int32, (parts, total), 0) * (total // parts)
    lower = (lax.broadcasted_iota(jnp.int32, (parts, total), 1) < slab).astype(jnp.float32)
    out_ref[:total] = turned
    out_ref[total:] = jnp.dot(
        lower, turned, precision=lax.Precision.HIGHEST, preferred_element_type=jnp.float32
    )


def lines_kernel(cells_z, pairs, in_ref, line_ref, out_ref):
    parts = in_ref.shape[0]
    total = parts * cells_z
    height = pairs * 3 * cells_z
    level = lax.broadcasted_iota(jnp.int32, (cells_z, LANES), 0)
    columns = []
    for q in range(pairs):
        for c in range(3):
            at = (q * 3 + c) * cells_z
            tiles = [load_tile(in_ref, s, at, cells_z) for s in range(parts)]
            if c < 2:
                low = height + q * 4 + c * 2
                for s in range(parts):
                    if s < parts - 1:
                        tiles[s] = tiles[s] + jnp.where(
                            level == cells_z - 1, one_row(in_ref, s + 1, low), 0.0
                        )
                    if s > 0:
                        tiles[s] = tiles[s] + jnp.where(
                            level == 0, one_row(in_ref, s - 1, low + 1), 0.0
                        )
            columns.append(jnp.concatenate(tiles, axis=0))
    product = full_dot(line_ref[...], jnp.concatenate(columns, axis=1))
    for g in range(3 * pairs):
        part = product[:, g * LANES : (g + 1) * LANES]
        row = height + g
        for s in range(parts):
            store_tile(out_ref, s, g * cells_z, part[s * cells_z : (s + 1) * cells_z])
            out_ref[s, row // SHORT, row % SHORT : row % SHORT + 1, :] = part[total + s : total + s + 1]


def finish_kernel(scale, cells_z, each, in_ref, next_ref, pot_ref, buffer, sems):
    _, cells_x, _, cells_y = next_ref.shape
    halves = cells_y // LANES
    batch = cells_x // PIECES
    level = lax.broadcasted_iota(jnp.int32, (cells_z, LANES), 0)
    copies = []
    for piece in range(3 * PIECES):
        c, x = divmod(piece * batch, cells_x)
        factor = -scale if c == 0 else scale
        for i in range(batch):
            for half in range(halves):
                part, q = divmod((x + i) * halves + half, each // 3)
                at = q * 3 + c
                tile = load_tile(in_ref, part, at * cells_z, cells_z)
                total, step = tile, 1
                while step < cells_z:
                    total = total + jnp.where(level >= step, pltpu.roll(total, step, 0), 0.0)
                    step *= 2
                offset = one_row(in_ref, part, each * cells_z + at)
                lanes = slice(half * LANES, (half + 1) * LANES)
                buffer[0, piece, i, :, lanes] = tile
                buffer[1, piece, i, :, lanes] = (total + offset) * factor
        for k, (target, ref) in enumerate(((c, next_ref), ((1, 0, 2)[c], pot_ref))):
            copy = pltpu.make_async_copy(
                buffer.at[k, piece], ref.at[target, pl.ds(x, batch)], sems.at[k, piece]
            )
            copy.start()
            copies.append(copy)
    for copy in copies:
        copy.wait()


def limit(mib):
    return pltpu.CompilerParams(vmem_limit_bytes=mib * 2**20)


def kernel_form(b_field, resist, ymix, zmix):
    _, cells_x, cells_z, cells_y = b_field.shape
    parts = lax.axis_size("gz")
    total_z = cells_z * parts
    f32 = jnp.float32
    shape = lambda *sizes: jax.ShapeDtypeStruct(sizes, f32)
    place = (lax.axis_index("gx") + 2 * (lax.axis_index("gz") & 1)).astype(jnp.int32).reshape(1)
    swap = lambda value: lax.ppermute(value, "gx", [(0, 1), (1, 0)])

    far, near, side = pl.pallas_call(
        pack_kernel,
        out_shape=(shape(2 * cells_x, cells_y), shape(2 * cells_x, cells_y), shape(2, cells_z, cells_y)),
        in_specs=[VMEM, SMEM],
        out_specs=(VMEM, VMEM, VMEM),
        compiler_params=limit(6),
    )(b_field, place)
    exchange = lambda value, low: lax.ppermute(
        value,
        "gz",
        [pair for i in range(low, parts - 1, 2) for pair in ((i, i + 1), (i + 1, i))],
    )
    far, near = exchange(far, 1), exchange(near, 0)
    line = pl.pallas_call(
        line_matrix_kernel,
        out_shape=shape(total_z + parts, total_z),
        in_specs=[VMEM],
        out_specs=VMEM,
        compiler_params=limit(4),
    )(zmix)
    line, far = lax.optimization_barrier((line, far))
    known = (b_field, resist, swap(side), far, near, place)
    edge = pl.pallas_call(
        edge_kernel,
        out_shape=shape(2, cells_z, cells_y),
        in_specs=[VMEM] * 5 + [SMEM],
        out_specs=VMEM,
        compiler_params=limit(6),
    )(*known)
    rows = pl.pallas_call(
        step_kernel,
        out_shape=shape(3 * cells_x * cells_z + 4 * cells_x, cells_y),
        in_specs=[VMEM] * 5 + [SMEM],
        out_specs=VMEM,
        scratch_shapes=[pltpu.VMEM(b_field.shape, f32)],
        compiler_params=limit(6),
        cost_estimate=estimate(400.0 * b_field.size),
    )(*known)
    pairs = cells_x * (cells_y // LANES) // parts
    sent = pl.pallas_call(
        functools.partial(mix_kernel, cells_x, cells_z),
        out_shape=shape(parts, pairs * (3 * cells_z + 4) // SHORT, SHORT, LANES),
        in_specs=[VMEM] * 3 + [SMEM],
        out_specs=VMEM,
        scratch_shapes=[pltpu.VMEM(rows.shape, f32)],
        compiler_params=limit(6),
    )(rows, swap(edge), ymix, place)
    lines = lax.all_to_all(sent, "gz", split_axis=0, concat_axis=0, tiled=True)
    product = pl.pallas_call(
        functools.partial(lines_kernel, cells_z, pairs),
        out_shape=shape(parts, -(-pairs * 3 * (cells_z + 1) // SHORT), SHORT, LANES),
        in_specs=[VMEM, VMEM],
        out_specs=VMEM,
        compiler_params=limit(6),
    )(lines, line)
    returned = lax.all_to_all(product, "gz", split_axis=0, concat_axis=0, tiled=True)
    whole = jax.ShapeDtypeStruct(b_field.shape, f32)
    hbm = pl.BlockSpec(memory_space=pl.ANY)
    return pl.pallas_call(
        functools.partial(finish_kernel, total_z ** (-0.5), cells_z, 3 * pairs),
        out_shape=(whole, whole),
        in_specs=[VMEM],
        out_specs=(hbm, hbm),
        scratch_shapes=[
            pltpu.VMEM((2, 3 * PIECES, cells_x // PIECES, cells_z, cells_y), f32),
            pltpu.SemaphoreType.DMA((2, 3 * PIECES)),
        ],
        compiler_params=limit(6),
    )(returned)


def estimate(flops):
    return pl.CostEstimate(flops=int(flops), bytes_accessed=0, transcendentals=0)


def on_device(b_field, resist, ymix, zmix):
    _, cells_x, cells_z, cells_y = b_field.shape
    parts = lax.axis_size("gz")
    fits = (
        lax.axis_size("gx") == 2
        and parts > 1
        and cells_z == SUBLANES
        and cells_x % PIECES == 0
        and cells_y % LANES == 0
        and cells_x >= 4
        and cells_x * (cells_y // LANES) % parts == 0
    )
    return (kernel_form if fits else plain_form)(b_field, resist, ymix, zmix)


def solution(mesh):
    in_specs = (P(None, "gx", "gz", None), P("gx", "gz", None), P(), P())
    out_specs = (P(None, "gx", "gz", None), P(None, "gx", "gz", None))
    return jax.shard_map(
        on_device, mesh=mesh, in_specs=in_specs, out_specs=out_specs, check_vma=False
    )
```

```python
import functools
import jax
import jax.numpy as jnp
from jax import lax
from jax.experimental import pallas as pl
from jax.experimental.pallas import tpu as pltpu
from jax.sharding import PartitionSpec as P

time_step = 0.1
friction = 1.0
LANES = 128
SUBLANES = 8
SHORT = 4
PIECES = 2
BATCH = 11
VMEM = pl.BlockSpec(memory_space=pltpu.VMEM)
SMEM = pl.BlockSpec(memory_space=pltpu.SMEM)


def with_halo(block, sides, width):
    for axis, dim in sides:
        count = lax.axis_size(axis)
        forward = [(i, i + 1) for i in range(count - 1)]
        backward = [(target, source) for source, target in forward]
        low = lax.ppermute(
            lax.slice_in_dim(block, block.shape[dim] - width, None, axis=dim), axis, forward
        )
        high = lax.ppermute(lax.slice_in_dim(block, 0, width, axis=dim), axis, backward)
        block = jnp.concatenate([low, block, high], axis=dim)
    return block


def curl_of(padded):
    centre = padded[:, 1:-1, 1:-1, :]
    grad_x = (padded[:, 2:, 1:-1, :] - padded[:, :-2, 1:-1, :]) * 0.5
    grad_z = (padded[:, 1:-1, 2:, :] - padded[:, 1:-1, :-2, :]) * 0.5
    grad_y = (jnp.roll(centre, -1, 3) - jnp.roll(centre, 1, 3)) * 0.5
    return jnp.stack([grad_y[2] - grad_z[1], grad_z[0] - grad_x[2], grad_x[1] - grad_y[0]])


def cross_parts(lhs, rhs):
    return (
        lhs[1] * rhs[2] - lhs[2] * rhs[1],
        lhs[2] * rhs[0] - lhs[0] * rhs[2],
        lhs[0] * rhs[1] - lhs[1] * rhs[0],
    )


def electric_parts(current, field, resist):
    strength = field[0] * field[0] + field[1] * field[1] + field[2] * field[2] + 1.0
    inverse = 1.0 / (friction * strength)
    velocity = [part * inverse for part in cross_parts(current, field)]
    pushed = cross_parts(velocity, field)
    return [resist * current[c] - pushed[c] for c in range(3)]


def plain_form(b_field, resist, ymix, zmix):
    cells_z = b_field.shape[2]
    total_z = cells_z * lax.axis_size("gz")
    padded = with_halo(b_field, (("gz", 2), ("gx", 1)), 1)
    efield = jnp.stack(electric_parts(curl_of(padded), b_field, resist))
    curl_e = curl_of(with_halo(efield, (("gz", 2), ("gx", 1)), 1))
    stepped = b_field - time_step * curl_e
    along_y = jnp.einsum("cxzi,ij->cxjz", stepped, ymix, precision=lax.Precision.HIGHEST)
    running = jnp.cumsum(zmix, axis=1)
    slab_ends = running[:, cells_z - 1 :: cells_z][:, :-1]
    lower_flux = jnp.concatenate([jnp.zeros((total_z, 1), jnp.float32), slab_ends], axis=1)
    line_matrix = jnp.concatenate([zmix, lower_flux], axis=1)
    product = jnp.einsum(
        "cxym,mk->cxyk",
        lax.all_to_all(along_y, "gz", split_axis=2, concat_axis=3, tiled=True),
        line_matrix,
        precision=lax.Precision.HIGHEST,
    )
    returned, returned_flux = (
        lax.all_to_all(part, "gz", split_axis=3, concat_axis=2, tiled=True)
        for part in (product[..., :total_z], product[..., total_z:])
    )
    b_next = jnp.transpose(returned, (0, 1, 3, 2))
    offset = jnp.transpose(returned_flux, (0, 1, 3, 2))
    column = (jnp.cumsum(b_next, axis=2) + offset) * total_z ** (-0.5)
    return b_next, jnp.stack([column[1], -column[0], column[2]])


def store_tile(ref, part, at, tile):
    count = tile.shape[0] // SHORT
    ref[part, at // SHORT : at // SHORT + count] = tile.reshape(count, SHORT, LANES)


def load_tile(ref, part, at, height):
    return ref[part, at // SHORT : (at + height) // SHORT].reshape(height, LANES)


def one_row(ref, part, at):
    return ref[part, at // SHORT, at % SHORT : at % SHORT + 1, :]


def slope(after, before):
    return (after - before) * 0.5


def along_row(value):
    cells_y = value.shape[1]
    return slope(pltpu.roll(value, cells_y - 1, 1), pltpu.roll(value, 1, 1))


def along_z(value, above, below):
    cells_z = value.shape[0]
    level = lax.broadcasted_iota(jnp.int32, value.shape, 0)
    after = jnp.where(level == cells_z - 1, above, pltpu.roll(value, cells_z - 1, 0))
    before = jnp.where(level == 0, below, pltpu.roll(value, 1, 0))
    return slope(after, before)


def over_x(cells_x, body):
    batch = next(size for size in range(BATCH, 0, -1) if (cells_x - 2) % size == 0)

    def trip(i, carry):
        for j in range(batch):
            body(1 + i * batch + j)
        return carry

    lax.fori_loop(0, (cells_x - 2) // batch, trip, 0)
    body(0)
    body(cells_x - 1)


def pack_kernel(b_ref, place_ref, far_ref, near_ref, side_ref):
    cells_x, cells_z = b_ref.shape[1], b_ref.shape[2]
    edge = jnp.where((place_ref[0] & 1) == 0, cells_x - 1, 0)
    odd = place_ref[0] >= 2
    far_row = jnp.where(odd, cells_z - 1, 0)
    near_row = jnp.where(odd, 0, cells_z - 1)
    for c in range(2):
        side_ref[c] = b_ref[c + 1, edge]
        for x in range(cells_x):
            at = pl.ds(c * cells_x + x, 1)
            far_ref[at, :] = b_ref[c, x, pl.ds(far_row, 1), :]
            near_ref[at, :] = b_ref[c, x, pl.ds(near_row, 1), :]


def x_slope(ref, side_ref, first, c, x):
    last = ref.shape[1] - 1

    def beyond(mine):
        if side_ref is None:
            return 0.0
        return jnp.where(mine, side_ref[c - 1], 0.0)

    if isinstance(x, int) and x == 0:
        return slope(ref[c, 1], beyond(jnp.logical_not(first) if side_ref is not None else None))
    if isinstance(x, int) and x == last:
        return slope(beyond(first), ref[c, last - 1])
    return slope(ref[c, x + 1], ref[c, x - 1])


def electric_at(b_ref, r_ref, side_ref, far_ref, near_ref, place_ref, x):
    cells_x = b_ref.shape[1]
    odd = place_ref[0] >= 2
    here = [b_ref[c, x] for c in range(3)]
    dz = []
    for c in range(2):
        at = pl.ds(c * cells_x + x, 1)
        far, near = far_ref[at, :], near_ref[at, :]
        dz.append(along_z(here[c], jnp.where(odd, far, near), jnp.where(odd, near, far)))
    first = (place_ref[0] & 1) == 0
    dx = [None] + [x_slope(b_ref, side_ref, first, c, x) for c in (1, 2)]
    current = (along_row(here[2]) - dz[1], dz[0] - dx[2], dx[1] - along_row(here[0]))
    return electric_parts(current, here, r_ref[x])


def edge_kernel(b_ref, r_ref, side_ref, far_ref, near_ref, place_ref, edge_ref):
    known = (b_ref, r_ref, side_ref, far_ref, near_ref, place_ref)
    low, high = electric_at(*known, 0), electric_at(*known, b_ref.shape[1] - 1)
    first = (place_ref[0] & 1) == 0
    for c in range(2):
        edge_ref[c] = jnp.where(first, high[c + 1], low[c + 1])


def step_kernel(b_ref, r_ref, side_ref, far_ref, near_ref, place_ref, rows_ref, elec_ref):
    cells_x, cells_z = b_ref.shape[1], b_ref.shape[2]
    half = 0.5 * time_step

    def make(x):
        made = electric_at(b_ref, r_ref, side_ref, far_ref, near_ref, place_ref, x)
        for c in range(3):
            elec_ref[c, x] = made[c]

    def step(x):
        here = [elec_ref[c, x] for c in range(3)]
        dz = [along_z(here[c], 0.0, 0.0) for c in range(2)]
        dx = [None] + [x_slope(elec_ref, None, None, c, x) for c in (1, 2)]
        curl = (along_row(here[2]) - dz[1], dz[0] - dx[2], dx[1] - along_row(here[0]))
        for c in range(3):
            start = pl.multiple_of((c * cells_x + x) * cells_z, cells_z)
            rows_ref[pl.ds(start, cells_z), :] = b_ref[c, x] - time_step * curl[c]
        extra = 3 * cells_x * cells_z + 4 * x
        rows_ref[pl.ds(extra, 1), :] = half * here[1][:1]
        rows_ref[pl.ds(extra + 1, 1), :] = -half * here[1][cells_z - 1 :]
        rows_ref[pl.ds(extra + 2, 1), :] = -half * here[0][:1]
        rows_ref[pl.ds(extra + 3, 1), :] = half * here[0][cells_z - 1 :]

    over_x(cells_x, make)
    over_x(cells_x, step)


def split(value):
    high = value.astype(jnp.bfloat16)
    return high, (value - high.astype(jnp.float32)).astype(jnp.bfloat16)


def full_dot(lhs, rhs):
    dot = functools.partial(jnp.dot, preferred_element_type=jnp.float32)
    (lhs_high, lhs_low), (rhs_high, rhs_low) = split(lhs), split(rhs)
    return dot(lhs_high, rhs_high) + (dot(lhs_high, rhs_low) + dot(lhs_low, rhs_high))


def mix_kernel(cells_x, cells_z, rows_ref, edge_ref, ymix_ref, place_ref, out_ref, mixed):
    cells_y = rows_ref.shape[1]
    halves = cells_y // LANES
    mixed[...] = full_dot(rows_ref[...], ymix_ref[...])
    first = (place_ref[0] & 1) == 0
    factor = jnp.where(first, 0.5 * time_step, -0.5 * time_step)
    added = full_dot(edge_ref[...].reshape(2 * cells_z, cells_y), ymix_ref[...]) * factor
    edge = jnp.where(first, cells_x - 1, 0)
    for c, term in ((1, added[cells_z:]), (2, -added[:cells_z])):
        at = pl.ds(pl.multiple_of((c * cells_x + edge) * cells_z, cells_z), cells_z)
        mixed[at, :] = mixed[at, :] + term
    pairs = cells_x * halves // out_ref.shape[0]
    extra = 3 * cells_x * cells_z
    for x in range(cells_x):
        for half in range(halves):
            part, q = divmod(x * halves + half, pairs)
            lanes = slice(half * LANES, (half + 1) * LANES)
            for c in range(3):
                at = (q * 3 + c) * cells_z
                line = (c * cells_x + x) * cells_z
                store_tile(out_ref, part, at, mixed[line : line + cells_z, lanes])
            at = pairs * 3 * cells_z + q * 4
            store_tile(out_ref, part, at, mixed[extra + 4 * x : extra + 4 * x + 4, lanes])


def line_matrix_kernel(zmix_ref, out_ref):
    total = zmix_ref.shape[0]
    parts = out_ref.shape[0] - total
    turned = jnp.transpose(zmix_ref[...])
    slab = lax.broadcasted_iota(jnp.int32, (parts, total), 0) * (total // parts)
    lower = (lax.broadcasted_iota(jnp.int32, (parts, total), 1) < slab).astype(jnp.float32)
    out_ref[:total] = turned
    out_ref[total:] = jnp.dot(
        lower, turned, precision=lax.Precision.HIGHEST, preferred_element_type=jnp.float32
    )


def lines_kernel(cells_z, pairs, in_ref, line_ref, out_ref):
    parts = in_ref.shape[0]
    total = parts * cells_z
    height = pairs * 3 * cells_z
    level = lax.broadcasted_iota(jnp.int32, (cells_z, LANES), 0)
    columns = []
    for q in range(pairs):
        for c in range(3):
            at = (q * 3 + c) * cells_z
            tiles = [load_tile(in_ref, s, at, cells_z) for s in range(parts)]
            if c < 2:
                low = height + q * 4 + c * 2
                for s in range(parts):
                    if s < parts - 1:
                        tiles[s] = tiles[s] + jnp.where(
                            level == cells_z - 1, one_row(in_ref, s + 1, low), 0.0
                        )
                    if s > 0:
                        tiles[s] = tiles[s] + jnp.where(
                            level == 0, one_row(in_ref, s - 1, low + 1), 0.0
                        )
            columns.append(jnp.concatenate(tiles, axis=0))
    product = full_dot(line_ref[...], jnp.concatenate(columns, axis=1))
    for g in range(3 * pairs):
        part = product[:, g * LANES : (g + 1) * LANES]
        row = height + g
        for s in range(parts):
            store_tile(out_ref, s, g * cells_z, part[s * cells_z : (s + 1) * cells_z])
            out_ref[s, row // SHORT, row % SHORT : row % SHORT + 1, :] = part[total + s : total + s + 1]


def finish_kernel(scale, cells_z, each, in_ref, next_ref, pot_ref, buffer, sems):
    _, cells_x, _, cells_y = next_ref.shape
    halves = cells_y // LANES
    batch = cells_x // PIECES
    level = lax.broadcasted_iota(jnp.int32, (cells_z, LANES), 0)
    copies = []
    for piece in range(3 * PIECES):
        c, x = divmod(piece * batch, cells_x)
        factor = -scale if c == 0 else scale
        for i in range(batch):
            for half in range(halves):
                part, q = divmod((x + i) * halves + half, each // 3)
                at = q * 3 + c
                tile = load_tile(in_ref, part, at * cells_z, cells_z)
                total, step = tile, 1
                while step < cells_z:
                    total = total + jnp.where(level >= step, pltpu.roll(total, step, 0), 0.0)
                    step *= 2
                offset = one_row(in_ref, part, each * cells_z + at)
                lanes = slice(half * LANES, (half + 1) * LANES)
                buffer[0, piece, i, :, lanes] = tile
                buffer[1, piece, i, :, lanes] = (total + offset) * factor
        for k, (target, ref) in enumerate(((c, next_ref), ((1, 0, 2)[c], pot_ref))):
            copy = pltpu.make_async_copy(
                buffer.at[k, piece], ref.at[target, pl.ds(x, batch)], sems.at[k, piece]
            )
            copy.start()
            copies.append(copy)
    for copy in copies:
        copy.wait()


def limit(mib):
    return pltpu.CompilerParams(vmem_limit_bytes=mib * 2**20)


def kernel_form(b_field, resist, ymix, zmix):
    _, cells_x, cells_z, cells_y = b_field.shape
    parts = lax.axis_size("gz")
    total_z = cells_z * parts
    f32 = jnp.float32
    shape = lambda *sizes: jax.ShapeDtypeStruct(sizes, f32)
    place = (lax.axis_index("gx") + 2 * (lax.axis_index("gz") & 1)).astype(jnp.int32).reshape(1)
    swap = lambda value: lax.ppermute(value, "gx", [(0, 1), (1, 0)])

    far, near, side = pl.pallas_call(
        pack_kernel,
        out_shape=(shape(2 * cells_x, cells_y), shape(2 * cells_x, cells_y), shape(2, cells_z, cells_y)),
        in_specs=[VMEM, SMEM],
        out_specs=(VMEM, VMEM, VMEM),
        compiler_params=limit(6),
    )(b_field, place)
    exchange = lambda value, low: lax.ppermute(
        value,
        "gz",
        [pair for i in range(low, parts - 1, 2) for pair in ((i, i + 1), (i + 1, i))],
    )
    far, near = exchange(far, 1), exchange(near, 0)
    line = pl.pallas_call(
        line_matrix_kernel,
        out_shape=shape(total_z + parts, total_z),
        in_specs=[VMEM],
        out_specs=VMEM,
        compiler_params=limit(4),
    )(zmix)
    line, far = lax.optimization_barrier((line, far))
    known = (b_field, resist, swap(side), far, near, place)
    edge = pl.pallas_call(
        edge_kernel,
        out_shape=shape(2, cells_z, cells_y),
        in_specs=[VMEM] * 5 + [SMEM],
        out_specs=VMEM,
        compiler_params=limit(6),
    )(*known)
    rows = pl.pallas_call(
        step_kernel,
        out_shape=shape(3 * cells_x * cells_z + 4 * cells_x, cells_y),
        in_specs=[VMEM] * 5 + [SMEM],
        out_specs=VMEM,
        scratch_shapes=[pltpu.VMEM(b_field.shape, f32)],
        compiler_params=limit(6),
        cost_estimate=estimate(400.0 * b_field.size),
    )(*known)
    pairs = cells_x * (cells_y // LANES) // parts
    sent = pl.pallas_call(
        functools.partial(mix_kernel, cells_x, cells_z),
        out_shape=shape(parts, pairs * (3 * cells_z + 4) // SHORT, SHORT, LANES),
        in_specs=[VMEM] * 3 + [SMEM],
        out_specs=VMEM,
        scratch_shapes=[pltpu.VMEM(rows.shape, f32)],
        compiler_params=limit(6),
    )(rows, swap(edge), ymix, place)
    lines = lax.all_to_all(sent, "gz", split_axis=0, concat_axis=0, tiled=True)
    product = pl.pallas_call(
        functools.partial(lines_kernel, cells_z, pairs),
        out_shape=shape(parts, -(-pairs * 3 * (cells_z + 1) // SHORT), SHORT, LANES),
        in_specs=[VMEM, VMEM],
        out_specs=VMEM,
        compiler_params=limit(6),
    )(lines, line)
    returned = lax.all_to_all(product, "gz", split_axis=0, concat_axis=0, tiled=True)
    whole = jax.ShapeDtypeStruct(b_field.shape, f32)
    hbm = pl.BlockSpec(memory_space=pl.ANY)
    return pl.pallas_call(
        functools.partial(finish_kernel, total_z ** (-0.5), cells_z, 3 * pairs),
        out_shape=(whole, whole),
        in_specs=[VMEM],
        out_specs=(hbm, hbm),
        scratch_shapes=[
            pltpu.VMEM((2, 3 * PIECES, cells_x // PIECES, cells_z, cells_y), f32),
            pltpu.SemaphoreType.DMA((2, 3 * PIECES)),
        ],
        compiler_params=limit(6),
    )(returned)


def estimate(flops):
    return pl.CostEstimate(flops=int(flops), bytes_accessed=0, transcendentals=0)


def on_device(b_field, resist, ymix, zmix):
    _, cells_x, cells_z, cells_y = b_field.shape
    parts = lax.axis_size("gz")
    fits = (
        lax.axis_size("gx") == 2
        and parts > 1
        and cells_z == SUBLANES
        and cells_x % PIECES == 0
        and cells_y % LANES == 0
        and cells_x >= 4
        and cells_x * (cells_y // LANES) % parts == 0
    )
    return (kernel_form if fits else plain_form)(b_field, resist, ymix, zmix)


def solution(mesh):
    in_specs = (P(None, "gx", "gz", None), P("gx", "gz", None), P(), P())
    out_specs = (P(None, "gx", "gz", None), P(None, "gx", "gz", None))
    return jax.shard_map(
        on_device, mesh=mesh, in_specs=in_specs, out_specs=out_specs, check_vma=False
    )
```

```python
import functools
import jax
import jax.numpy as jnp
from jax import lax
from jax.experimental import pallas as pl
from jax.experimental.pallas import tpu as pltpu
from jax.sharding import PartitionSpec as P

time_step = 0.1
friction = 1.0
LANES = 128
SUBLANES = 8
SHORT = 4
PIECES = 1
BATCH = 22
VMEM = pl.BlockSpec(memory_space=pltpu.VMEM)
SMEM = pl.BlockSpec(memory_space=pltpu.SMEM)


def with_halo(block, sides, width):
    for axis, dim in sides:
        count = lax.axis_size(axis)
        forward = [(i, i + 1) for i in range(count - 1)]
        backward = [(target, source) for source, target in forward]
        low = lax.ppermute(
            lax.slice_in_dim(block, block.shape[dim] - width, None, axis=dim), axis, forward
        )
        high = lax.ppermute(lax.slice_in_dim(block, 0, width, axis=dim), axis, backward)
        block = jnp.concatenate([low, block, high], axis=dim)
    return block


def curl_of(padded):
    centre = padded[:, 1:-1, 1:-1, :]
    grad_x = (padded[:, 2:, 1:-1, :] - padded[:, :-2, 1:-1, :]) * 0.5
    grad_z = (padded[:, 1:-1, 2:, :] - padded[:, 1:-1, :-2, :]) * 0.5
    grad_y = (jnp.roll(centre, -1, 3) - jnp.roll(centre, 1, 3)) * 0.5
    return jnp.stack([grad_y[2] - grad_z[1], grad_z[0] - grad_x[2], grad_x[1] - grad_y[0]])


def cross_parts(lhs, rhs):
    return (
        lhs[1] * rhs[2] - lhs[2] * rhs[1],
        lhs[2] * rhs[0] - lhs[0] * rhs[2],
        lhs[0] * rhs[1] - lhs[1] * rhs[0],
    )


def electric_parts(current, field, resist):
    strength = field[0] * field[0] + field[1] * field[1] + field[2] * field[2] + 1.0
    inverse = 1.0 / (friction * strength)
    velocity = [part * inverse for part in cross_parts(current, field)]
    pushed = cross_parts(velocity, field)
    return [resist * current[c] - pushed[c] for c in range(3)]


def plain_form(b_field, resist, ymix, zmix):
    cells_z = b_field.shape[2]
    total_z = cells_z * lax.axis_size("gz")
    padded = with_halo(b_field, (("gz", 2), ("gx", 1)), 1)
    efield = jnp.stack(electric_parts(curl_of(padded), b_field, resist))
    curl_e = curl_of(with_halo(efield, (("gz", 2), ("gx", 1)), 1))
    stepped = b_field - time_step * curl_e
    along_y = jnp.einsum("cxzi,ij->cxjz", stepped, ymix, precision=lax.Precision.HIGHEST)
    running = jnp.cumsum(zmix, axis=1)
    slab_ends = running[:, cells_z - 1 :: cells_z][:, :-1]
    lower_flux = jnp.concatenate([jnp.zeros((total_z, 1), jnp.float32), slab_ends], axis=1)
    line_matrix = jnp.concatenate([zmix, lower_flux], axis=1)
    product = jnp.einsum(
        "cxym,mk->cxyk",
        lax.all_to_all(along_y, "gz", split_axis=2, concat_axis=3, tiled=True),
        line_matrix,
        precision=lax.Precision.HIGHEST,
    )
    returned, returned_flux = (
        lax.all_to_all(part, "gz", split_axis=3, concat_axis=2, tiled=True)
        for part in (product[..., :total_z], product[..., total_z:])
    )
    b_next = jnp.transpose(returned, (0, 1, 3, 2))
    offset = jnp.transpose(returned_flux, (0, 1, 3, 2))
    column = (jnp.cumsum(b_next, axis=2) + offset) * total_z ** (-0.5)
    return b_next, jnp.stack([column[1], -column[0], column[2]])


def store_tile(ref, part, at, tile):
    count = tile.shape[0] // SHORT
    ref[part, at // SHORT : at // SHORT + count] = tile.reshape(count, SHORT, LANES)


def load_tile(ref, part, at, height):
    return ref[part, at // SHORT : (at + height) // SHORT].reshape(height, LANES)


def one_row(ref, part, at):
    return ref[part, at // SHORT, at % SHORT : at % SHORT + 1, :]


def slope(after, before):
    return (after - before) * 0.5


def along_row(value):
    cells_y = value.shape[1]
    return slope(pltpu.roll(value, cells_y - 1, 1), pltpu.roll(value, 1, 1))


def along_z(value, above, below):
    cells_z = value.shape[0]
    level = lax.broadcasted_iota(jnp.int32, value.shape, 0)
    after = jnp.where(level == cells_z - 1, above, pltpu.roll(value, cells_z - 1, 0))
    before = jnp.where(level == 0, below, pltpu.roll(value, 1, 0))
    return slope(after, before)


def over_x(cells_x, body):
    batch = next(size for size in range(BATCH, 0, -1) if (cells_x - 2) % size == 0)

    def trip(i, carry):
        for j in range(batch):
            body(1 + i * batch + j)
        return carry

    lax.fori_loop(0, (cells_x - 2) // batch, trip, 0)
    body(0)
    body(cells_x - 1)


def pack_kernel(b_ref, place_ref, far_ref, near_ref, side_ref):
    cells_x, cells_z = b_ref.shape[1], b_ref.shape[2]
    edge = jnp.where((place_ref[0] & 1) == 0, cells_x - 1, 0)
    odd = place_ref[0] >= 2
    far_row = jnp.where(odd, cells_z - 1, 0)
    near_row = jnp.where(odd, 0, cells_z - 1)
    for c in range(2):
        side_ref[c] = b_ref[c + 1, edge]
        for x in range(cells_x):
            at = pl.ds(c * cells_x + x, 1)
            far_ref[at, :] = b_ref[c, x, pl.ds(far_row, 1), :]
            near_ref[at, :] = b_ref[c, x, pl.ds(near_row, 1), :]


def x_slope(ref, side_ref, first, c, x):
    last = ref.shape[1] - 1

    def beyond(mine):
        if side_ref is None:
            return 0.0
        return jnp.where(mine, side_ref[c - 1], 0.0)

    if isinstance(x, int) and x == 0:
        return slope(ref[c, 1], beyond(jnp.logical_not(first) if side_ref is not None else None))
    if isinstance(x, int) and x == last:
        return slope(beyond(first), ref[c, last - 1])
    return slope(ref[c, x + 1], ref[c, x - 1])


def electric_at(b_ref, r_ref, side_ref, far_ref, near_ref, place_ref, x):
    cells_x = b_ref.shape[1]
    odd = place_ref[0] >= 2
    here = [b_ref[c, x] for c in range(3)]
    dz = []
    for c in range(2):
        at = pl.ds(c * cells_x + x, 1)
        far, near = far_ref[at, :], near_ref[at, :]
        dz.append(along_z(here[c], jnp.where(odd, far, near), jnp.where(odd, near, far)))
    first = (place_ref[0] & 1) == 0
    dx = [None] + [x_slope(b_ref, side_ref, first, c, x) for c in (1, 2)]
    current = (along_row(here[2]) - dz[1], dz[0] - dx[2], dx[1] - along_row(here[0]))
    return electric_parts(current, here, r_ref[x])


def edge_kernel(b_ref, r_ref, side_ref, far_ref, near_ref, place_ref, edge_ref):
    known = (b_ref, r_ref, side_ref, far_ref, near_ref, place_ref)
    low, high = electric_at(*known, 0), electric_at(*known, b_ref.shape[1] - 1)
    first = (place_ref[0] & 1) == 0
    for c in range(2):
        edge_ref[c] = jnp.where(first, high[c + 1], low[c + 1])


def step_kernel(b_ref, r_ref, side_ref, far_ref, near_ref, place_ref, rows_ref, elec_ref):
    cells_x, cells_z = b_ref.shape[1], b_ref.shape[2]
    half = 0.5 * time_step

    def make(x):
        made = electric_at(b_ref, r_ref, side_ref, far_ref, near_ref, place_ref, x)
        for c in range(3):
            elec_ref[c, x] = made[c]

    def step(x):
        here = [elec_ref[c, x] for c in range(3)]
        dz = [along_z(here[c], 0.0, 0.0) for c in range(2)]
        dx = [None] + [x_slope(elec_ref, None, None, c, x) for c in (1, 2)]
        curl = (along_row(here[2]) - dz[1], dz[0] - dx[2], dx[1] - along_row(here[0]))
        for c in range(3):
            start = pl.multiple_of((c * cells_x + x) * cells_z, cells_z)
            rows_ref[pl.ds(start, cells_z), :] = b_ref[c, x] - time_step * curl[c]
        extra = 3 * cells_x * cells_z + 4 * x
        rows_ref[pl.ds(extra, 1), :] = half * here[1][:1]
        rows_ref[pl.ds(extra + 1, 1), :] = -half * here[1][cells_z - 1 :]
        rows_ref[pl.ds(extra + 2, 1), :] = -half * here[0][:1]
        rows_ref[pl.ds(extra + 3, 1), :] = half * here[0][cells_z - 1 :]

    over_x(cells_x, make)
    over_x(cells_x, step)


def split(value):
    high = value.astype(jnp.bfloat16)
    return high, (value - high.astype(jnp.float32)).astype(jnp.bfloat16)


def full_dot(lhs, rhs):
    dot = functools.partial(jnp.dot, preferred_element_type=jnp.float32)
    (lhs_high, lhs_low), (rhs_high, rhs_low) = split(lhs), split(rhs)
    return dot(lhs_high, rhs_high) + (dot(lhs_high, rhs_low) + dot(lhs_low, rhs_high))


def mix_kernel(cells_x, cells_z, rows_ref, edge_ref, ymix_ref, place_ref, out_ref, mixed):
    cells_y = rows_ref.shape[1]
    halves = cells_y // LANES
    mixed[...] = full_dot(rows_ref[...], ymix_ref[...])
    first = (place_ref[0] & 1) == 0
    factor = jnp.where(first, 0.5 * time_step, -0.5 * time_step)
    added = full_dot(edge_ref[...].reshape(2 * cells_z, cells_y), ymix_ref[...]) * factor
    edge = jnp.where(first, cells_x - 1, 0)
    for c, term in ((1, added[cells_z:]), (2, -added[:cells_z])):
        at = pl.ds(pl.multiple_of((c * cells_x + edge) * cells_z, cells_z), cells_z)
        mixed[at, :] = mixed[at, :] + term
    pairs = cells_x * halves // out_ref.shape[0]
    extra = 3 * cells_x * cells_z
    for x in range(cells_x):
        for half in range(halves):
            part, q = divmod(x * halves + half, pairs)
            lanes = slice(half * LANES, (half + 1) * LANES)
            for c in range(3):
                at = (q * 3 + c) * cells_z
                line = (c * cells_x + x) * cells_z
                store_tile(out_ref, part, at, mixed[line : line + cells_z, lanes])
            at = pairs * 3 * cells_z + q * 4
            store_tile(out_ref, part, at, mixed[extra + 4 * x : extra + 4 * x + 4, lanes])


def line_matrix_kernel(zmix_ref, out_ref):
    total = zmix_ref.shape[0]
    parts = out_ref.shape[0] - total
    turned = jnp.transpose(zmix_ref[...])
    slab = lax.broadcasted_iota(jnp.int32, (parts, total), 0) * (total // parts)
    lower = (lax.broadcasted_iota(jnp.int32, (parts, total), 1) < slab).astype(jnp.float32)
    out_ref[:total] = turned
    out_ref[total:] = jnp.dot(
        lower, turned, precision=lax.Precision.HIGHEST, preferred_element_type=jnp.float32
    )


def lines_kernel(cells_z, pairs, in_ref, line_ref, out_ref):
    parts = in_ref.shape[0]
    total = parts * cells_z
    height = pairs * 3 * cells_z
    level = lax.broadcasted_iota(jnp.int32, (cells_z, LANES), 0)
    columns = []
    for q in range(pairs):
        for c in range(3):
            at = (q * 3 + c) * cells_z
            tiles = [load_tile(in_ref, s, at, cells_z) for s in range(parts)]
            if c < 2:
                low = height + q * 4 + c * 2
                for s in range(parts):
                    if s < parts - 1:
                        tiles[s] = tiles[s] + jnp.where(
                            level == cells_z - 1, one_row(in_ref, s + 1, low), 0.0
                        )
                    if s > 0:
                        tiles[s] = tiles[s] + jnp.where(
                            level == 0, one_row(in_ref, s - 1, low + 1), 0.0
                        )
            columns.append(jnp.concatenate(tiles, axis=0))
    product = full_dot(line_ref[...], jnp.concatenate(columns, axis=1))
    for g in range(3 * pairs):
        part = product[:, g * LANES : (g + 1) * LANES]
        row = height + g
        for s in range(parts):
            store_tile(out_ref, s, g * cells_z, part[s * cells_z : (s + 1) * cells_z])
            out_ref[s, row // SHORT, row % SHORT : row % SHORT + 1, :] = part[total + s : total + s + 1]


def finish_kernel(scale, cells_z, each, in_ref, next_ref, pot_ref, buffer, sems):
    _, cells_x, _, cells_y = next_ref.shape
    halves = cells_y // LANES
    batch = cells_x // PIECES
    level = lax.broadcasted_iota(jnp.int32, (cells_z, LANES), 0)
    copies = []
    for piece in range(3 * PIECES):
        c, x = divmod(piece * batch, cells_x)
        factor = -scale if c == 0 else scale
        for i in range(batch):
            for half in range(halves):
                part, q = divmod((x + i) * halves + half, each // 3)
                at = q * 3 + c
                tile = load_tile(in_ref, part, at * cells_z, cells_z)
                total, step = tile, 1
                while step < cells_z:
                    total = total + jnp.where(level >= step, pltpu.roll(total, step, 0), 0.0)
                    step *= 2
                offset = one_row(in_ref, part, each * cells_z + at)
                lanes = slice(half * LANES, (half + 1) * LANES)
                buffer[0, piece, i, :, lanes] = tile
                buffer[1, piece, i, :, lanes] = (total + offset) * factor
        for k, (target, ref) in enumerate(((c, next_ref), ((1, 0, 2)[c], pot_ref))):
            copy = pltpu.make_async_copy(
                buffer.at[k, piece], ref.at[target, pl.ds(x, batch)], sems.at[k, piece]
            )
            copy.start()
            copies.append(copy)
    for copy in copies:
        copy.wait()


def limit(mib):
    return pltpu.CompilerParams(vmem_limit_bytes=mib * 2**20)


def kernel_form(b_field, resist, ymix, zmix):
    _, cells_x, cells_z, cells_y = b_field.shape
    parts = lax.axis_size("gz")
    total_z = cells_z * parts
    f32 = jnp.float32
    shape = lambda *sizes: jax.ShapeDtypeStruct(sizes, f32)
    place = (lax.axis_index("gx") + 2 * (lax.axis_index("gz") & 1)).astype(jnp.int32).reshape(1)
    swap = lambda value: lax.ppermute(value, "gx", [(0, 1), (1, 0)])

    far, near, side = pl.pallas_call(
        pack_kernel,
        out_shape=(shape(2 * cells_x, cells_y), shape(2 * cells_x, cells_y), shape(2, cells_z, cells_y)),
        in_specs=[VMEM, SMEM],
        out_specs=(VMEM, VMEM, VMEM),
        compiler_params=limit(6),
    )(b_field, place)
    exchange = lambda value, low: lax.ppermute(
        value,
        "gz",
        [pair for i in range(low, parts - 1, 2) for pair in ((i, i + 1), (i + 1, i))],
    )
    far, near = exchange(far, 1), exchange(near, 0)
    line = pl.pallas_call(
        line_matrix_kernel,
        out_shape=shape(total_z + parts, total_z),
        in_specs=[VMEM],
        out_specs=VMEM,
        compiler_params=limit(4),
    )(zmix)
    line, far = lax.optimization_barrier((line, far))
    known = (b_field, resist, swap(side), far, near, place)
    edge = pl.pallas_call(
        edge_kernel,
        out_shape=shape(2, cells_z, cells_y),
        in_specs=[VMEM] * 5 + [SMEM],
        out_specs=VMEM,
        compiler_params=limit(6),
    )(*known)
    rows = pl.pallas_call(
        step_kernel,
        out_shape=shape(3 * cells_x * cells_z + 4 * cells_x, cells_y),
        in_specs=[VMEM] * 5 + [SMEM],
        out_specs=VMEM,
        scratch_shapes=[pltpu.VMEM(b_field.shape, f32)],
        compiler_params=limit(6),
        cost_estimate=estimate(400.0 * b_field.size),
    )(*known)
    pairs = cells_x * (cells_y // LANES) // parts
    sent = pl.pallas_call(
        functools.partial(mix_kernel, cells_x, cells_z),
        out_shape=shape(parts, pairs * (3 * cells_z + 4) // SHORT, SHORT, LANES),
        in_specs=[VMEM] * 3 + [SMEM],
        out_specs=VMEM,
        scratch_shapes=[pltpu.VMEM(rows.shape, f32)],
        compiler_params=limit(6),
    )(rows, swap(edge), ymix, place)
    lines = lax.all_to_all(sent, "gz", split_axis=0, concat_axis=0, tiled=True)
    product = pl.pallas_call(
        functools.partial(lines_kernel, cells_z, pairs),
        out_shape=shape(parts, -(-pairs * 3 * (cells_z + 1) // SHORT), SHORT, LANES),
        in_specs=[VMEM, VMEM],
        out_specs=VMEM,
        compiler_params=limit(6),
    )(lines, line)
    returned = lax.all_to_all(product, "gz", split_axis=0, concat_axis=0, tiled=True)
    whole = jax.ShapeDtypeStruct(b_field.shape, f32)
    hbm = pl.BlockSpec(memory_space=pl.ANY)
    return pl.pallas_call(
        functools.partial(finish_kernel, total_z ** (-0.5), cells_z, 3 * pairs),
        out_shape=(whole, whole),
        in_specs=[VMEM],
        out_specs=(hbm, hbm),
        scratch_shapes=[
            pltpu.VMEM((2, 3 * PIECES, cells_x // PIECES, cells_z, cells_y), f32),
            pltpu.SemaphoreType.DMA((2, 3 * PIECES)),
        ],
        compiler_params=limit(6),
    )(returned)


def estimate(flops):
    return pl.CostEstimate(flops=int(flops), bytes_accessed=0, transcendentals=0)


def on_device(b_field, resist, ymix, zmix):
    _, cells_x, cells_z, cells_y = b_field.shape
    parts = lax.axis_size("gz")
    fits = (
        lax.axis_size("gx") == 2
        and parts > 1
        and cells_z == SUBLANES
        and cells_x % PIECES == 0
        and cells_y % LANES == 0
        and cells_x >= 4
        and cells_x * (cells_y // LANES) % parts == 0
    )
    return (kernel_form if fits else plain_form)(b_field, resist, ymix, zmix)


def solution(mesh):
    in_specs = (P(None, "gx", "gz", None), P("gx", "gz", None), P(), P())
    out_specs = (P(None, "gx", "gz", None), P(None, "gx", "gz", None))
    return jax.shard_map(
        on_device, mesh=mesh, in_specs=in_specs, out_specs=out_specs, check_vma=False
    )
```

```python
import functools
import jax
import jax.numpy as jnp
from jax import lax
from jax.experimental import pallas as pl
from jax.experimental.pallas import tpu as pltpu
from jax.sharding import PartitionSpec as P

time_step = 0.1
friction = 1.0
LANES = 128
SUBLANES = 8
SHORT = 4
PIECES = 1
BATCH = 22
VMEM = pl.BlockSpec(memory_space=pltpu.VMEM)
SMEM = pl.BlockSpec(memory_space=pltpu.SMEM)


def with_halo(block, sides, width):
    for axis, dim in sides:
        count = lax.axis_size(axis)
        forward = [(i, i + 1) for i in range(count - 1)]
        backward = [(target, source) for source, target in forward]
        low = lax.ppermute(
            lax.slice_in_dim(block, block.shape[dim] - width, None, axis=dim), axis, forward
        )
        high = lax.ppermute(lax.slice_in_dim(block, 0, width, axis=dim), axis, backward)
        block = jnp.concatenate([low, block, high], axis=dim)
    return block


def curl_of(padded):
    centre = padded[:, 1:-1, 1:-1, :]
    grad_x = (padded[:, 2:, 1:-1, :] - padded[:, :-2, 1:-1, :]) * 0.5
    grad_z = (padded[:, 1:-1, 2:, :] - padded[:, 1:-1, :-2, :]) * 0.5
    grad_y = (jnp.roll(centre, -1, 3) - jnp.roll(centre, 1, 3)) * 0.5
    return jnp.stack([grad_y[2] - grad_z[1], grad_z[0] - grad_x[2], grad_x[1] - grad_y[0]])


def cross_parts(lhs, rhs):
    return (
        lhs[1] * rhs[2] - lhs[2] * rhs[1],
        lhs[2] * rhs[0] - lhs[0] * rhs[2],
        lhs[0] * rhs[1] - lhs[1] * rhs[0],
    )


def electric_parts(current, field, resist):
    strength = field[0] * field[0] + field[1] * field[1] + field[2] * field[2] + 1.0
    inverse = 1.0 / (friction * strength)
    velocity = [part * inverse for part in cross_parts(current, field)]
    pushed = cross_parts(velocity, field)
    return [resist * current[c] - pushed[c] for c in range(3)]


def plain_form(b_field, resist, ymix, zmix):
    cells_z = b_field.shape[2]
    total_z = cells_z * lax.axis_size("gz")
    padded = with_halo(b_field, (("gz", 2), ("gx", 1)), 1)
    efield = jnp.stack(electric_parts(curl_of(padded), b_field, resist))
    curl_e = curl_of(with_halo(efield, (("gz", 2), ("gx", 1)), 1))
    stepped = b_field - time_step * curl_e
    along_y = jnp.einsum("cxzi,ij->cxjz", stepped, ymix, precision=lax.Precision.HIGHEST)
    running = jnp.cumsum(zmix, axis=1)
    slab_ends = running[:, cells_z - 1 :: cells_z][:, :-1]
    lower_flux = jnp.concatenate([jnp.zeros((total_z, 1), jnp.float32), slab_ends], axis=1)
    line_matrix = jnp.concatenate([zmix, lower_flux], axis=1)
    product = jnp.einsum(
        "cxym,mk->cxyk",
        lax.all_to_all(along_y, "gz", split_axis=2, concat_axis=3, tiled=True),
        line_matrix,
        precision=lax.Precision.HIGHEST,
    )
    returned, returned_flux = (
        lax.all_to_all(part, "gz", split_axis=3, concat_axis=2, tiled=True)
        for part in (product[..., :total_z], product[..., total_z:])
    )
    b_next = jnp.transpose(returned, (0, 1, 3, 2))
    offset = jnp.transpose(returned_flux, (0, 1, 3, 2))
    column = (jnp.cumsum(b_next, axis=2) + offset) * total_z ** (-0.5)
    return b_next, jnp.stack([column[1], -column[0], column[2]])


def store_tile(ref, part, at, tile):
    count = tile.shape[0] // SHORT
    ref[part, at // SHORT : at // SHORT + count] = tile.reshape(count, SHORT, LANES)


def load_tile(ref, part, at, height):
    return ref[part, at // SHORT : (at + height) // SHORT].reshape(height, LANES)


def one_row(ref, part, at):
    return ref[part, at // SHORT, at % SHORT : at % SHORT + 1, :]


def slope(after, before):
    return (after - before) * 0.5


def along_row(value):
    cells_y = value.shape[1]
    return slope(pltpu.roll(value, cells_y - 1, 1), pltpu.roll(value, 1, 1))


def along_z(value, above, below):
    cells_z = value.shape[0]
    level = lax.broadcasted_iota(jnp.int32, value.shape, 0)
    after = jnp.where(level == cells_z - 1, above, pltpu.roll(value, cells_z - 1, 0))
    before = jnp.where(level == 0, below, pltpu.roll(value, 1, 0))
    return slope(after, before)


def over_x(cells_x, body):
    batch = next(size for size in range(BATCH, 0, -1) if (cells_x - 2) % size == 0)

    def trip(i, carry):
        for j in range(batch):
            body(1 + i * batch + j)
        return carry

    lax.fori_loop(0, (cells_x - 2) // batch, trip, 0)
    body(0)
    body(cells_x - 1)


def pack_kernel(b_ref, place_ref, far_ref, near_ref, side_ref):
    cells_x, cells_z = b_ref.shape[1], b_ref.shape[2]
    edge = jnp.where((place_ref[0] & 1) == 0, cells_x - 1, 0)
    odd = place_ref[0] >= 2
    far_row = jnp.where(odd, cells_z - 1, 0)
    near_row = jnp.where(odd, 0, cells_z - 1)
    for c in range(2):
        side_ref[c] = b_ref[c + 1, edge]
        for x in range(cells_x):
            at = pl.ds(c * cells_x + x, 1)
            far_ref[at, :] = b_ref[c, x, pl.ds(far_row, 1), :]
            near_ref[at, :] = b_ref[c, x, pl.ds(near_row, 1), :]


def x_slope(ref, side_ref, first, c, x):
    last = ref.shape[1] - 1

    def beyond(mine):
        if side_ref is None:
            return 0.0
        return jnp.where(mine, side_ref[c - 1], 0.0)

    if isinstance(x, int) and x == 0:
        return slope(ref[c, 1], beyond(jnp.logical_not(first) if side_ref is not None else None))
    if isinstance(x, int) and x == last:
        return slope(beyond(first), ref[c, last - 1])
    return slope(ref[c, x + 1], ref[c, x - 1])


def electric_at(b_ref, r_ref, side_ref, far_ref, near_ref, place_ref, x):
    cells_x = b_ref.shape[1]
    odd = place_ref[0] >= 2
    here = [b_ref[c, x] for c in range(3)]
    dz = []
    for c in range(2):
        at = pl.ds(c * cells_x + x, 1)
        far, near = far_ref[at, :], near_ref[at, :]
        dz.append(along_z(here[c], jnp.where(odd, far, near), jnp.where(odd, near, far)))
    first = (place_ref[0] & 1) == 0
    dx = [None] + [x_slope(b_ref, side_ref, first, c, x) for c in (1, 2)]
    current = (along_row(here[2]) - dz[1], dz[0] - dx[2], dx[1] - along_row(here[0]))
    return electric_parts(current, here, r_ref[x])


def edge_kernel(b_ref, r_ref, side_ref, far_ref, near_ref, place_ref, edge_ref):
    known = (b_ref, r_ref, side_ref, far_ref, near_ref, place_ref)
    low, high = electric_at(*known, 0), electric_at(*known, b_ref.shape[1] - 1)
    first = (place_ref[0] & 1) == 0
    for c in range(2):
        edge_ref[c] = jnp.where(first, high[c + 1], low[c + 1])


def step_kernel(b_ref, r_ref, side_ref, far_ref, near_ref, place_ref, rows_ref, elec_ref):
    cells_x, cells_z = b_ref.shape[1], b_ref.shape[2]
    half = 0.5 * time_step

    def make(x):
        made = electric_at(b_ref, r_ref, side_ref, far_ref, near_ref, place_ref, x)
        for c in range(3):
            elec_ref[c, x] = made[c]

    def step(x):
        here = [elec_ref[c, x] for c in range(3)]
        dz = [along_z(here[c], 0.0, 0.0) for c in range(2)]
        dx = [None] + [x_slope(elec_ref, None, None, c, x) for c in (1, 2)]
        curl = (along_row(here[2]) - dz[1], dz[0] - dx[2], dx[1] - along_row(here[0]))
        for c in range(3):
            start = pl.multiple_of((c * cells_x + x) * cells_z, cells_z)
            rows_ref[pl.ds(start, cells_z), :] = b_ref[c, x] - time_step * curl[c]
        extra = 3 * cells_x * cells_z + 4 * x
        rows_ref[pl.ds(extra, 1), :] = half * here[1][:1]
        rows_ref[pl.ds(extra + 1, 1), :] = -half * here[1][cells_z - 1 :]
        rows_ref[pl.ds(extra + 2, 1), :] = -half * here[0][:1]
        rows_ref[pl.ds(extra + 3, 1), :] = half * here[0][cells_z - 1 :]

    over_x(cells_x, make)
    over_x(cells_x, step)


def split(value):
    high = value.astype(jnp.bfloat16)
    return high, (value - high.astype(jnp.float32)).astype(jnp.bfloat16)


def full_dot(lhs, rhs):
    dot = functools.partial(jnp.dot, preferred_element_type=jnp.float32)
    (lhs_high, lhs_low), (rhs_high, rhs_low) = split(lhs), split(rhs)
    return dot(lhs_high, rhs_high) + (dot(lhs_high, rhs_low) + dot(lhs_low, rhs_high))


def mix_kernel(cells_x, cells_z, rows_ref, edge_ref, ymix_ref, place_ref, out_ref):
    cells_y = rows_ref.shape[1]
    halves = cells_y // LANES
    mixed = full_dot(rows_ref[...], ymix_ref[...])
    first = (place_ref[0] & 1) == 0
    added = full_dot(edge_ref[...].reshape(2 * cells_z, cells_y), ymix_ref[...]) * (0.5 * time_step)
    terms = {1: added[cells_z:], 2: -added[:cells_z]}
    pairs = cells_x * halves // out_ref.shape[0]
    extra = 3 * cells_x * cells_z
    for x in range(cells_x):
        for half in range(halves):
            part, q = divmod(x * halves + half, pairs)
            lanes = slice(half * LANES, (half + 1) * LANES)
            for c in range(3):
                at = (q * 3 + c) * cells_z
                line = (c * cells_x + x) * cells_z
                tile = mixed[line : line + cells_z, lanes]
                if c and x == 0:
                    tile = tile - jnp.where(first, 0.0, terms[c][:, lanes])
                if c and x == cells_x - 1:
                    tile = tile + jnp.where(first, terms[c][:, lanes], 0.0)
                store_tile(out_ref, part, at, tile)
            at = pairs * 3 * cells_z + q * 4
            store_tile(out_ref, part, at, mixed[extra + 4 * x : extra + 4 * x + 4, lanes])


def line_matrix_kernel(zmix_ref, out_ref):
    total = zmix_ref.shape[0]
    parts = out_ref.shape[0] - total
    turned = jnp.transpose(zmix_ref[...])
    slab = lax.broadcasted_iota(jnp.int32, (parts, total), 0) * (total // parts)
    lower = (lax.broadcasted_iota(jnp.int32, (parts, total), 1) < slab).astype(jnp.float32)
    out_ref[:total] = turned
    out_ref[total:] = jnp.dot(
        lower, turned, precision=lax.Precision.HIGHEST, preferred_element_type=jnp.float32
    )


def lines_kernel(cells_z, pairs, in_ref, line_ref, out_ref):
    parts = in_ref.shape[0]
    total = parts * cells_z
    height = pairs * 3 * cells_z
    level = lax.broadcasted_iota(jnp.int32, (cells_z, LANES), 0)
    columns = []
    for q in range(pairs):
        for c in range(3):
            at = (q * 3 + c) * cells_z
            tiles = [load_tile(in_ref, s, at, cells_z) for s in range(parts)]
            if c < 2:
                low = height + q * 4 + c * 2
                for s in range(parts):
                    if s < parts - 1:
                        tiles[s] = tiles[s] + jnp.where(
                            level == cells_z - 1, one_row(in_ref, s + 1, low), 0.0
                        )
                    if s > 0:
                        tiles[s] = tiles[s] + jnp.where(
                            level == 0, one_row(in_ref, s - 1, low + 1), 0.0
                        )
            columns.append(jnp.concatenate(tiles, axis=0))
    product = full_dot(line_ref[...], jnp.concatenate(columns, axis=1))
    for g in range(3 * pairs):
        part = product[:, g * LANES : (g + 1) * LANES]
        row = height + g
        for s in range(parts):
            store_tile(out_ref, s, g * cells_z, part[s * cells_z : (s + 1) * cells_z])
            out_ref[s, row // SHORT, row % SHORT : row % SHORT + 1, :] = part[total + s : total + s + 1]


def finish_kernel(scale, cells_z, each, in_ref, next_ref, pot_ref, buffer, sems):
    _, cells_x, _, cells_y = next_ref.shape
    halves = cells_y // LANES
    batch = cells_x // PIECES
    level = lax.broadcasted_iota(jnp.int32, (cells_z, LANES), 0)
    copies = []
    for piece in range(3 * PIECES):
        c, x = divmod(piece * batch, cells_x)
        factor = -scale if c == 0 else scale
        for i in range(batch):
            for half in range(halves):
                part, q = divmod((x + i) * halves + half, each // 3)
                at = q * 3 + c
                tile = load_tile(in_ref, part, at * cells_z, cells_z)
                total, step = tile, 1
                while step < cells_z:
                    total = total + jnp.where(level >= step, pltpu.roll(total, step, 0), 0.0)
                    step *= 2
                offset = one_row(in_ref, part, each * cells_z + at)
                lanes = slice(half * LANES, (half + 1) * LANES)
                buffer[0, piece, i, :, lanes] = tile
                buffer[1, piece, i, :, lanes] = (total + offset) * factor
        for k, (target, ref) in enumerate(((c, next_ref), ((1, 0, 2)[c], pot_ref))):
            copy = pltpu.make_async_copy(
                buffer.at[k, piece], ref.at[target, pl.ds(x, batch)], sems.at[k, piece]
            )
            copy.start()
            copies.append(copy)
    for copy in copies:
        copy.wait()


def limit(mib):
    return pltpu.CompilerParams(vmem_limit_bytes=mib * 2**20)


def kernel_form(b_field, resist, ymix, zmix):
    _, cells_x, cells_z, cells_y = b_field.shape
    parts = lax.axis_size("gz")
    total_z = cells_z * parts
    f32 = jnp.float32
    shape = lambda *sizes: jax.ShapeDtypeStruct(sizes, f32)
    place = (lax.axis_index("gx") + 2 * (lax.axis_index("gz") & 1)).astype(jnp.int32).reshape(1)
    swap = lambda value: lax.ppermute(value, "gx", [(0, 1), (1, 0)])

    far, near, side = pl.pallas_call(
        pack_kernel,
        out_shape=(shape(2 * cells_x, cells_y), shape(2 * cells_x, cells_y), shape(2, cells_z, cells_y)),
        in_specs=[VMEM, SMEM],
        out_specs=(VMEM, VMEM, VMEM),
        compiler_params=limit(6),
    )(b_field, place)
    exchange = lambda value, low: lax.ppermute(
        value,
        "gz",
        [pair for i in range(low, parts - 1, 2) for pair in ((i, i + 1), (i + 1, i))],
    )
    far, near = exchange(far, 1), exchange(near, 0)
    line = pl.pallas_call(
        line_matrix_kernel,
        out_shape=shape(total_z + parts, total_z),
        in_specs=[VMEM],
        out_specs=VMEM,
        compiler_params=limit(4),
    )(zmix)
    line, far = lax.optimization_barrier((line, far))
    known = (b_field, resist, swap(side), far, near, place)
    edge = pl.pallas_call(
        edge_kernel,
        out_shape=shape(2, cells_z, cells_y),
        in_specs=[VMEM] * 5 + [SMEM],
        out_specs=VMEM,
        compiler_params=limit(6),
    )(*known)
    rows = pl.pallas_call(
        step_kernel,
        out_shape=shape(3 * cells_x * cells_z + 4 * cells_x, cells_y),
        in_specs=[VMEM] * 5 + [SMEM],
        out_specs=VMEM,
        scratch_shapes=[pltpu.VMEM(b_field.shape, f32)],
        compiler_params=limit(6),
        cost_estimate=estimate(400.0 * b_field.size),
    )(*known)
    pairs = cells_x * (cells_y // LANES) // parts
    sent = pl.pallas_call(
        functools.partial(mix_kernel, cells_x, cells_z),
        out_shape=shape(parts, pairs * (3 * cells_z + 4) // SHORT, SHORT, LANES),
        in_specs=[VMEM] * 3 + [SMEM],
        out_specs=VMEM,
        compiler_params=limit(6),
    )(rows, swap(edge), ymix, place)
    lines = lax.all_to_all(sent, "gz", split_axis=0, concat_axis=0, tiled=True)
    product = pl.pallas_call(
        functools.partial(lines_kernel, cells_z, pairs),
        out_shape=shape(parts, -(-pairs * 3 * (cells_z + 1) // SHORT), SHORT, LANES),
        in_specs=[VMEM, VMEM],
        out_specs=VMEM,
        compiler_params=limit(6),
    )(lines, line)
    returned = lax.all_to_all(product, "gz", split_axis=0, concat_axis=0, tiled=True)
    whole = jax.ShapeDtypeStruct(b_field.shape, f32)
    hbm = pl.BlockSpec(memory_space=pl.ANY)
    return pl.pallas_call(
        functools.partial(finish_kernel, total_z ** (-0.5), cells_z, 3 * pairs),
        out_shape=(whole, whole),
        in_specs=[VMEM],
        out_specs=(hbm, hbm),
        scratch_shapes=[
            pltpu.VMEM((2, 3 * PIECES, cells_x // PIECES, cells_z, cells_y), f32),
            pltpu.SemaphoreType.DMA((2, 3 * PIECES)),
        ],
        compiler_params=limit(6),
    )(returned)


def estimate(flops):
    return pl.CostEstimate(flops=int(flops), bytes_accessed=0, transcendentals=0)


def on_device(b_field, resist, ymix, zmix):
    _, cells_x, cells_z, cells_y = b_field.shape
    parts = lax.axis_size("gz")
    fits = (
        lax.axis_size("gx") == 2
        and parts > 1
        and cells_z == SUBLANES
        and cells_x % PIECES == 0
        and cells_y % LANES == 0
        and cells_x >= 4
        and cells_x * (cells_y // LANES) % parts == 0
    )
    return (kernel_form if fits else plain_form)(b_field, resist, ymix, zmix)


def solution(mesh):
    in_specs = (P(None, "gx", "gz", None), P("gx", "gz", None), P(), P())
    out_specs = (P(None, "gx", "gz", None), P(None, "gx", "gz", None))
    return jax.shard_map(
        on_device, mesh=mesh, in_specs=in_specs, out_specs=out_specs, check_vma=False
    )
```
